128 devices in a mesh: dp: 8 (over z, y_lo), tensor: 16 (over x, y_hi, core).
Axes of the slice: x: 4, y: 4 (y_hi: 2, y_lo: 2; y = y_hi * 2 + y_lo), z: 4, core: 2. Of those that a mesh axis runs over, the one named last changes fastest.
Arguments:
- tokens: bfloat16 [2048, 4096], P(('dp', 'tensor')), may hold values from -4 to 4
- lengths: int32 [8], replicated, may hold values from 64 to 256, as said below
- norm_gains: float32 [2, 4096], replicated, may hold values from 0.25 to 1.75
- query_weight: bfloat16 [2, 4096, 4096], P(None, None, 'tensor'), may hold values from -0.09375 to 0.09375
- key_weight: bfloat16 [2, 4096, 1024], P(None, None, 'tensor'), may hold values from -0.09375 to 0.09375
- value_weight: bfloat16 [2, 4096, 1024], P(None, None, 'tensor'), may hold values from -0.09375 to 0.09375
- out_weight: bfloat16 [2, 4096, 4096], P(None, 'tensor'), may hold values from -0.09375 to 0.09375
- query_probe: bfloat16 [2, 4096, 4096], P(None, 'dp', 'tensor'), may hold values from -0.09375 to 0.09375
- key_probe: bfloat16 [2, 4096, 1024], P(None, 'dp', 'tensor'), may hold values from -0.09375 to 0.09375
- value_probe: bfloat16 [2, 4096, 1024], P(None, 'dp', 'tensor'), may hold values from -0.09375 to 0.09375
- out_probe: bfloat16 [2, 4096, 4096], P(None, 'tensor', 'dp'), may hold values from -0.09375 to 0.09375
Outputs:
- query_product: float32 [2, 4096, 4096], P(None, 'dp', 'tensor')
- key_product: float32 [2, 4096, 1024], P(None, 'dp', 'tensor')
- value_product: float32 [2, 4096, 1024], P(None, 'dp', 'tensor')
- out_product: float32 [2, 4096, 4096], P(None, 'tensor', 'dp')
The draws below stay inside these ranges and needn't reach their ends.
Inputs may be any that keep to these rules, and one draw needn't show every extreme that they name: lengths[i] counts the leading valid positions of sequence i; the last sequence is full.
All inputs are finite; a program needn't handle non-finite values.
Results may differ from the reference program's by a relative error of at most 0.035.
Values may be sent and summed in bfloat16 or wider, within the bound.
A program may use at most 128 MiB of HBM per device.

```python
import math
import jax
import jax.numpy as jnp
from jax import lax

D = 4096
HEADS = 32
KVH = 8
HD = 128
LAYERS = 2
LEN = 256
SEQUENCES = 8
TOKENS = 2048
N_DP = 8
N_TENSOR = 16


def draw_tokens(key, part):
    keys = jax.random.split(key, 3)
    row_scale = jnp.exp(jax.random.uniform(keys[1], (TOKENS, 1), jnp.float32, 0.0, math.log(10.0)))
    column_scale = jnp.exp(jax.random.uniform(keys[2], (1, D), jnp.float32, 0.0, math.log(10.0)))
    base = jax.random.truncated_normal(keys[0], -4.0, 4.0, (TOKENS, D), jnp.float32)
    return (0.01 * base * row_scale * column_scale).astype(jnp.bfloat16)


def draw_lengths(key, part):
    number = jnp.arange(SEQUENCES)
    lowest = LEN // 4 + LEN // 2 * number // max(SEQUENCES - 1, 1)
    extra = jax.random.randint(key, (SEQUENCES,), 0, LEN // 4 + 1)
    drawn = jnp.minimum(lowest + extra, LEN)
    return jnp.where(number == SEQUENCES - 1, LEN, drawn).astype(jnp.int32)


def block_scale(stream_key, extent, cuts, smallest, high):
    def one(axis_at, shards_of):
        draws = jax.random.uniform(jax.random.fold_in(jax.random.fold_in(stream_key, 6), axis_at), (shards_of,), jnp.float32, smallest / len(cuts), high / len(cuts))
        return jnp.repeat(jnp.exp(draws), extent[axis_at] // shards_of).reshape((-1,) + (1,) * (len(extent) - axis_at - 1))

    level = one(*cuts[0])
    for cut in cuts[1:]:
        level = level * one(*cut)
    return level


def scatter_about(rng, shape, deviation, reach, cuts=(), kind=jnp.bfloat16):
    gain = block_scale(rng, shape, cuts, -0.22, 0.18) if cuts else 1.0
    values = jax.random.normal(rng, shape, jnp.float32) * deviation * gain
    return jnp.minimum(jnp.maximum(values, -reach), reach).astype(kind)


def setup_inputs(seed: int = 0) -> dict:
    seeds = jax.random.split(jax.random.key(seed), 12)
    tokens = draw_tokens(jax.random.fold_in(seeds[11], 71), 0)
    lengths = draw_lengths(jax.random.fold_in(seeds[11], 71), 0)
    norm_gains = jnp.clip(1.0 + 0.15 * jax.random.normal(seeds[2], (LAYERS, D), jnp.float32), 0.25, 1.75)
    query_weight = scatter_about(seeds[3], (LAYERS, D, HEADS * HD), D ** -0.5, 0.09375, ((2, 16),))
    key_weight = scatter_about(seeds[4], (LAYERS, D, KVH * HD), D ** -0.5, 0.09375, ((2, 16),))
    value_weight = scatter_about(seeds[5], (LAYERS, D, KVH * HD), D ** -0.5, 0.09375, ((2, 16),))
    out_weight = scatter_about(seeds[6], (LAYERS, HEADS * HD, D), (HEADS * HD) ** -0.5, 0.09375, ((1, 16),))
    query_probe = scatter_about(seeds[7], (LAYERS, D, HEADS * HD), D ** -0.5, 0.09375, ((1, 8), (2, 16)))
    key_probe = scatter_about(seeds[8], (LAYERS, D, KVH * HD), D ** -0.5, 0.09375, ((1, 8), (2, 16)))
    value_probe = scatter_about(seeds[9], (LAYERS, D, KVH * HD), D ** -0.5, 0.09375, ((1, 8), (2, 16)))
    out_probe = scatter_about(seeds[10], (LAYERS, HEADS * HD, D), (HEADS * HD) ** -0.5, 0.09375, ((1, 16), (2, 8)))
    return dict(tokens=tokens, lengths=lengths, norm_gains=norm_gains, query_weight=query_weight, key_weight=key_weight, value_weight=value_weight, out_weight=out_weight, query_probe=query_probe, key_probe=key_probe, value_probe=value_probe, out_probe=out_probe)


EPS = 1e-05
THETA = 500000.0

def multiply(pattern, left_side, right_side):
    return jnp.einsum(pattern, left_side.astype(jnp.float32), right_side.astype(jnp.float32))

def matmul(left_side, right_side):
    return jnp.dot(left_side, right_side, preferred_element_type=jnp.float32)

def rope_tables(length, head_size):
    position = jnp.arange(length).astype(jnp.float32)
    column = jnp.arange(head_size // 2).astype(jnp.float32)
    frequency = jnp.exp(-math.log(THETA) * 2.0 * column / head_size)
    angles = position[:, None] * frequency[None, :]
    return (jnp.cos(angles), jnp.sin(angles))

def rotate(values, cosine_table, sine_table, direction):
    middle = values.shape[-1] // 2
    leading = values[..., :middle]
    trailing = values[..., middle:]
    cosine = cosine_table[None, :, None, :]
    sine_part = direction * sine_table[None, :, None, :]
    return jnp.concatenate([leading * cosine - trailing * sine_part, trailing * cosine + leading * sine_part], axis=-1)

def allowed_mask(size, length):
    row_index = jnp.arange(size)[:, None]
    column_index = jnp.arange(size)[None, :]
    return (column_index <= row_index) & (column_index < length)

def attend(queries, key_heads, value_heads, tangent_queries, tangent_keys, tangent_values, length):
    repeat = queries.shape[1] // key_heads.shape[1]
    key_heads = jnp.repeat(key_heads, repeat, axis=1)
    value_heads = jnp.repeat(value_heads, repeat, axis=1)
    tangent_keys = jnp.repeat(tangent_keys, repeat, axis=1)
    tangent_values = jnp.repeat(tangent_values, repeat, axis=1)
    scaling = 1.0 / math.sqrt(queries.shape[-1])
    allowed = allowed_mask(queries.shape[0], length)[None]
    scores = multiply('ihd,jhd->hij', queries, key_heads) * scaling
    powers = jnp.where(allowed, jnp.exp(scores), 0.0)
    weights = powers / lax.optimization_barrier(jnp.sum(powers, axis=-1, keepdims=True))
    weights_low = weights.astype(jnp.bfloat16)
    blended = multiply('hij,jhd->ihd', weights_low, value_heads).astype(jnp.bfloat16)
    tangent_scores = (multiply('ihd,jhd->hij', tangent_queries, key_heads) + multiply('ihd,jhd->hij', queries, tangent_keys)) * scaling
    tangent_weights = weights * (tangent_scores - lax.optimization_barrier(jnp.sum(weights * tangent_scores, axis=-1, keepdims=True)))
    tangent_blended = multiply('hij,jhd->ihd', tangent_weights.astype(jnp.bfloat16), value_heads) + multiply('hij,jhd->ihd', weights_low, tangent_values)
    return (blended, tangent_blended.astype(jnp.bfloat16))

def attend_back(queries, key_heads, value_heads, grad_mixed, length):
    repeat = queries.shape[1] // key_heads.shape[1]
    key_heads = jnp.repeat(key_heads, repeat, axis=1)
    value_heads = jnp.repeat(value_heads, repeat, axis=1)
    scaling = 1.0 / math.sqrt(queries.shape[-1])
    allowed = allowed_mask(queries.shape[0], length)[None]
    scores = multiply('ihd,jhd->hij', queries, key_heads) * scaling
    powers = jnp.where(allowed, jnp.exp(scores), 0.0)
    weights = powers / lax.optimization_barrier(jnp.sum(powers, axis=-1, keepdims=True))
    weights_low = weights.astype(jnp.bfloat16)
    grad_weights = multiply('ihd,jhd->hij', grad_mixed, value_heads)
    grad_values = multiply('hij,ihd->jhd', weights_low, grad_mixed)
    grad_scores = (weights * (grad_weights - lax.optimization_barrier(jnp.sum(weights * grad_weights, axis=-1, keepdims=True))) * scaling).astype(jnp.bfloat16)
    grad_queries = multiply('hij,jhd->ihd', grad_scores, key_heads)
    grad_keys = multiply('hij,ihd->jhd', grad_scores, queries)
    return (grad_queries, grad_keys, grad_values)

def normalize(stream, gain_row):
    wide_stream = stream.astype(jnp.float32)
    inverse = lax.rsqrt(lax.optimization_barrier(jnp.mean(wide_stream * wide_stream, axis=-1, keepdims=True)) + EPS)
    return (wide_stream, inverse, (wide_stream * inverse * gain_row).astype(jnp.bfloat16))

def norm_tangent(wide_stream, inverse, tangent, gain_row):
    shift = lax.optimization_barrier(jnp.mean(wide_stream * tangent, axis=-1, keepdims=True))
    return (gain_row * (tangent * inverse - wide_stream * inverse * inverse * inverse * shift)).astype(jnp.bfloat16)

def norm_back(wide_stream, inverse, grad_normed, gain_row):
    scaled = grad_normed * gain_row
    shift = lax.optimization_barrier(jnp.mean(wide_stream * scaled, axis=-1, keepdims=True))
    return inverse * (scaled - wide_stream * inverse * inverse * shift)

def device_sum(left_terms, right_terms):

    def accumulate(running, pieces):
        partial_value = jnp.zeros_like(running)
        for left_side, right_side in zip(pieces[0], pieces[1]):
            partial_value = partial_value + matmul(left_side, right_side)
        return (running + lax.optimization_barrier(partial_value.astype(jnp.bfloat16)).astype(jnp.float32), None)
    start = jnp.zeros((left_terms[0].shape[1], right_terms[0].shape[2]), jnp.float32)
    running, unused = lax.scan(accumulate, start, (left_terms, right_terms))
    return running

def group_sum(function, arrays, shape):
    batches = tuple((member.reshape((N_DP, member.shape[0] // N_DP) + member.shape[1:]) for member in arrays))

    def accumulate(running, pieces):
        partial_value = function(*pieces)
        return (running + lax.optimization_barrier(partial_value.astype(jnp.bfloat16)).astype(jnp.float32), None)
    running, unused = lax.scan(accumulate, jnp.zeros(shape, jnp.float32), batches)
    return running

def transpose_product(left_side, right_side):
    return matmul(left_side.T, right_side)

def head_pairs(normed_piece, key_piece):
    per_group = multiply('td,tnc->ndc', normed_piece, key_piece)
    group_size = N_TENSOR // KVH
    summed = per_group.reshape(KVH, group_size, per_group.shape[1], per_group.shape[2]).sum(axis=1)
    return summed.transpose(1, 0, 2).reshape(per_group.shape[1], -1)

def reference(tokens, lengths, norm_gains, query_weight, key_weight, value_weight, out_weight, query_probe, key_probe, value_probe, out_probe):
    group_size = N_TENSOR // KVH
    per_device = HEADS // N_TENSOR
    cosine_table, sine_table = rope_tables(LEN, HD)
    token_count = lengths.shape[0] * LEN
    position = jnp.arange(token_count) % LEN
    row_mask = (position < jnp.repeat(lengths, LEN)).astype(jnp.float32)

    def heads_of(values, count):
        return values.reshape(-1, LEN, count, HD)

    def flatten(values):
        return values.reshape(token_count, -1)

    def split_devices(values, columns):
        return values.reshape(token_count, N_TENSOR, columns).transpose(1, 0, 2)
    stream = tokens
    tangent = None
    stored = []
    for layer_index in range(LAYERS):
        gain_row = norm_gains[layer_index].astype(jnp.float32)
        wide_stream, inverse, normed = normalize(stream, gain_row)
        query_primal = matmul(normed, query_weight[layer_index])
        key_primal = matmul(normed, key_weight[layer_index])
        value_primal = matmul(normed, value_weight[layer_index])
        query_moved = matmul(normed, query_probe[layer_index])
        key_moved = matmul(normed, key_probe[layer_index])
        value_moved = matmul(normed, value_probe[layer_index])
        if tangent is not None:
            tangent_normed = norm_tangent(wide_stream, inverse, tangent, gain_row)
            query_moved = query_moved + matmul(tangent_normed, query_weight[layer_index])
            key_moved = key_moved + matmul(tangent_normed, key_weight[layer_index])
            value_moved = value_moved + matmul(tangent_normed, value_weight[layer_index])
        queries = rotate(heads_of(query_primal, HEADS), cosine_table, sine_table, 1.0).astype(jnp.bfloat16)
        key_heads = rotate(heads_of(key_primal, KVH), cosine_table, sine_table, 1.0).astype(jnp.bfloat16)
        value_heads = heads_of(value_primal, KVH).astype(jnp.bfloat16)
        tangent_queries = rotate(heads_of(query_moved, HEADS), cosine_table, sine_table, 1.0).astype(jnp.bfloat16)
        tangent_keys = rotate(heads_of(key_moved, KVH), cosine_table, sine_table, 1.0).astype(jnp.bfloat16)
        tangent_values = heads_of(value_moved, KVH).astype(jnp.bfloat16)
        blended, tangent_blended = lax.map(lambda pieces: attend(*pieces), (queries, key_heads, value_heads, tangent_queries, tangent_keys, tangent_values, lengths))
        blended = flatten(blended)
        tangent_blended = flatten(tangent_blended)
        out_split = out_weight[layer_index].reshape(N_TENSOR, per_device * HD, D)
        probe_split = out_probe[layer_index].reshape(N_TENSOR, per_device * HD, D)
        blended_split = split_devices(blended, per_device * HD)
        tangent_out = device_sum((split_devices(tangent_blended, per_device * HD), blended_split), (out_split, probe_split))
        stored.append((wide_stream, inverse, normed, queries, key_heads, value_heads, blended))
        if layer_index < LAYERS - 1:
            primal_out = device_sum((blended_split,), (out_split,))
            stream = (wide_stream + primal_out).astype(jnp.bfloat16)
        tangent = tangent_out if tangent is None else tangent + tangent_out
    cotangent = row_mask[:, None] * tangent
    query_products = [None] * LAYERS
    key_products = [None] * LAYERS
    value_products = [None] * LAYERS
    out_products = [None] * LAYERS
    for layer_index in reversed(range(LAYERS)):
        wide_stream, inverse, normed, queries, key_heads, value_heads, blended = stored[layer_index]
        cotangent_low = cotangent.astype(jnp.bfloat16)
        out_products[layer_index] = group_sum(transpose_product, (blended, cotangent_low), (HEADS * HD, D))
        grad_mixed = matmul(cotangent_low, out_weight[layer_index].T).astype(jnp.bfloat16)
        grad_queries, grad_keys, grad_values = lax.map(lambda pieces: attend_back(*pieces), (queries, key_heads, value_heads, heads_of(grad_mixed, HEADS), lengths))
        query_low = flatten(rotate(grad_queries, cosine_table, sine_table, -1.0).astype(jnp.bfloat16))
        key_grouped = grad_keys.reshape(-1, LEN, N_TENSOR, per_device, HD).sum(axis=3)
        key_low = rotate(key_grouped, cosine_table, sine_table, -1.0).astype(jnp.bfloat16).reshape(token_count, N_TENSOR, HD)
        value_low = grad_values.reshape(-1, LEN, N_TENSOR, per_device, HD).sum(axis=3).astype(jnp.bfloat16).reshape(token_count, N_TENSOR, HD)
        query_products[layer_index] = group_sum(transpose_product, (normed, query_low), (D, HEADS * HD))
        key_products[layer_index] = group_sum(head_pairs, (normed, key_low), (D, KVH * HD))
        value_products[layer_index] = group_sum(head_pairs, (normed, value_low), (D, KVH * HD))
        if layer_index > 0:
            key_split = jnp.repeat(key_weight[layer_index].reshape(D, KVH, HD).transpose(1, 2, 0), group_size, axis=0)
            value_split = jnp.repeat(value_weight[layer_index].reshape(D, KVH, HD).transpose(1, 2, 0), group_size, axis=0)
            query_split = query_weight[layer_index].T.reshape(N_TENSOR, per_device * HD, D)
            grad_normed = device_sum((split_devices(query_low, per_device * HD), key_low.transpose(1, 0, 2), value_low.transpose(1, 0, 2)), (query_split, key_split, value_split))
            cotangent = cotangent + norm_back(wide_stream, inverse, grad_normed, norm_gains[layer_index].astype(jnp.float32))
    return (jnp.stack(query_products), jnp.stack(key_products), jnp.stack(value_products), jnp.stack(out_products))
```

```python
import functools
import math

import jax
import jax.numpy as jnp
from jax import lax
from jax.experimental import pallas as pl
from jax.experimental.pallas import tpu as pltpu
from jax.sharding import PartitionSpec as P

HD = 128
LEN = 256
EPS = 1e-05
THETA = 500000.0

MESH = pl.DeviceIdType.MESH
F32 = jnp.float32
BF16 = jnp.bfloat16
VMEM = pl.BlockSpec(memory_space=pltpu.VMEM)
HBM = pl.BlockSpec(memory_space=pl.ANY)
DMA = pltpu.SemaphoreType.DMA

HOPS = ((1, 1), (3, 1), (2, 1), (2, 0), (1, 0), (3, 0), (0, 1))


def back(hop):
    return ((4 - hop[0]) % 4, hop[1])


def data_at(d, hop):
    ring, pair = lax.div(d, 2), lax.rem(d, 2)
    return lax.rem(ring + hop[0], 4) * 2 + lax.rem(pair + hop[1], 2)


def chip_at(t, hop):
    return data_at(lax.div(t, 2), hop)


def tensor_at(t, hop):
    return chip_at(t, hop) * 2 + lax.rem(t, 2)


def other_core(t):
    return t + 1 - 2 * lax.rem(t, 2)


def places():
    return lax.axis_index("dp"), lax.axis_index("tensor")


def remote(src, dst, sends, recvs, j, device):
    return pltpu.make_async_remote_copy(
        src_ref=src,
        dst_ref=dst,
        send_sem=sends.at[j],
        recv_sem=recvs.at[j],
        device_id=device,
        device_id_type=MESH,
    )


def enter(over_tensor, over_data):
    d, t = places()
    barrier = pltpu.get_barrier_semaphore()
    peers = [(d, other_core(t))]
    if over_tensor:
        peers += [(d, tensor_at(t, hop)) for hop in HOPS]
    if over_data:
        peers += [(data_at(d, hop), t) for hop in HOPS]
    for peer in peers:
        pl.semaphore_signal(barrier, inc=1, device_id=peer, device_id_type=MESH)
    pl.semaphore_wait(barrier, len(peers))


class TensorGather:
    scratch = [DMA((16,)), DMA((16,))]

    def __init__(self, src, out, sends, recvs):
        self.src, self.out, self.sends, self.recvs = src, out, sends, recvs

    def cross(self, j):
        d, t = places()
        return remote(self.src, self.out.at[t], self.sends, self.recvs, j, (d, tensor_at(t, HOPS[j])))

    def arrived(self, j):
        d, t = places()
        slot = self.out.at[tensor_at(t, back(HOPS[j]))]
        return remote(slot, slot, self.sends, self.recvs, j, (d, other_core(t)))

    def handed(self, j):
        d, t = places()
        slot = self.out.at[tensor_at(t, back(HOPS[j]))]
        return remote(slot, slot, self.sends, self.recvs, 8 + j, (d, other_core(t)))

    def received(self, j):
        d, t = places()
        slot = self.out.at[tensor_at(other_core(t), back(HOPS[j]))]
        return remote(slot, slot, self.sends, self.recvs, 8 + j, (d, other_core(t)))

    def near(self):
        d, t = places()
        return remote(self.src, self.out.at[t], self.sends, self.recvs, 7, (d, other_core(t)))

    def own(self):
        d, t = places()
        return pltpu.make_async_copy(self.src, self.out.at[t], self.sends.at[15])

    def start(self):
        for j in range(7):
            self.cross(j).start()
        self.near().start()
        self.own().start()

    def finish(self):
        d, t = places()
        for j in (6, 4, 5, 3, 0, 1, 2):
            self.arrived(j).wait_recv()
            self.handed(j).start()
        slot = self.out.at[other_core(t)]
        remote(slot, slot, self.sends, self.recvs, 7, (d, other_core(t))).wait_recv()
        for j in (6, 4, 5, 3, 0, 1, 2):
            self.received(j).wait_recv()
            self.cross(j).wait_send()
            self.handed(j).wait_send()
        self.near().wait_send()
        self.own().wait()


class TensorSum:
    @staticmethod
    def scratch(columns):
        return [
            pltpu.VMEM((8, 16, columns), BF16),
            pltpu.VMEM((7, 16, columns), BF16),
            pltpu.VMEM((7, 16, columns), BF16),
            DMA((15,)),
            DMA((15,)),
        ]

    def __init__(self, part, near, sent, far, sends, recvs):
        self.part, self.near_, self.sent, self.far = part, near, sent, far
        self.sends, self.recvs = sends, recvs

    def swap(self, j):
        d, t = places()
        k = chip_at(t, HOPS[j] if j < 7 else (0, 0))
        c = lax.rem(t, 2)
        return remote(
            self.part.at[k, 1 - c], self.near_.at[k], self.sends, self.recvs, j, (d, other_core(t))
        )

    def cross(self, j):
        d, t = places()
        return remote(
            self.sent.at[j], self.far.at[j], self.sends, self.recvs, 8 + j, (d, tensor_at(t, HOPS[j]))
        )

    def pair_sum(self, k):
        d, t = places()
        c = lax.rem(t, 2)
        return self.part[k, c].astype(F32) + self.near_[k].astype(F32)

    def start(self):
        for j in range(8):
            self.swap(j).start()

    def send(self):
        d, t = places()
        for j in range(7):
            self.swap(j).wait_recv()
            self.sent[j] = self.pair_sum(chip_at(t, HOPS[j])).astype(BF16)
            self.cross(j).start()

    def total(self):
        d, t = places()
        self.swap(7).wait_recv()
        total = self.pair_sum(chip_at(t, (0, 0)))
        for j in (6, 4, 5, 3, 0, 1, 2):
            self.cross(j).wait_recv()
            total = total + self.far[j].astype(F32)
        return total

    def finish(self):
        for j in range(8):
            self.swap(j).wait_send()
        for j in range(7):
            self.cross(j).wait_send()


class DataGather:
    scratch = [DMA((8,)), DMA((7,))]
    ROUTES = (
        ((0, 1), (0, 0), (0, 1)),
        ((1, 0), (0, 0), (3, 0)),
        ((3, 0), (0, 0), (1, 0)),
        ((2, 0), (0, 0), (2, 0)),
        ((1, 0), (0, 1), (3, 1)),
        ((3, 0), (0, 1), (1, 1)),
        ((0, 1), (2, 0), (2, 1)),
    )

    def __init__(self, src, slot, sends, recvs):
        self.src, self.slot, self.sends, self.recvs = src, slot, sends, recvs

    def out(self, j):
        d, t = places()
        hop, block, unused = self.ROUTES[j]
        slot = self.slot(data_at(d, block))
        src = self.src if j < 4 else slot
        return remote(src, slot, self.sends, self.recvs, j, (data_at(d, hop), t))

    def into(self, j):
        d, t = places()
        slot = self.slot(data_at(d, self.ROUTES[j][2]))
        return remote(slot, slot, self.sends, self.recvs, j, (d, other_core(t)))

    def own(self):
        d, t = places()
        return pltpu.make_async_copy(self.src, self.slot(d), self.sends.at[7])

    def start(self):
        for j in range(4):
            self.out(j).start()
        self.own().start()

    def relay(self):
        self.into(0).wait_recv()
        self.out(4).start()
        self.out(5).start()
        self.into(3).wait_recv()
        self.out(6).start()

    def finish(self):
        for j in (1, 2, 4, 5, 6):
            self.into(j).wait_recv()
        for j in range(7):
            self.out(j).wait_send()
        self.own().wait()


class DataExchange:
    scratch = [DMA((15,)), DMA((14,))]

    def __init__(self, src, out, sends, recvs):
        self.src, self.out_, self.sends, self.recvs = src, out, sends, recvs
        self.half = src.shape[0] // 2
        self.share = src.shape[1] // 8

    def rows(self, t):
        return pl.ds(pl.multiple_of(lax.rem(t, 2) * self.half, self.half), self.half)

    def columns(self, d):
        return pl.ds(pl.multiple_of(d * self.share, self.share), self.share)

    def cross(self, j):
        d, t = places()
        peer = data_at(d, HOPS[j])
        return remote(
            self.src.at[self.rows(t), self.columns(peer)],
            self.out_.at[d, self.rows(t)],
            self.sends,
            self.recvs,
            j,
            (peer, t),
        )

    def hand(self, j, t_of):
        d, t = places()
        slot = self.out_.at[data_at(d, back(HOPS[j])), self.rows(t_of)]
        return slot

    def arrived(self, j):
        d, t = places()
        slot = self.hand(j, t)
        return remote(slot, slot, self.sends, self.recvs, j, (d, other_core(t)))

    def handed(self, j):
        d, t = places()
        slot = self.hand(j, t)
        return remote(slot, slot, self.sends, self.recvs, 7 + j, (d, other_core(t)))

    def received(self, j):
        d, t = places()
        slot = self.hand(j, other_core(t))
        return remote(slot, slot, self.sends, self.recvs, 7 + j, (d, other_core(t)))

    def own(self):
        d, t = places()
        return pltpu.make_async_copy(
            self.src.at[:, self.columns(d)], self.out_.at[d], self.sends.at[14]
        )

    def start(self):
        for j in range(7):
            self.cross(j).start()
        self.own().start()

    def finish(self):
        for j in (6, 4, 5, 3, 0, 1, 2):
            self.arrived(j).wait_recv()
            self.handed(j).start()
        for j in range(7):
            self.received(j).wait_recv()
            self.cross(j).wait_send()
            self.handed(j).wait_send()
        self.own().wait()


def taken(refs, *counts):
    out, at = [], 0
    for count in counts:
        out.append(refs[at : at + count])
        at += count
    return out


def comm_call(kernel, name, number, in_specs, out_specs, out_shape, scratch, args):
    return pl.pallas_call(
        kernel,
        name=name,
        in_specs=in_specs,
        out_specs=out_specs,
        out_shape=out_shape,
        scratch_shapes=scratch,
        compiler_params=pltpu.CompilerParams(
            collective_id=number, has_side_effects=True, vmem_limit_bytes=40 * 2**20
        ),
    )(*args)


def shape(dims, dtype):
    return jax.ShapeDtypeStruct(dims, dtype)


def slot_of(ref):
    return lambda block: ref.at[block]


def columns_of(ref):
    width = ref.shape[1] // 8
    return lambda block: ref.at[:, pl.ds(pl.multiple_of(block * width, width), width)]


def mean_of(values):
    return jnp.sum(values, axis=-1, keepdims=True) * (1.0 / values.shape[-1])


def probe_jobs(layer, probes, gathered, sems):
    q, kv, o = probes
    gq, gkv, go = gathered
    return [
        DataGather(q.at[layer], slot_of(gq), *sems[0:2]),
        DataGather(kv.at[layer], slot_of(gkv), *sems[2:4]),
        DataGather(o.at[layer], columns_of(go), *sems[4:6]),
    ]


def probe_shapes(probes):
    q, kv, o = probes
    return [
        shape((8,) + q.shape[1:], BF16),
        shape((8,) + kv.shape[1:], BF16),
        shape((o.shape[1], 8 * o.shape[2]), BF16),
    ]


def first_kernel(tokens, gain, q, kv, o, h_all, gq, gkv, go, h_low, *sems):
    wide = tokens[...].astype(F32)
    inverse = lax.rsqrt(mean_of(wide * wide) + EPS)
    h_low[...] = (wide * inverse * gain[...]).astype(BF16)
    enter(True, True)
    rows = TensorGather(h_low, h_all, *sems[:2])
    jobs = probe_jobs(0, (q, kv, o), (gq, gkv, go), sems[2:])
    rows.start()
    for job in jobs:
        job.start()
    rows.finish()
    for job in jobs:
        job.relay()
    for job in jobs:
        job.finish()


def first(tokens, gain, probes):
    rows, width = tokens.shape
    return comm_call(
        first_kernel,
        "first",
        1,
        [VMEM, VMEM, HBM, HBM, HBM],
        [VMEM, HBM, HBM, HBM],
        [shape((16, rows, width), BF16)] + probe_shapes(probes),
        [pltpu.VMEM((rows, width), BF16)] + TensorGather.scratch + DataGather.scratch * 3,
        (tokens, gain) + probes,
    )


def between_kernel(*refs):
    (
        (primal, moved, tokens, gain, q, kv, o),
        (x_out, t_out, h_all, th_all, gq, gkv, go),
        (h_low, th_low),
        sum_a,
        sum_b,
        gather_a,
        gather_b,
        sems,
    ) = taken(refs, 7, 7, 2, 5, 5, 2, 2, 6)
    enter(True, True)
    sums = [TensorSum(primal, *sum_a), TensorSum(moved, *sum_b)]
    jobs = probe_jobs(1, (q, kv, o), (gq, gkv, go), sems)
    for one in sums:
        one.start()
    for one in sums:
        one.send()
    for job in jobs:
        job.start()
    stream = (tokens[...].astype(F32) + sums[0].total()).astype(BF16)
    x_out[...] = stream
    wide = stream.astype(F32)
    inverse = lax.rsqrt(mean_of(wide * wide) + EPS)
    h_low[...] = (wide * inverse * gain[...]).astype(BF16)
    rows_a = TensorGather(h_low, h_all, *gather_a)
    tangent = sums[1].total()
    t_out[...] = tangent
    rows_a.start()
    shift = mean_of(wide * tangent)
    th_low[...] = (
        gain[...] * (tangent * inverse - wide * inverse * inverse * inverse * shift)
    ).astype(BF16)
    rows_b = TensorGather(th_low, th_all, *gather_b)
    for job in jobs:
        job.relay()
    rows_b.start()
    for one in sums:
        one.finish()
    rows_a.finish()
    rows_b.finish()
    for job in jobs:
        job.finish()


def between(primal, moved, tokens, gain, probes):
    rows, width = tokens.shape
    return comm_call(
        between_kernel,
        "between",
        2,
        [VMEM] * 4 + [HBM] * 3,
        [VMEM] * 4 + [HBM] * 3,
        [
            shape((rows, width), BF16),
            shape((rows, width), F32),
            shape((16, rows, width), BF16),
            shape((16, rows, width), BF16),
        ]
        + probe_shapes(probes),
        [pltpu.VMEM((rows, width), BF16)] * 2
        + TensorSum.scratch(width) * 2
        + TensorGather.scratch * 2
        + DataGather.scratch * 3,
        (primal, moved, tokens, gain) + probes,
    )


def turn_kernel(*refs):
    (
        (moved, t_one, mask, a_zero, a_one, h_one),
        (c_out, cb_all, ga_zero, ga_one, hs_one),
        (c_low,),
        sum_a,
        gather_a,
        sems,
    ) = taken(refs, 6, 5, 1, 5, 2, 6)
    enter(True, True)
    total = TensorSum(moved, *sum_a)
    jobs = [
        DataGather(a_zero, slot_of(ga_zero), *sems[0:2]),
        DataGather(a_one, slot_of(ga_one), *sems[2:4]),
    ]
    swap = DataExchange(h_one, hs_one, *sems[4:6])
    total.start()
    total.send()
    for job in jobs:
        job.start()
    swap.start()
    cotangent = mask[:, 0:1] * (t_one[...] + total.total())
    c_out[...] = cotangent
    c_low[...] = cotangent.astype(BF16)
    for job in jobs:
        job.relay()
    rows = TensorGather(c_low, cb_all, *gather_a)
    rows.start()
    total.finish()
    rows.finish()
    swap.finish()
    for job in jobs:
        job.finish()


def turn(moved, t_one, mask, a_zero, a_one, h_one):
    rows, width = t_one.shape
    return comm_call(
        turn_kernel,
        "turn",
        3,
        [VMEM] * 3 + [HBM] * 3,
        [VMEM] * 2 + [HBM] * 3,
        [
            shape((rows, width), F32),
            shape((16, rows, width), BF16),
            shape((8,) + a_zero.shape, BF16),
            shape((8,) + a_one.shape, BF16),
            shape((8, h_one.shape[0], h_one.shape[1] // 8), BF16),
        ],
        [pltpu.VMEM((rows, width), BF16)]
        + TensorSum.scratch(width)
        + TensorGather.scratch
        + DataGather.scratch * 2
        + DataExchange.scratch,
        (moved, t_one, mask, a_zero, a_one, h_one),
    )


def lower_kernel(*refs):
    (
        (part, c_two, x_one, gain, g_one, cb_one, h_zero),
        (cb_all, gg_one, cbs_one, hs_zero),
        (c_low,),
        sum_a,
        gather_a,
        sems,
    ) = taken(refs, 7, 4, 1, 5, 2, 6)
    enter(True, True)
    total = TensorSum(part, *sum_a)
    job = DataGather(g_one, slot_of(gg_one), *sems[0:2])
    swaps = [
        DataExchange(cb_one, cbs_one, *sems[2:4]),
        DataExchange(h_zero, hs_zero, *sems[4:6]),
    ]
    total.start()
    total.send()
    job.start()
    for swap in swaps:
        swap.start()
    scaled = total.total() * gain[...]
    wide = x_one[...].astype(F32)
    inverse = lax.rsqrt(mean_of(wide * wide) + EPS)
    shift = mean_of(wide * scaled)
    cotangent = c_two[...] + inverse * (scaled - wide * inverse * inverse * shift)
    c_low[...] = cotangent.astype(BF16)
    job.relay()
    rows = TensorGather(c_low, cb_all, *gather_a)
    rows.start()
    total.finish()
    rows.finish()
    for swap in swaps:
        swap.finish()
    job.finish()


def lower(part, c_two, x_one, gain, g_one, cb_one, h_zero):
    rows, width = c_two.shape
    return comm_call(
        lower_kernel,
        "lower",
        4,
        [VMEM] * 4 + [HBM] * 3,
        [VMEM] + [HBM] * 3,
        [
            shape((16, rows, width), BF16),
            shape((8,) + g_one.shape, BF16),
            shape((8, cb_one.shape[0], width // 8), BF16),
            shape((8, h_zero.shape[0], width // 8), BF16),
        ],
        [pltpu.VMEM((rows, width), BF16)]
        + TensorSum.scratch(width)
        + TensorGather.scratch
        + DataGather.scratch
        + DataExchange.scratch * 2,
        (part, c_two, x_one, gain, g_one, cb_one, h_zero),
    )


def last_kernel(*refs):
    (g_zero, cb_zero), (gg_zero, cbs_zero), sems = taken(refs, 2, 2, 4)
    enter(False, True)
    job = DataGather(g_zero, slot_of(gg_zero), *sems[0:2])
    swap = DataExchange(cb_zero, cbs_zero, *sems[2:4])
    job.start()
    swap.start()
    job.relay()
    swap.finish()
    job.finish()


def last(g_zero, cb_zero):
    return comm_call(
        last_kernel,
        "last",
        5,
        [HBM] * 2,
        [HBM] * 2,
        [
            shape((8,) + g_zero.shape, BF16),
            shape((8, cb_zero.shape[0], cb_zero.shape[1] // 8), BF16),
        ],
        DataGather.scratch + DataExchange.scratch,
        (g_zero, cb_zero),
    )


def swapped(value, axis, apart):
    mask = 2**apart
    pairs = [(source, source ^ mask) for source in range(lax.axis_size(axis))]
    return lax.ppermute(value, axis, pairs)


def multiply(pattern, left_side, right_side):
    return jnp.einsum(pattern, left_side, right_side, preferred_element_type=F32)


def matmul(left_side, right_side):
    return jnp.dot(left_side, right_side, preferred_element_type=F32)


def contract_rows(left_side, right_side):
    return lax.dot_general(
        left_side, right_side, (((0,), (0,)), ((), ())), preferred_element_type=F32
    )


def contract_last(left_side, right_side):
    return lax.dot_general(
        left_side, right_side, (((1,), (1,)), ((), ())), preferred_element_type=F32
    )


def rope_tables(length, head_size):
    position = jnp.arange(length).astype(F32)
    column = jnp.arange(head_size // 2).astype(F32)
    frequency = jnp.exp(-math.log(THETA) * 2.0 * column / head_size)
    angles = position[:, None] * frequency[None, :]
    return (jnp.cos(angles), jnp.sin(angles))


def rotate(values, cosine_table, sine_table, direction):
    middle = values.shape[-1] // 2
    leading = values[..., :middle]
    trailing = values[..., middle:]
    cosine = cosine_table[:, None, :]
    sine_part = direction * sine_table[:, None, :]
    return jnp.concatenate(
        [leading * cosine - trailing * sine_part, trailing * cosine + leading * sine_part], axis=-1
    )


def attention_weights(queries, key_heads, allowed):
    scaling = 1.0 / math.sqrt(queries.shape[-1])
    scores = multiply("ihd,jd->hij", queries, key_heads) * scaling
    powers = jnp.where(allowed, jnp.exp(scores), 0.0)
    return powers / jnp.sum(powers, axis=-1, keepdims=True)


def attend(q, k, v, tq, tk, tv, allowed):
    scaling = 1.0 / math.sqrt(q.shape[-1])
    weights = attention_weights(q, k, allowed)
    weights_low = weights.astype(BF16)
    blended = multiply("hij,jd->ihd", weights_low, v).astype(BF16)
    tangent_scores = (multiply("ihd,jd->hij", tq, k) + multiply("ihd,jd->hij", q, tk)) * scaling
    tangent_weights = weights * (
        tangent_scores - jnp.sum(weights * tangent_scores, axis=-1, keepdims=True)
    )
    tangent_blended = multiply("hij,jd->ihd", tangent_weights.astype(BF16), v) + multiply(
        "hij,jd->ihd", weights_low, tv
    )
    return (blended, tangent_blended.astype(BF16))


def attend_back(q, k, v, grad_mixed, allowed):
    scaling = 1.0 / math.sqrt(q.shape[-1])
    weights = attention_weights(q, k, allowed)
    weights_low = weights.astype(BF16)
    grad_weights = multiply("ihd,jd->hij", grad_mixed, v)
    grad_values = multiply("hij,ihd->jd", weights_low, grad_mixed)
    grad_scores = (
        weights * (grad_weights - jnp.sum(weights * grad_weights, axis=-1, keepdims=True)) * scaling
    ).astype(BF16)
    grad_queries = multiply("hij,jd->ihd", grad_scores, k)
    grad_keys = multiply("hij,ihd->jd", grad_scores, q)
    return (grad_queries, grad_keys, grad_values)


def body(
    tokens,
    lengths,
    norm_gains,
    query_weight,
    key_weight,
    value_weight,
    out_weight,
    query_probe,
    key_probe,
    value_probe,
    out_probe,
):
    tensor_index = lax.axis_index("tensor")
    data_index = lax.axis_index("dp")
    share_rows, width = tokens.shape
    half = key_weight.shape[2]
    cosine_table, sine_table = rope_tables(LEN, HD)
    length = lax.dynamic_slice_in_dim(lengths, data_index, 1)[0]
    row_index = jnp.arange(LEN)[:, None]
    column_index = jnp.arange(LEN)[None, :]
    allowed = ((column_index <= row_index) & (column_index < length))[None]
    share_position = tensor_index * share_rows + jnp.arange(share_rows)
    share_mask = jnp.broadcast_to(
        (share_position < length).astype(F32)[:, None], (share_rows, 128)
    )
    lower_half = tensor_index % 2 == 0
    gains = [norm_gains[layer][None, :] for layer in range(2)]

    kv_probe = jnp.concatenate([key_probe, value_probe], axis=-1)
    kv_weight = [
        jnp.concatenate([key_weight[layer], value_weight[layer]], axis=-1) for layer in range(2)
    ]
    probes = (query_probe, kv_probe, out_probe)

    def heads_of(values):
        return values.reshape(LEN, -1, HD)

    def turned(values, direction=1.0):
        return rotate(heads_of(values), cosine_table, sine_table, direction)

    def joined(own, other):
        return jnp.where(
            lower_half,
            jnp.concatenate([own, other], axis=-1),
            jnp.concatenate([other, own], axis=-1),
        )

    def forward(layer, normed, normed_tangent, probe_q, probe_kv, probe_o):
        q = matmul(normed, query_weight[layer])
        tq = matmul(normed, probe_q)
        kv = matmul(normed, kv_weight[layer])
        tkv = matmul(normed, probe_kv)
        if normed_tangent is not None:
            tq = tq + matmul(normed_tangent, query_weight[layer])
            tkv = tkv + matmul(normed_tangent, kv_weight[layer])
        own = jnp.concatenate([kv, tkv], axis=-1)
        other = swapped(own.astype(BF16), "tensor", 0).astype(F32)
        k, v, tk, tv = [
            joined(own[:, at : at + half], other[:, at : at + half])
            for at in range(0, 4 * half, half)
        ]
        q, tq = turned(q).astype(BF16), turned(tq).astype(BF16)
        k, tk = turned(k)[:, 0].astype(BF16), turned(tk)[:, 0].astype(BF16)
        v, tv = v.astype(BF16), tv.astype(BF16)
        a, ta = attend(q, k, v, tq, tk, tv, allowed)
        a, ta = a.reshape(LEN, -1), ta.reshape(LEN, -1)
        moved = (matmul(ta, out_weight[layer]) + matmul(a, probe_o)).astype(BF16)
        primal = matmul(a, out_weight[layer]).astype(BF16) if layer == 0 else None
        return (q, k, v, a, primal, moved)

    def backward(layer, q, k, v, cb):
        grad_mixed = contract_last(cb, out_weight[layer]).astype(BF16)
        gq, gk, gv = attend_back(q, k, v, heads_of(grad_mixed), allowed)
        gq = rotate(gq, cosine_table, sine_table, -1.0).astype(BF16).reshape(LEN, -1)
        gk = rotate(gk[:, None], cosine_table, sine_table, -1.0)[:, 0].astype(BF16)
        gv = gv.astype(BF16)
        low = jnp.concatenate([gk[:, :half], gv[:, :half]], axis=-1)
        high = jnp.concatenate([gk[:, half:], gv[:, half:]], axis=-1)
        mine, theirs = jnp.where(lower_half, low, high), jnp.where(lower_half, high, low)
        came = swapped(theirs, "tensor", 0)
        gkv = (mine.astype(F32) + came.astype(F32)).astype(BF16)
        return (gq, gkv)

    def by_owner(part):
        return part.reshape(8, 2, share_rows, width)

    def whole(rows):
        return rows.reshape(LEN, width)

    def all_rows(blocks):
        return blocks.reshape(-1, blocks.shape[-1])

    h_zero, pq, pkv, po = first(tokens, gains[0], probes)
    h_zero = whole(h_zero)
    q0, k0, v0, a_zero, primal, moved = forward(
        0, h_zero, None, all_rows(pq), all_rows(pkv), po
    )
    x_one, t_one, h_one, th_one, pq, pkv, po = between(
        by_owner(primal), by_owner(moved), tokens, gains[1], probes
    )
    h_one, th_one = whole(h_one), whole(th_one)
    q1, k1, v1, a_one, unused, moved = forward(
        1, h_one, th_one, all_rows(pq), all_rows(pkv), po
    )
    c_two, cb_one, ga_zero, ga_one, hs_one = turn(
        by_owner(moved), t_one, share_mask, a_zero, a_one, h_one
    )
    cb_one = whole(cb_one)
    gq, gkv = backward(1, q1, k1, v1, cb_one)
    g_one = jnp.concatenate([gq, gkv], axis=-1)
    part = contract_last(gq, query_weight[1]) + contract_last(gkv, kv_weight[1])
    cb_zero, gg_one, cbs_one, hs_zero = lower(
        by_owner(part.astype(BF16)), c_two, x_one, gains[1], g_one, cb_one, h_zero
    )
    cb_zero = whole(cb_zero)
    gq, gkv = backward(0, q0, k0, v0, cb_zero)
    g_zero = jnp.concatenate([gq, gkv], axis=-1)
    gg_zero, cbs_zero = last(g_zero, cb_zero)

    sides = [(hs_zero, gg_zero, ga_zero, cbs_zero), (hs_one, gg_one, ga_one, cbs_one)]
    products = []
    for hs, gg, ga, cbs in sides:
        inner = contract_rows(all_rows(hs), all_rows(gg))
        outer = contract_rows(all_rows(ga), all_rows(cbs))
        q_width = inner.shape[1] - 2 * half
        products.append(
            (inner[:, :q_width], inner[:, q_width:-half], inner[:, -half:], outer)
        )
    return tuple(jnp.stack([products[0][n], products[1][n]]) for n in range(4))


def solution(mesh):
    placed = (
        P(("dp", "tensor"), None),
        P(),
        P(),
        P(None, None, "tensor"),
        P(None, None, "tensor"),
        P(None, None, "tensor"),
        P(None, "tensor", None),
        P(None, "dp", "tensor"),
        P(None, "dp", "tensor"),
        P(None, "dp", "tensor"),
        P(None, "tensor", "dp"),
    )
    return jax.shard_map(
        body,
        mesh=mesh,
        in_specs=placed,
        out_specs=(
            P(None, "dp", "tensor"),
            P(None, "dp", "tensor"),
            P(None, "dp", "tensor"),
            P(None, "tensor", "dp"),
        ),
        check_vma=False,
    )
```

```python
import functools
import math

import jax
import jax.numpy as jnp
import numpy as np
from jax import lax
from jax.experimental import pallas as pl
from jax.experimental.pallas import tpu as pltpu
from jax.sharding import PartitionSpec as P

HD = 128
LEN = 256
EPS = 1e-05
THETA = 500000.0

MESH = pl.DeviceIdType.MESH
F32 = jnp.float32
BF16 = jnp.bfloat16
VMEM = pl.BlockSpec(memory_space=pltpu.VMEM)
HBM = pl.BlockSpec(memory_space=pl.ANY)
DMA = pltpu.SemaphoreType.DMA

HOPS = ((1, 1), (3, 1), (2, 1), (2, 0), (1, 0), (3, 0), (0, 1))


def back(hop):
    return ((4 - hop[0]) % 4, hop[1])


def data_at(d, hop):
    ring, pair = lax.div(d, 2), lax.rem(d, 2)
    return lax.rem(ring + hop[0], 4) * 2 + lax.rem(pair + hop[1], 2)


def chip_at(t, hop):
    return data_at(lax.div(t, 2), hop)


def tensor_at(t, hop):
    return chip_at(t, hop) * 2 + lax.rem(t, 2)


def other_core(t):
    return t + 1 - 2 * lax.rem(t, 2)


def places():
    return lax.axis_index("dp"), lax.axis_index("tensor")


def remote(src, dst, sends, recvs, j, device):
    return pltpu.make_async_remote_copy(
        src_ref=src,
        dst_ref=dst,
        send_sem=sends.at[j],
        recv_sem=recvs.at[j],
        device_id=device,
        device_id_type=MESH,
    )


def enter(over_tensor, over_data):
    d, t = places()
    barrier = pltpu.get_barrier_semaphore()
    peers = [(d, other_core(t))]
    if over_tensor:
        peers += [(d, tensor_at(t, hop)) for hop in HOPS]
    if over_data:
        peers += [(data_at(d, hop), t) for hop in HOPS]
    for peer in peers:
        pl.semaphore_signal(barrier, inc=1, device_id=peer, device_id_type=MESH)
    pl.semaphore_wait(barrier, len(peers))


class RingGather:
    ROUTES = (
        ((0, 1), (0, 0), (0, 1)),
        ((1, 0), (0, 0), (3, 0)),
        ((3, 0), (0, 0), (1, 0)),
        ((2, 0), (0, 0), (2, 0)),
        ((1, 0), (0, 1), (3, 1)),
        ((3, 0), (0, 1), (1, 1)),
    )
    LAST = ((0, 1), (2, 0), (2, 1))
    WAITS = 7

    def __init__(self, src, slot, sends, recvs):
        self.src, self.slot, self.sends, self.recvs = src, slot, sends, recvs
        self.routes = self.ROUTES + (self.LAST,)

    def place(self, hop):
        d, t = places()
        return data_at(d, hop)

    def device(self, hop):
        d, t = places()
        return (data_at(d, hop), t)

    def out(self, j):
        hop, block, unused = self.routes[j]
        slot = self.slot(self.place(block))
        src = self.src if j < 4 else slot
        return remote(src, slot, self.sends, self.recvs, j, self.device(hop))

    def into(self, j):
        slot = self.slot(self.place(self.routes[j][2]))
        return remote(slot, slot, self.sends, self.recvs, j, self.device((0, 1)))

    def own(self):
        return pltpu.make_async_copy(self.src, self.slot(self.place((0, 0))), self.sends.at[7])

    def hand(self, j):
        pass

    def start(self):
        for j in range(4):
            self.out(j).start()
        self.own().start()

    def relay(self):
        self.into(0).wait_recv()
        self.out(4).start()
        self.out(5).start()
        if self.LAST[0] == (0, 1):
            self.into(3).wait_recv()
        self.out(6).start()
        self.hand(0)

    def finish(self):
        for j in (1, 2, 3, 4, 5, 6):
            if j != 3 or self.LAST[0] != (0, 1):
                self.into(j).wait_recv()
                self.hand(j)
        for j in range(7):
            self.out(j).wait_send()
        self.own().wait()


class DataGather(RingGather):
    scratch = [DMA((8,)), DMA((7,))]


class TensorGather(RingGather):
    scratch = [DMA((16,)), DMA((15,))]
    LAST = ((2, 0), (0, 1), (2, 1))

    def place(self, hop):
        d, t = places()
        return tensor_at(t, hop)

    def device(self, hop):
        d, t = places()
        return (d, tensor_at(t, hop))

    def near(self):
        d, t = places()
        return pltpu.make_async_remote_copy(
            src_ref=self.src,
            dst_ref=self.slot(t),
            send_sem=self.sends.at[15],
            recv_sem=self.recvs.at[14],
            device_id=(d, other_core(t)),
            device_id_type=MESH,
        )

    def handover(self, j, block):
        d, t = places()
        slot = self.slot(block)
        return pltpu.make_async_remote_copy(
            src_ref=slot,
            dst_ref=slot,
            send_sem=self.sends.at[8 + j],
            recv_sem=self.recvs.at[7 + j],
            device_id=(d, other_core(t)),
            device_id_type=MESH,
        )

    def hand(self, j):
        self.handover(j, self.place(self.routes[j][2])).start()

    def start(self):
        super().start()
        self.near().start()

    def finish(self):
        super().finish()
        d, t = places()
        far = other_core(t)
        slot = self.slot(far)
        pltpu.make_async_remote_copy(
            src_ref=slot,
            dst_ref=slot,
            send_sem=self.sends.at[15],
            recv_sem=self.recvs.at[14],
            device_id=(d, far),
            device_id_type=MESH,
        ).wait_recv()
        self.near().wait_send()
        for j in range(7):
            self.handover(j, tensor_at(far, self.routes[j][2])).wait_recv()
            self.handover(j, self.place(self.routes[j][2])).wait_send()


class TensorSum:
    STEPS = ((2, 1), (1, 1), (3, 1), (2, 0), (1, 0), (3, 0))
    BLOCKS = STEPS + ((0, 1), (0, 0))

    @staticmethod
    def scratch(columns):
        return [
            pltpu.VMEM((8, 16, columns), BF16),
            pltpu.VMEM((7, 16, columns), BF16),
            pltpu.VMEM((7, 16, columns), BF16),
            DMA((15,)),
            DMA((15,)),
        ]

    def __init__(self, part, near, sent, far, sends, recvs):
        self.part, self.near_, self.sent, self.far = part, near, sent, far
        self.sends, self.recvs = sends, recvs

    def swap(self, j):
        d, t = places()
        k = chip_at(t, self.BLOCKS[j])
        c = lax.rem(t, 2)
        return remote(
            self.part.at[k, 1 - c], self.near_.at[k], self.sends, self.recvs, j, (d, other_core(t))
        )

    def cross(self, j):
        d, t = places()
        hop = (self.STEPS[j][0], 0) if j < 6 else (0, 1)
        return remote(
            self.sent.at[j], self.far.at[j], self.sends, self.recvs, 8 + j, (d, tensor_at(t, hop))
        )

    def pair_sum(self, j):
        d, t = places()
        k = chip_at(t, self.BLOCKS[j])
        c = lax.rem(t, 2)
        return self.part[k, c].astype(F32) + self.near_[k].astype(F32)

    def start(self):
        for j in range(8):
            self.swap(j).start()

    def send(self):
        for j in range(6):
            self.swap(j).wait_recv()
            self.sent[j] = self.pair_sum(j).astype(BF16)
            self.cross(j).start()

    def middle(self):
        self.swap(6).wait_recv()
        total = self.pair_sum(6)
        for j in (1, 2, 0):
            self.cross(j).wait_recv()
            total = total + self.far[j].astype(F32)
        self.sent[6] = total.astype(BF16)
        self.cross(6).start()

    def total(self):
        self.swap(7).wait_recv()
        total = self.pair_sum(7)
        for j in (4, 5, 3, 6):
            self.cross(j).wait_recv()
            total = total + self.far[j].astype(F32)
        return total

    def finish(self):
        for j in range(8):
            self.swap(j).wait_send()
        for j in range(7):
            self.cross(j).wait_send()


class DataSpread:
    scratch = [DMA((8,)), DMA((7,))]

    def __init__(self, src, out, sends, recvs):
        self.src, self.out_, self.sends, self.recvs = src, out, sends, recvs
        self.share = src.shape[1] // 8

    def columns(self, d):
        return pl.ds(pl.multiple_of(d * self.share, self.share), self.share)

    def cross(self, j):
        d, t = places()
        peer = data_at(d, HOPS[j])
        return remote(
            self.src.at[:, self.columns(peer)],
            self.out_.at[d],
            self.sends,
            self.recvs,
            j,
            (peer, t),
        )

    def arrived(self, j):
        d, t = places()
        slot = self.out_.at[data_at(d, back(HOPS[j]))]
        return remote(slot, slot, self.sends, self.recvs, j, (d, other_core(t)))

    def own(self):
        d, t = places()
        return pltpu.make_async_copy(
            self.src.at[:, self.columns(d)], self.out_.at[d], self.sends.at[7]
        )

    def start(self):
        for j in range(7):
            self.cross(j).start()
        self.own().start()

    def finish(self):
        for j in range(7):
            self.arrived(j).wait_recv()
            self.cross(j).wait_send()
        self.own().wait()


class DataExchange:
    scratch = [DMA((15,)), DMA((14,))]

    def __init__(self, src, out, sends, recvs):
        self.src, self.out_, self.sends, self.recvs = src, out, sends, recvs
        self.half = src.shape[0] // 2
        self.share = src.shape[1] // 8

    def rows(self, t):
        return pl.ds(pl.multiple_of(lax.rem(t, 2) * self.half, self.half), self.half)

    def columns(self, d):
        return pl.ds(pl.multiple_of(d * self.share, self.share), self.share)

    def cross(self, j):
        d, t = places()
        peer = data_at(d, HOPS[j])
        return remote(
            self.src.at[self.rows(t), self.columns(peer)],
            self.out_.at[d, self.rows(t)],
            self.sends,
            self.recvs,
            j,
            (peer, t),
        )

    def hand(self, j, t_of):
        d, t = places()
        slot = self.out_.at[data_at(d, back(HOPS[j])), self.rows(t_of)]
        return slot

    def arrived(self, j):
        d, t = places()
        slot = self.hand(j, t)
        return remote(slot, slot, self.sends, self.recvs, j, (d, other_core(t)))

    def handed(self, j):
        d, t = places()
        slot = self.hand(j, t)
        return remote(slot, slot, self.sends, self.recvs, 7 + j, (d, other_core(t)))

    def received(self, j):
        d, t = places()
        slot = self.hand(j, other_core(t))
        return remote(slot, slot, self.sends, self.recvs, 7 + j, (d, other_core(t)))

    def own(self):
        d, t = places()
        return pltpu.make_async_copy(
            self.src.at[:, self.columns(d)], self.out_.at[d], self.sends.at[14]
        )

    def start(self):
        for j in range(7):
            self.cross(j).start()
        self.own().start()

    def finish(self):
        for j in (6, 4, 5, 3, 0, 1, 2):
            self.arrived(j).wait_recv()
            self.handed(j).start()
        for j in range(7):
            self.received(j).wait_recv()
            self.cross(j).wait_send()
            self.handed(j).wait_send()
        self.own().wait()


def taken(refs, *counts):
    out, at = [], 0
    for count in counts:
        out.append(refs[at : at + count])
        at += count
    return out


def comm_call(kernel, name, number, in_specs, out_specs, out_shape, scratch, args):
    return pl.pallas_call(
        kernel,
        name=name,
        in_specs=in_specs,
        out_specs=out_specs,
        out_shape=out_shape,
        scratch_shapes=scratch,
        compiler_params=pltpu.CompilerParams(
            collective_id=number, has_side_effects=True, vmem_limit_bytes=40 * 2**20
        ),
    )(*args)


def shape(dims, dtype):
    return jax.ShapeDtypeStruct(dims, dtype)


def slot_of(ref):
    return lambda block: ref.at[block]


def columns_of(ref):
    width = ref.shape[1] // 8
    return lambda block: ref.at[:, pl.ds(pl.multiple_of(block * width, width), width)]


def mean_of(values):
    return jnp.sum(values, axis=-1, keepdims=True) * (1.0 / values.shape[-1])


def strip(which, core):
    return pl.ds(pl.multiple_of(which * 128 + core * 64, 64), 64)


class CoreShare:
    scratch = [DMA((2,)), DMA((2,))]

    def __init__(self, sources, slot, sends, recvs):
        self.sources, self.slot, self.sends, self.recvs = sources, slot, sends, recvs

    def copy(self, j, core):
        d, t = places()
        slot = self.slot(j, core)
        src = slot if self.sources is None else self.sources[j]
        return remote(src, slot, self.sends, self.recvs, j, (d, other_core(t)))

    def start(self):
        d, t = places()
        for j in range(2):
            self.copy(j, lax.rem(t, 2)).start()

    def finish(self):
        d, t = places()
        for j in range(2):
            self.copy(j, 1 - lax.rem(t, 2)).wait_recv()
            self.copy(j, lax.rem(t, 2)).wait_send()


class Probes:
    COUNT = 4
    scratch = DataGather.scratch * 4 + CoreShare.scratch

    def __init__(self, layer, probes, gathered, sems):
        q, k, v, o = probes
        gq, gkv, go = gathered
        d, t = places()
        core = lax.rem(t, 2)
        width = k.shape[2]

        def part(which):
            return lambda block: gkv.at[
                strip(which, core), pl.ds(pl.multiple_of(block * width, width), width)
            ]

        self.jobs = [
            DataGather(k.at[layer], part(0), *sems[0:2]),
            DataGather(v.at[layer], part(1), *sems[2:4]),
            DataGather(q.at[layer], slot_of(gq), *sems[4:6]),
            DataGather(o.at[layer], columns_of(go), *sems[6:8]),
        ]
        self.share = CoreShare(None, lambda j, c: gkv.at[strip(j, c)], *sems[8:10])

    @staticmethod
    def shapes(probes):
        q, k, v, o = probes
        return [
            shape((8,) + q.shape[1:], BF16),
            shape((4 * k.shape[1], 8 * k.shape[2]), BF16),
            shape((o.shape[1], 8 * o.shape[2]), BF16),
        ]

    def start(self):
        for job in self.jobs:
            job.start()

    def relay(self):
        for job in self.jobs:
            job.relay()

    def finish(self):
        for job in self.jobs[:2]:
            job.finish()
        self.share.start()
        for job in self.jobs[2:]:
            job.finish()
        self.share.finish()


def first_kernel(*refs):
    (
        (tokens, gains, q, k, v, o, kw, vw),
        (h_all, hs, gq, gkv, go, kv),
        (h_low, mini),
        row_sems,
        spread_sems,
        slice_sems,
        share_sems,
        own_sems,
        probe_sems,
    ) = taken(refs, 8, 6, 2, 2, 2, 2, 2, 1, 10)
    d, t = places()
    core = lax.rem(t, 2)
    wide = tokens[...].astype(F32)
    inverse = lax.rsqrt(mean_of(wide * wide) + EPS)
    h_low[...] = (wide * inverse * gains[0:1]).astype(BF16)
    enter(True, True)
    spread = DataSpread(h_low, mini, *spread_sems)
    rows = TensorGather(h_low, slot_of(h_all), *row_sems)
    slices = TensorGather(mini, lambda block: hs.at[:, block], *slice_sems)
    share = CoreShare((kw, vw), lambda j, c: kv.at[:, strip(j, c)], *share_sems)
    probes = Probes(0, (q, k, v, o), (gq, gkv, go), probe_sems)
    own = [
        pltpu.make_async_copy(src, kv.at[:, strip(j, core)], own_sems[0].at[j])
        for j, src in enumerate((kw, vw))
    ]
    spread.start()
    rows.start()
    probes.start()
    rows.relay()
    spread.finish()
    slices.start()
    share.start()
    for copy in own:
        copy.start()
    rows.finish()
    probes.relay()
    slices.relay()
    slices.finish()
    share.finish()
    for copy in own:
        copy.wait()
    probes.finish()


def first(tokens, gains, probes, kw, vw):
    rows, width = tokens.shape
    return comm_call(
        first_kernel,
        "first",
        1,
        [VMEM, VMEM] + [HBM] * 6,
        [VMEM] + [HBM] * 5,
        [shape((16, rows, width), BF16), shape((8, 16, rows, width // 8), BF16)]
        + Probes.shapes(probes)
        + [shape((2, 4 * kw.shape[1], width), BF16)],
        [pltpu.VMEM((rows, width), BF16), pltpu.VMEM((8, rows, width // 8), BF16)]
        + TensorGather.scratch
        + DataSpread.scratch
        + TensorGather.scratch
        + CoreShare.scratch
        + [DMA((2,))]
        + Probes.scratch,
        (tokens, gains) + probes + (kw, vw),
    )


def between_kernel(*refs):
    (
        (primal, moved, tokens, gains, q, k, v, o),
        (x_out, t_out, h_all, th_all, gq, gkv, go),
        (h_low, th_low),
        sum_a,
        sum_b,
        gather_a,
        gather_b,
        sems,
    ) = taken(refs, 8, 7, 2, 5, 5, 2, 2, 10)
    gain = gains[1:2]
    enter(True, True)
    sums = [TensorSum(primal, *sum_a), TensorSum(moved, *sum_b)]
    probes = Probes(1, (q, k, v, o), (gq, gkv, go), sems)
    for one in sums:
        one.start()
    for one in sums:
        one.send()
    probes.start()
    for one in sums:
        one.middle()
    stream = (tokens[...].astype(F32) + sums[0].total()).astype(BF16)
    x_out[...] = stream
    wide = stream.astype(F32)
    inverse = lax.rsqrt(mean_of(wide * wide) + EPS)
    h_low[...] = (wide * inverse * gain).astype(BF16)
    rows_a = TensorGather(h_low, slot_of(h_all), *gather_a)
    rows_a.start()
    tangent = sums[1].total()
    t_out[...] = tangent
    shift = mean_of(wide * tangent)
    th_low[...] = (gain * (tangent * inverse - wide * inverse * inverse * inverse * shift)).astype(
        BF16
    )
    rows_b = TensorGather(th_low, slot_of(th_all), *gather_b)
    rows_b.start()
    rows_a.relay()
    probes.relay()
    rows_b.relay()
    for one in sums:
        one.finish()
    rows_a.finish()
    rows_b.finish()
    probes.finish()


def between(primal, moved, tokens, gains, probes):
    rows, width = tokens.shape
    return comm_call(
        between_kernel,
        "between",
        2,
        [VMEM] * 4 + [HBM] * 4,
        [VMEM] * 4 + [HBM] * 3,
        [
            shape((rows, width), BF16),
            shape((rows, width), F32),
            shape((16, rows, width), BF16),
            shape((16, rows, width), BF16),
        ]
        + Probes.shapes(probes),
        [pltpu.VMEM((rows, width), BF16)] * 2
        + TensorSum.scratch(width) * 2
        + TensorGather.scratch * 2
        + Probes.scratch,
        (primal, moved, tokens, gains) + probes,
    )


def turn_kernel(*refs):
    (
        (lengths, moved, t_one, a_zero, a_one, h_one),
        (c_out, cb_all, ga_zero, ga_one, hs_one),
        (c_low,),
        sum_a,
        gather_a,
        sems,
    ) = taken(refs, 6, 5, 1, 5, 2, 6)
    d, t = places()
    enter(True, True)
    total = TensorSum(moved, *sum_a)
    jobs = [
        DataGather(a_zero, slot_of(ga_zero), *sems[0:2]),
        DataGather(a_one, slot_of(ga_one), *sems[2:4]),
    ]
    swap = DataExchange(h_one, hs_one, *sems[4:6])
    total.start()
    total.send()
    for job in jobs:
        job.start()
    total.middle()
    swap.start()
    position = t * t_one.shape[0] + lax.broadcasted_iota(jnp.int32, t_one.shape, 0)
    mask = jnp.where(position < lengths[d], 1.0, 0.0)
    cotangent = mask * (t_one[...] + total.total())
    c_out[...] = cotangent
    c_low[...] = cotangent.astype(BF16)
    rows = TensorGather(c_low, slot_of(cb_all), *gather_a)
    rows.start()
    for job in jobs:
        job.relay()
    rows.relay()
    total.finish()
    rows.finish()
    swap.finish()
    for job in jobs:
        job.finish()


SMEM = pl.BlockSpec(memory_space=pltpu.SMEM)


def turn(lengths, moved, t_one, a_zero, a_one, h_one):
    rows, width = t_one.shape
    return comm_call(
        turn_kernel,
        "turn",
        3,
        [SMEM] + [VMEM] * 2 + [HBM] * 3,
        [VMEM] * 2 + [HBM] * 3,
        [
            shape((rows, width), F32),
            shape((16, rows, width), BF16),
            shape((8,) + a_zero.shape, BF16),
            shape((8,) + a_one.shape, BF16),
            shape((8, h_one.shape[0], h_one.shape[1] // 8), BF16),
        ],
        [pltpu.VMEM((rows, width), BF16)]
        + TensorSum.scratch(width)
        + TensorGather.scratch
        + DataGather.scratch * 2
        + DataExchange.scratch,
        (lengths, moved, t_one, a_zero, a_one, h_one),
    )


class Cotangents:
    def __init__(self, gq, gkv, gathered, came, merged, sems):
        self.gkv, self.came, self.merged = gkv, came, merged
        width = gq.shape[1]
        self.jobs = [
            DataGather(gq, lambda block: gathered.at[block, :, 0:width], *sems[0:2]),
            DataGather(
                merged,
                lambda block: gathered.at[block, :, width : width + merged.shape[1]],
                *sems[2:4],
            ),
        ]
        self.sends, self.recvs = sems[4:6]

    @staticmethod
    def scratch(gkv):
        return (
            [pltpu.VMEM(gkv.shape[1:], BF16)] * 2
            + DataGather.scratch * 2
            + [DMA((1,)), DMA((1,))]
        )

    def swap(self):
        d, t = places()
        return remote(
            self.gkv.at[1 - lax.rem(t, 2)],
            self.came,
            self.sends,
            self.recvs,
            0,
            (d, other_core(t)),
        )

    def start(self):
        d, t = places()
        self.swap().start()
        self.jobs[0].start()
        self.swap().wait()
        mine = self.gkv[lax.rem(t, 2)].astype(F32) + self.came[...].astype(F32)
        self.merged[...] = mine.astype(BF16)
        self.jobs[1].start()

    def relay(self):
        for job in self.jobs:
            job.relay()

    def finish(self):
        for job in self.jobs:
            job.finish()


def lower_kernel(*refs):
    (
        (part, c_two, x_one, gains, gkv, gq, cb_one),
        (cb_all, gg, cbs, mini),
        (c_low,),
        sum_a,
        gather_a,
        (came, merged),
        sems,
        swap_sems,
        spread_sems,
    ) = taken(refs, 7, 4, 1, 5, 2, 2, 6, 2, 2)
    enter(True, True)
    total = TensorSum(part, *sum_a)
    jobs = Cotangents(gq, gkv, gg, came, merged, sems)
    swap = DataExchange(cb_one, cbs, *swap_sems)
    total.start()
    total.send()
    jobs.start()
    total.middle()
    swap.start()
    scaled = total.total() * gains[1:2]
    wide = x_one[...].astype(F32)
    inverse = lax.rsqrt(mean_of(wide * wide) + EPS)
    shift = mean_of(wide * scaled)
    cotangent = c_two[...] + inverse * (scaled - wide * inverse * inverse * shift)
    c_low[...] = cotangent.astype(BF16)
    rows = TensorGather(c_low, slot_of(cb_all), *gather_a)
    spread = DataSpread(c_low, mini, *spread_sems)
    rows.start()
    spread.start()
    jobs.relay()
    rows.relay()
    total.finish()
    rows.finish()
    swap.finish()
    spread.finish()
    jobs.finish()


def lower(part, c_two, x_one, gains, gkv, gq, cb_one):
    rows, width = c_two.shape
    return comm_call(
        lower_kernel,
        "lower",
        4,
        [VMEM] * 5 + [HBM] * 2,
        [VMEM] + [HBM] * 3,
        [
            shape((16, rows, width), BF16),
            shape((8, gq.shape[0], gq.shape[1] + gkv.shape[2]), BF16),
            shape((8, cb_one.shape[0], width // 8), BF16),
            shape((8, rows, width // 8), BF16),
        ],
        [pltpu.VMEM((rows, width), BF16)]
        + TensorSum.scratch(width)
        + TensorGather.scratch
        + Cotangents.scratch(gkv)
        + DataExchange.scratch
        + DataSpread.scratch,
        (part, c_two, x_one, gains, gkv, gq, cb_one),
    )


def last_kernel(*refs):
    (gkv, mini, gq), (gg, cbs), (came, merged), sems, slice_sems = taken(refs, 3, 2, 2, 6, 2)
    enter(True, True)
    slices = TensorGather(mini, lambda block: cbs.at[:, block], *slice_sems)
    jobs = Cotangents(gq, gkv, gg, came, merged, sems)
    slices.start()
    jobs.start()
    slices.relay()
    jobs.relay()
    slices.finish()
    jobs.finish()


def last(gkv, mini, gq):
    return comm_call(
        last_kernel,
        "last",
        5,
        [VMEM] * 2 + [HBM],
        [HBM] * 2,
        [
            shape((8, gq.shape[0], gq.shape[1] + gkv.shape[2]), BF16),
            shape((8, 16) + mini.shape[1:], BF16),
        ],
        Cotangents.scratch(gkv) + TensorGather.scratch,
        (gkv, mini, gq),
    )


def contract(left_side, right_side, left_dim, right_dim):
    return lax.dot_general(
        left_side,
        right_side,
        (((left_dim,), (right_dim,)), ((), ())),
        preferred_element_type=F32,
    )


def turned(values, cosine, sine):
    return values * cosine + pltpu.roll(values, values.shape[1] // 2, 1) * sine


def attention_weights(q, k, length):
    size = q.shape[0]
    row = lax.broadcasted_iota(jnp.int32, (size, size), 0)
    column = lax.broadcasted_iota(jnp.int32, (size, size), 1)
    allowed = (column <= row) & (column < length)
    scores = contract(q, k, 1, 1) * (1.0 / math.sqrt(q.shape[1]))
    powers = jnp.where(allowed, jnp.exp(scores), 0.0)
    return powers / jnp.sum(powers, axis=-1, keepdims=True)


def forward_kernel(steps, second, *refs):
    more = 1 if second else 0
    (
        (lengths, cosine, sine, wq, kv, pq, pkv, wo, po, h),
        th,
        (q_out, k_out, v_out, a_out, moved),
        primal,
        (q_sum, tq_sum, kv_sum, tkv_sum, ta_low),
    ) = taken(refs, 10, more, 5, 1 - more, 5)
    i = pl.program_id(0)
    sums = (q_sum, tq_sum, kv_sum, tkv_sum)

    @pl.when(i == 0)
    def _():
        for one in sums:
            one[...] = jnp.zeros_like(one)

    @pl.when(i < steps)
    def _():
        normed = h[...]
        q_sum[...] += contract(normed, wq[...], 1, 0)
        kv_sum[...] += contract(normed, kv[...], 1, 1)
        tq = contract(normed, pq[...], 1, 0)
        tkv = contract(normed, pkv[...], 1, 1)
        if second:
            tq = tq + contract(th[0][...], wq[...], 1, 0)
            tkv = tkv + contract(th[0][...], kv[...], 1, 1)
        tq_sum[...] += tq
        tkv_sum[...] += tkv

    @pl.when(i == steps - 1)
    def _():
        length = lengths[lax.axis_index("dp")]
        scaling = 1.0 / math.sqrt(HD)
        cos, sin = cosine[...], sine[...]
        k = turned(kv_sum[:, 0:HD], cos, sin).astype(BF16)
        v = kv_sum[:, HD:].astype(BF16)
        tk = turned(tkv_sum[:, 0:HD], cos, sin).astype(BF16)
        tv = tkv_sum[:, HD:].astype(BF16)
        k_out[...] = k
        v_out[...] = v
        for at in range(0, q_sum.shape[1], HD):
            head = slice(at, at + HD)
            q = turned(q_sum[:, head], cos, sin).astype(BF16)
            tq = turned(tq_sum[:, head], cos, sin).astype(BF16)
            q_out[:, head] = q
            weights = attention_weights(q, k, length)
            low = weights.astype(BF16)
            a_out[:, head] = contract(low, v, 1, 0).astype(BF16)
            scores = (contract(tq, k, 1, 1) + contract(q, tk, 1, 1)) * scaling
            change = weights * (scores - jnp.sum(weights * scores, axis=-1, keepdims=True))
            ta = contract(change.astype(BF16), v, 1, 0) + contract(low, tv, 1, 0)
            ta_low[:, head] = ta.astype(BF16)

    @pl.when(i >= steps)
    def _():
        moved[...] = (
            contract(ta_low[...], wo[...], 1, 0) + contract(a_out[...], po[...], 1, 0)
        ).astype(BF16)
        if not second:
            primal[0][...] = contract(a_out[...], wo[...], 1, 0).astype(BF16)


def whole(dims):
    return pl.BlockSpec(dims, lambda i: (0,) * len(dims))


TILE = 1024


def forward(layer, lengths, tables, wq, kv, pq, pkv, wo, po, h, th=None):
    rows, width = h.shape
    columns = wq.shape[2]
    steps = width // TILE
    second = th is not None

    def now(i):
        return jnp.minimum(i, steps - 1)

    def later(i):
        return jnp.maximum(i - steps, 0)

    into = pl.BlockSpec((rows, TILE), lambda i: (0, now(i)))
    out = pl.BlockSpec((rows, TILE), lambda i: (0, later(i)))
    in_specs = [
        SMEM,
        whole((rows, HD)),
        whole((rows, HD)),
        pl.BlockSpec((None, TILE, columns), lambda i: (layer, now(i), 0)),
        pl.BlockSpec((None, 2 * HD, TILE), lambda i: (layer, 0, now(i))),
        pl.BlockSpec((TILE, columns), lambda i: (now(i), 0)),
        pl.BlockSpec((2 * HD, TILE), lambda i: (0, now(i))),
        pl.BlockSpec((None, columns, TILE), lambda i: (layer, 0, later(i))),
        pl.BlockSpec((columns, TILE), lambda i: (0, later(i))),
        into,
    ] + [into] * second
    out_specs = [
        whole((rows, columns)),
        whole((rows, HD)),
        whole((rows, HD)),
        whole((rows, columns)),
        out,
    ] + [out] * (not second)
    out_shape = [
        shape((rows, columns), BF16),
        shape((rows, HD), BF16),
        shape((rows, HD), BF16),
        shape((rows, columns), BF16),
        shape((rows, width), BF16),
    ] + [shape((rows, width), BF16)] * (not second)
    args = (lengths,) + tables + (wq, kv, pq, pkv, wo, po, h) + ((th,) if second else ())
    return pl.pallas_call(
        functools.partial(forward_kernel, steps, second),
        name=f"forward_{layer}",
        grid=(2 * steps,),
        in_specs=in_specs,
        out_specs=out_specs,
        out_shape=out_shape,
        scratch_shapes=[
            pltpu.VMEM((rows, columns), F32),
            pltpu.VMEM((rows, columns), F32),
            pltpu.VMEM((rows, 2 * HD), F32),
            pltpu.VMEM((rows, 2 * HD), F32),
            pltpu.VMEM((rows, columns), BF16),
        ],
        compiler_params=pltpu.CompilerParams(vmem_limit_bytes=40 * 2**20),
    )(*args)


def backward_kernel(steps, lowest, *refs):
    more = 0 if lowest else 1
    (
        (lengths, cosine, sine, q_in, k_in, v_in, cb, wo),
        weights_in,
        (gq_out, gkv_out),
        part,
        (ga_sum, gkv_low),
    ) = taken(refs, 8, 2 * more, 2, more, 2)
    i = pl.program_id(0)

    @pl.when(i == 0)
    def _():
        ga_sum[...] = jnp.zeros_like(ga_sum)

    @pl.when(i < steps)
    def _():
        ga_sum[...] += contract(cb[...], wo[...], 1, 1)

    @pl.when(i == steps - 1)
    def _():
        length = lengths[lax.axis_index("dp")]
        scaling = 1.0 / math.sqrt(HD)
        cos, sin = cosine[...], -sine[...]
        k, v = k_in[...], v_in[...]
        gk, gv = None, None
        for at in range(0, ga_sum.shape[1], HD):
            head = slice(at, at + HD)
            q = q_in[:, head]
            ga = ga_sum[:, head].astype(BF16)
            weights = attention_weights(q, k, length)
            grads = contract(ga, v, 1, 1)
            value = contract(weights.astype(BF16), ga, 0, 0)
            scores = (
                weights * (grads - jnp.sum(weights * grads, axis=-1, keepdims=True)) * scaling
            ).astype(BF16)
            gq_out[:, head] = turned(contract(scores, k, 1, 0), cos, sin).astype(BF16)
            key = contract(scores, q, 0, 0)
            gk = key if gk is None else gk + key
            gv = value if gv is None else gv + value
        gk = turned(gk, cos, sin).astype(BF16)
        gv = gv.astype(BF16)
        half = HD // 2
        gkv_low[:, 0:HD] = gk
        gkv_low[:, HD:] = gv
        gkv_out[0] = jnp.concatenate([gk[:, 0:half], gv[:, 0:half]], axis=-1)
        gkv_out[1] = jnp.concatenate([gk[:, half:], gv[:, half:]], axis=-1)

    if not lowest:

        @pl.when(i >= steps)
        def _():
            part[0][...] = (
                contract(gq_out[...], weights_in[0][...], 1, 1)
                + contract(gkv_low[...], weights_in[1][...], 1, 0)
            ).astype(BF16)


def backward(layer, lengths, tables, q, k, v, cb, wo, wq, kv):
    rows, width = cb.shape
    columns = wo.shape[1]
    steps = width // TILE
    lowest = layer == 0

    def now(i):
        return jnp.minimum(i, steps - 1)

    def later(i):
        return jnp.maximum(i - steps, 0)

    in_specs = [
        SMEM,
        whole((rows, HD)),
        whole((rows, HD)),
        whole((rows, columns)),
        whole((rows, HD)),
        whole((rows, HD)),
        pl.BlockSpec((rows, TILE), lambda i: (0, now(i))),
        pl.BlockSpec((None, columns, TILE), lambda i: (layer, 0, now(i))),
    ]
    out_specs = [whole((rows, columns)), whole((2, rows, HD))]
    out_shape = [shape((rows, columns), BF16), shape((2, rows, HD), BF16)]
    args = (lengths,) + tables + (q, k, v, cb, wo)
    if not lowest:
        in_specs += [
            pl.BlockSpec((None, TILE, columns), lambda i: (layer, later(i), 0)),
            pl.BlockSpec((None, 2 * HD, TILE), lambda i: (layer, 0, later(i))),
        ]
        out_specs.append(pl.BlockSpec((rows, TILE), lambda i: (0, later(i))))
        out_shape.append(shape((rows, width), BF16))
        args += (wq, kv)
    return pl.pallas_call(
        functools.partial(backward_kernel, steps, lowest),
        name=f"backward_{layer}",
        grid=(steps if lowest else 2 * steps,),
        in_specs=in_specs,
        out_specs=out_specs,
        out_shape=out_shape,
        scratch_shapes=[
            pltpu.VMEM((rows, columns), F32),
            pltpu.VMEM((rows, 2 * HD), BF16),
        ],
        compiler_params=pltpu.CompilerParams(vmem_limit_bytes=40 * 2**20),
    )(*args)


def products_kernel(*refs):
    sides, (q_out, k_out, v_out, o_out) = taken(refs, 8, 4)
    i = pl.program_id(0)
    columns, half = q_out.shape[2], k_out.shape[1]
    for layer in range(2):
        hs, gg, ga, cs = [ref[...].reshape(-1, ref.shape[-1]) for ref in sides[4 * layer :][:4]]
        q = contract(hs, gg[:, 0:columns], 0, 0)
        kv = contract(gg[:, columns:], hs, 0, 0)
        o = contract(ga, cs, 0, 0)

        @pl.when(i == 0)
        def _():
            q_out[layer] = q
            k_out[layer] = kv[0:half]
            v_out[layer] = kv[half:]
            o_out[layer] = o

        @pl.when(i > 0)
        def _():
            q_out[layer] += q
            k_out[layer] += kv[0:half]
            v_out[layer] += kv[half:]
            o_out[layer] += o


def products(*sides):
    chunk = 2
    columns, share = sides[2].shape[2], sides[0].shape[2]
    half = (sides[1].shape[2] - columns) // 2
    out_shape = [
        shape((2, share, columns), F32),
        shape((2, half, share), F32),
        shape((2, half, share), F32),
        shape((2, columns, share), F32),
    ]
    return pl.pallas_call(
        products_kernel,
        name="products",
        grid=(8 // chunk,),
        in_specs=[
            pl.BlockSpec((chunk,) + side.shape[1:], lambda i: (i, 0, 0)) for side in sides
        ],
        out_specs=[whole(out.shape) for out in out_shape],
        out_shape=out_shape,
        compiler_params=pltpu.CompilerParams(vmem_limit_bytes=40 * 2**20),
    )(*sides)


def rope_tables():
    angles = np.arange(LEN)[:, None] * THETA ** (-2.0 * np.arange(HD // 2) / HD)[None, :]
    cosine, sine = np.cos(angles), np.sin(angles)
    return (
        jnp.asarray(np.concatenate([cosine, cosine], axis=1), F32),
        jnp.asarray(np.concatenate([-sine, sine], axis=1), F32),
    )


def body(
    tokens,
    lengths,
    gains,
    query_weight,
    key_weight,
    value_weight,
    out_weight,
    query_probe,
    key_probe,
    value_probe,
    out_probe,
):
    rows, width = tokens.shape
    tables = rope_tables()

    def turned_over(array):
        return jnp.swapaxes(array, 1, 2)

    def by_owner(part):
        return part.reshape(8, 2, rows, width)

    def all_rows(blocks):
        return blocks.reshape(-1, blocks.shape[-1])

    def by_batch(blocks):
        return blocks.reshape(blocks.shape[0], -1, blocks.shape[-1])

    probes = (query_probe, turned_over(key_probe), turned_over(value_probe), out_probe)
    h_zero, hs_zero, pq, pkv, po, kv = first(
        tokens, gains, probes, turned_over(key_weight), turned_over(value_weight)
    )
    q0, k0, v0, a_zero, moved, primal = forward(
        0, lengths, tables, query_weight, kv, all_rows(pq), pkv, out_weight, po, all_rows(h_zero)
    )
    x_one, t_one, h_one, th_one, pq, pkv, po = between(
        by_owner(primal), by_owner(moved), tokens, gains, probes
    )
    h_one = all_rows(h_one)
    q1, k1, v1, a_one, moved = forward(
        1,
        lengths,
        tables,
        query_weight,
        kv,
        all_rows(pq),
        pkv,
        out_weight,
        po,
        h_one,
        all_rows(th_one),
    )
    c_two, cb_one, ga_zero, ga_one, hs_one = turn(
        lengths, by_owner(moved), t_one, a_zero, a_one, h_one
    )
    cb_one = all_rows(cb_one)
    gq, gkv, part = backward(
        1, lengths, tables, q1, k1, v1, cb_one, out_weight, query_weight, kv
    )
    cb_zero, gg_one, cs_one, mini = lower(
        by_owner(part), c_two, x_one, gains, gkv, gq, cb_one
    )
    gq, gkv = backward(
        0, lengths, tables, q0, k0, v0, all_rows(cb_zero), out_weight, query_weight, kv
    )
    gg_zero, cs_zero = last(gkv, mini, gq)
    q, k, v, o = products(
        by_batch(hs_zero), gg_zero, ga_zero, by_batch(cs_zero), hs_one, gg_one, ga_one, cs_one
    )
    return (q, turned_over(k), turned_over(v), o)


def solution(mesh):
    placed = (
        P(("dp", "tensor"), None),
        P(),
        P(),
        P(None, None, "tensor"),
        P(None, None, "tensor"),
        P(None, None, "tensor"),
        P(None, "tensor", None),
        P(None, "dp", "tensor"),
        P(None, "dp", "tensor"),
        P(None, "dp", "tensor"),
        P(None, "tensor", "dp"),
    )
    return jax.shard_map(
        body,
        mesh=mesh,
        in_specs=placed,
        out_specs=(
            P(None, "dp", "tensor"),
            P(None, "dp", "tensor"),
            P(None, "dp", "tensor"),
            P(None, "tensor", "dp"),
        ),
        check_vma=False,
    )
```

```python
import functools
import math

import jax
import jax.numpy as jnp
import numpy as np
from jax import lax
from jax.experimental import pallas as pl
from jax.experimental.pallas import tpu as pltpu
from jax.sharding import PartitionSpec as P

HD = 128
LEN = 256
EPS = 1e-05
THETA = 500000.0

MESH = pl.DeviceIdType.MESH
F32 = jnp.float32
BF16 = jnp.bfloat16
VMEM = pl.BlockSpec(memory_space=pltpu.VMEM)
ANY = pl.BlockSpec(memory_space=pl.ANY)
HBM = pl.BlockSpec(memory_space=pltpu.HBM)
DMA = pltpu.SemaphoreType.DMA

HOPS = ((1, 1), (3, 1), (2, 1), (2, 0), (1, 0), (3, 0), (0, 1))
NEAR = HOPS[3:]


def back(hop):
    return ((4 - hop[0]) % 4, hop[1])


def data_at(d, hop):
    ring, pair = lax.div(d, 2), lax.rem(d, 2)
    return lax.rem(ring + hop[0], 4) * 2 + lax.rem(pair + hop[1], 2)


def chip_at(t, hop):
    return data_at(lax.div(t, 2), hop)


def tensor_at(t, hop):
    return chip_at(t, hop) * 2 + lax.rem(t, 2)


def other_core(t):
    return t + 1 - 2 * lax.rem(t, 2)


def places():
    return lax.axis_index("dp"), lax.axis_index("tensor")


def remote(src, dst, sends, recvs, j, device):
    return pltpu.make_async_remote_copy(
        src_ref=src,
        dst_ref=dst,
        send_sem=sends.at[j],
        recv_sem=recvs.at[j],
        device_id=device,
        device_id_type=MESH,
    )


def enter(data_hops):
    d, t = places()
    barrier = pltpu.get_barrier_semaphore()
    peers = [(d, other_core(t))]
    peers += [(d, tensor_at(t, hop)) for hop in NEAR]
    peers += [(data_at(d, hop), t) for hop in data_hops]
    for peer in peers:
        pl.semaphore_signal(barrier, inc=1, device_id=peer, device_id_type=MESH)
    pl.semaphore_wait(barrier, len(peers))


def half_of(ref, half):
    if half is None:
        return ref
    rows = ref.shape[0] // 2
    return ref.at[pl.ds(half * rows, rows)]


class RingGather:
    ROUTES = ()
    FIRST = 0

    def __init__(self, src, slot, sends, recvs):
        self.src, self.slot, self.sends, self.recvs = src, slot, sends, recvs

    def out(self, j):
        hop, block, unused, half = self.ROUTES[j]
        slot = half_of(self.slot(self.place(block)), half)
        src = self.src if j < self.FIRST else slot
        return remote(src, slot, self.sends, self.recvs, j, self.device(hop))

    def into(self, j):
        slot = half_of(self.slot(self.place(self.ROUTES[j][2])), self.ROUTES[j][3])
        return remote(slot, slot, self.sends, self.recvs, j, self.device((0, 1)))

    def own(self):
        n = len(self.ROUTES)
        return pltpu.make_async_copy(self.src, self.slot(self.place((0, 0))), self.sends.at[n])

    def start(self):
        for j in range(self.FIRST):
            self.out(j).start()
        self.own().start()

    def sent(self):
        for j in range(len(self.ROUTES)):
            self.out(j).wait_send()
        self.own().wait()


class DataGather(RingGather):
    scratch = [DMA((8,)), DMA((7,))]
    FIRST = 4
    ROUTES = (
        ((0, 1), (0, 0), (0, 1), None),
        ((1, 0), (0, 0), (3, 0), None),
        ((3, 0), (0, 0), (1, 0), None),
        ((2, 0), (0, 0), (2, 0), None),
        ((1, 0), (0, 1), (3, 1), None),
        ((3, 0), (0, 1), (1, 1), None),
        ((0, 1), (2, 0), (2, 1), None),
    )

    def place(self, hop):
        d, t = places()
        return data_at(d, hop)

    def device(self, hop):
        d, t = places()
        return (data_at(d, hop), t)

    def relay(self):
        self.into(0).wait_recv()
        self.out(4).start()
        self.out(5).start()

    def pass_on(self):
        self.into(3).wait_recv()
        self.out(6).start()

    def finish(self):
        for j in (1, 2, 4, 5, 6):
            self.into(j).wait_recv()
        self.sent()


class LargeGather(DataGather):
    scratch = [DMA((12,)), DMA((11,))]
    FIRST = 3
    ROUTES = (
        ((0, 1), (0, 0), (0, 1), None),
        ((1, 0), (0, 0), (3, 0), None),
        ((3, 0), (0, 0), (1, 0), None),
        ((1, 0), (0, 1), (3, 1), 0),
        ((3, 0), (0, 1), (1, 1), 1),
        ((1, 0), (3, 0), (2, 0), 0),
        ((0, 1), (3, 0), (3, 1), 1),
        ((3, 0), (1, 0), (2, 0), 1),
        ((0, 1), (1, 0), (1, 1), 0),
        ((1, 0), (3, 1), (2, 1), 0),
        ((3, 0), (1, 1), (2, 1), 1),
    )

    def relay(self):
        for j in range(3):
            self.into(j).wait_recv()
            self.out(3 + 2 * j).start()
            self.out(4 + 2 * j).start()

    def pass_on(self):
        for j in (3, 4):
            self.into(j).wait_recv()
            self.out(6 + j).start()

    def finish(self):
        for j in range(5, 11):
            self.into(j).wait_recv()
        self.sent()


class TensorGather(RingGather):
    scratch = [DMA((16,)), DMA((15,))]
    FIRST = 4
    ROUTES = (
        ((0, 1), (0, 0), (0, 1), None),
        ((1, 0), (0, 0), (3, 0), None),
        ((3, 0), (0, 0), (1, 0), None),
        ((2, 0), (0, 0), (2, 0), None),
        ((1, 0), (0, 1), (3, 1), None),
        ((3, 0), (0, 1), (1, 1), None),
        ((2, 0), (0, 1), (2, 1), None),
    )

    def place(self, hop):
        d, t = places()
        return tensor_at(t, hop)

    def device(self, hop):
        d, t = places()
        return (d, tensor_at(t, hop))

    def handover(self, j, src, block):
        d, t = places()
        return pltpu.make_async_remote_copy(
            src_ref=src,
            dst_ref=self.slot(block),
            send_sem=self.sends.at[8 + j],
            recv_sem=self.recvs.at[7 + j],
            device_id=(d, other_core(t)),
            device_id_type=MESH,
        )

    def hand(self, j):
        block = self.place(self.ROUTES[j][2])
        return self.handover(j, self.slot(block), block)

    def near(self):
        return self.handover(7, self.src, self.place((0, 0)))

    def start(self):
        super().start()
        self.near().start()

    def relay(self):
        self.into(0).wait_recv()
        for j in range(4, 7):
            self.out(j).start()
        self.hand(0).start()

    def finish(self):
        for j in range(1, 7):
            self.into(j).wait_recv()
            self.hand(j).start()
        self.sent()
        d, t = places()
        far = other_core(t)
        self.handover(7, self.slot(far), far).wait_recv()
        self.near().wait_send()
        for j in range(7):
            block = tensor_at(far, self.ROUTES[j][2])
            self.handover(j, self.slot(block), block).wait_recv()
            self.hand(j).wait_send()


class TensorSum:
    STEPS = ((2, 1), (1, 1), (3, 1), (2, 0), (1, 0), (3, 0))
    BLOCKS = STEPS + ((0, 1), (0, 0))

    @staticmethod
    def scratch(columns):
        return [
            pltpu.VMEM((8, 8, columns), BF16),
            pltpu.VMEM((7, 8, columns), BF16),
            pltpu.VMEM((7, 8, columns), BF16),
            DMA((15,)),
            DMA((15,)),
        ]

    def __init__(self, rows, part, near, sent, far, sends, recvs):
        self.rows = rows
        self.part, self.near_, self.sent, self.far = part, near, sent, far
        self.sends, self.recvs = sends, recvs

    def swap(self, j):
        d, t = places()
        k = chip_at(t, self.BLOCKS[j])
        c = lax.rem(t, 2)
        return remote(
            self.part.at[k, 1 - c, self.rows], self.near_.at[k], self.sends, self.recvs, j, (d, other_core(t))
        )

    def cross(self, j):
        d, t = places()
        hop = (self.STEPS[j][0], 0) if j < 6 else (0, 1)
        return remote(
            self.sent.at[j], self.far.at[j], self.sends, self.recvs, 8 + j, (d, tensor_at(t, hop))
        )

    def pair_sum(self, j):
        d, t = places()
        k = chip_at(t, self.BLOCKS[j])
        c = lax.rem(t, 2)
        return self.part[k, c, self.rows].astype(F32) + self.near_[k].astype(F32)

    def start(self):
        for j in range(8):
            self.swap(j).start()

    def send(self):
        for j in range(6):
            self.swap(j).wait_recv()
            self.sent[j] = self.pair_sum(j).astype(BF16)
            self.cross(j).start()

    def middle(self):
        self.swap(6).wait_recv()
        total = self.pair_sum(6)
        for j in (1, 2, 0):
            self.cross(j).wait_recv()
            total = total + self.far[j].astype(F32)
        self.sent[6] = total.astype(BF16)
        self.cross(6).start()

    def total(self):
        self.swap(7).wait_recv()
        total = self.pair_sum(7)
        for j in (4, 5, 3, 6):
            self.cross(j).wait_recv()
            total = total + self.far[j].astype(F32)
        return total

    def finish(self):
        for j in range(8):
            self.swap(j).wait_send()
        for j in range(7):
            self.cross(j).wait_send()


class DataSpread:
    scratch = [DMA((8,)), DMA((7,))]

    def __init__(self, src, out, sends, recvs):
        self.src, self.out_, self.sends, self.recvs = src, out, sends, recvs
        self.share = src.shape[-1] // 8

    def columns(self, d):
        return pl.ds(pl.multiple_of(d * self.share, self.share), self.share)

    def cross(self, j):
        d, t = places()
        peer = data_at(d, HOPS[j])
        return remote(
            self.src.at[:, :, self.columns(peer)],
            self.out_.at[d],
            self.sends,
            self.recvs,
            j,
            (peer, t),
        )

    def arrived(self, j):
        d, t = places()
        slot = self.out_.at[data_at(d, back(HOPS[j]))]
        return remote(slot, slot, self.sends, self.recvs, j, (d, other_core(t)))

    def own(self):
        d, t = places()
        return pltpu.make_async_copy(
            self.src.at[:, :, self.columns(d)], self.out_.at[d], self.sends.at[7]
        )

    def start(self):
        for j in range(7):
            self.cross(j).start()
        self.own().start()

    def finish(self):
        for j in range(7):
            self.arrived(j).wait_recv()
            self.cross(j).wait_send()
        self.own().wait()


class DataExchange:
    scratch = [DMA((15,)), DMA((14,))]

    def __init__(self, src, out, sends, recvs):
        self.src, self.out_, self.sends, self.recvs = src, out, sends, recvs
        self.half = src.shape[0] // 2
        self.share = src.shape[1] // 8

    def rows(self, t):
        return pl.ds(pl.multiple_of(lax.rem(t, 2) * self.half, self.half), self.half)

    def columns(self, d):
        return pl.ds(pl.multiple_of(d * self.share, self.share), self.share)

    def cross(self, j):
        d, t = places()
        peer = data_at(d, HOPS[j])
        return remote(
            self.src.at[self.rows(t), self.columns(peer)],
            self.out_.at[d, self.rows(t)],
            self.sends,
            self.recvs,
            j,
            (peer, t),
        )

    def hand(self, j, t_of):
        d, t = places()
        slot = self.out_.at[data_at(d, back(HOPS[j])), self.rows(t_of)]
        return slot

    def arrived(self, j):
        d, t = places()
        slot = self.hand(j, t)
        return remote(slot, slot, self.sends, self.recvs, j, (d, other_core(t)))

    def handed(self, j):
        d, t = places()
        slot = self.hand(j, t)
        return remote(slot, slot, self.sends, self.recvs, 7 + j, (d, other_core(t)))

    def received(self, j):
        d, t = places()
        slot = self.hand(j, other_core(t))
        return remote(slot, slot, self.sends, self.recvs, 7 + j, (d, other_core(t)))

    def own(self):
        d, t = places()
        return pltpu.make_async_copy(
            self.src.at[:, self.columns(d)], self.out_.at[d], self.sends.at[14]
        )

    def start(self):
        for j in (3, 4, 5):
            self.cross(j).start()
        self.own().start()

    def start_pairs(self):
        for j in (6, 0, 1, 2):
            self.cross(j).start()

    def finish(self):
        for j in (4, 5, 3, 6, 0, 1, 2):
            self.arrived(j).wait_recv()
            self.handed(j).start()
        for j in range(7):
            self.received(j).wait_recv()
            self.cross(j).wait_send()
            self.handed(j).wait_send()
        self.own().wait()


def taken(refs, *counts):
    out, at = [], 0
    for count in counts:
        out.append(refs[at : at + count])
        at += count
    return out


def comm_call(kernel, name, number, in_specs, out_specs, out_shape, scratch, args, limit=24):
    return pl.pallas_call(
        kernel,
        name=name,
        in_specs=in_specs,
        out_specs=out_specs,
        out_shape=out_shape,
        scratch_shapes=scratch,
        cost_estimate=pl.CostEstimate(flops=10**10, bytes_accessed=0, transcendentals=0),
        compiler_params=pltpu.CompilerParams(
            collective_id=number, has_side_effects=True, vmem_limit_bytes=limit * 2**20
        ),
    )(*args)


def shape(dims, dtype):
    return jax.ShapeDtypeStruct(dims, dtype)


def slot_of(ref):
    return lambda block: ref.at[block]


def half_slot(ref, half):
    return lambda block: ref.at[block, half]


def columns_of(ref):
    width = ref.shape[1] // 8
    return lambda block: ref.at[:, pl.ds(pl.multiple_of(block * width, width), width)]


def mean_of(values):
    return jnp.sum(values, axis=-1, keepdims=True) * (1.0 / values.shape[-1])


def strip(which, core):
    return pl.ds(pl.multiple_of(which * 128 + core * 64, 64), 64)


class CoreShare:
    scratch = [DMA((2,)), DMA((2,))]

    def __init__(self, sources, slot, sends, recvs):
        self.sources, self.slot, self.sends, self.recvs = sources, slot, sends, recvs

    def copy(self, j, core):
        d, t = places()
        slot = self.slot(j, core)
        src = slot if self.sources is None else self.sources[j]
        return remote(src, slot, self.sends, self.recvs, j, (d, other_core(t)))

    def start(self):
        d, t = places()
        for j in range(2):
            self.copy(j, lax.rem(t, 2)).start()

    def finish(self):
        d, t = places()
        for j in range(2):
            self.copy(j, 1 - lax.rem(t, 2)).wait_recv()
            self.copy(j, lax.rem(t, 2)).wait_send()


class Probes:
    COUNT = 4
    @staticmethod
    def scratch(kind):
        return kind.scratch * 4 + CoreShare.scratch

    def __init__(self, kind, layer, probes, gathered, sems):
        q, k, v, o = probes
        gq, gkv, go = gathered
        d, t = places()
        core = lax.rem(t, 2)
        width = k.shape[2]

        def part(which):
            return lambda block: gkv.at[
                strip(which, core), pl.ds(pl.multiple_of(block * width, width), width)
            ]

        self.jobs = [
            kind(k.at[layer], part(0), *sems[0:2]),
            kind(v.at[layer], part(1), *sems[2:4]),
            kind(q.at[layer], slot_of(gq), *sems[4:6]),
            kind(o.at[layer], columns_of(go), *sems[6:8]),
        ]
        self.share = CoreShare(None, lambda j, c: gkv.at[strip(j, c)], *sems[8:10])

    @staticmethod
    def shapes(probes):
        q, k, v, o = probes
        return [
            shape((8,) + q.shape[1:], BF16),
            shape((4 * k.shape[1], 8 * k.shape[2]), BF16),
            shape((o.shape[1], 8 * o.shape[2]), BF16),
        ]

    def start(self):
        for job in self.jobs:
            job.start()

    def relay(self):
        for job in self.jobs:
            job.relay()

    def pass_on(self):
        for job in self.jobs:
            job.pass_on()

    def finish(self):
        for job in self.jobs[:2]:
            job.finish()
        self.share.start()
        for job in self.jobs[2:]:
            job.finish()
        self.share.finish()


def normed_kernel(tokens, gains, h_low):
    wide = tokens[...].astype(F32)
    inverse = lax.rsqrt(mean_of(wide * wide) + EPS)
    h_low[...] = (wide * inverse * gains[0:1]).astype(BF16)


def normed(tokens, gains):
    return pl.pallas_call(
        normed_kernel,
        name="normed",
        in_specs=[VMEM, VMEM],
        out_specs=VMEM,
        out_shape=shape(tokens.shape, BF16),
        cost_estimate=pl.CostEstimate(flops=10**9, bytes_accessed=0, transcendentals=0),
        compiler_params=pltpu.CompilerParams(vmem_limit_bytes=8 * 2**20),
    )(tokens, gains)


def first_kernel(*refs):
    (
        (h_low, q, k, v, o, kw, vw),
        (h_all, hs, gq, gkv, go, kv),
        (mini,),
        row_sems,
        spread_sems,
        slice_sems,
        share_sems,
        own_sems,
        probe_sems,
    ) = taken(refs, 7, 6, 1, 2, 2, 2, 2, 1, 10)
    d, t = places()
    core = lax.rem(t, 2)
    enter(HOPS)
    spread = DataSpread(h_low, mini, *spread_sems)
    rows = TensorGather(h_low, slot_of(h_all), *row_sems)
    slices = TensorGather(mini, lambda block: hs.at[:, block], *slice_sems)
    share = CoreShare((kw, vw), lambda j, c: kv.at[:, strip(j, c)], *share_sems)
    probes = Probes(LargeGather, 0, (q, k, v, o), (gq, gkv, go), probe_sems)
    own = [
        pltpu.make_async_copy(src, kv.at[:, strip(j, core)], own_sems[0].at[j])
        for j, src in enumerate((kw, vw))
    ]
    spread.start()
    rows.start()
    probes.start()
    rows.relay()
    spread.finish()
    slices.start()
    share.start()
    for copy in own:
        copy.start()
    rows.finish()
    probes.relay()
    slices.relay()
    probes.pass_on()
    slices.finish()
    share.finish()
    for copy in own:
        copy.wait()
    probes.finish()


def first(h_low, probes, kw, vw):
    half, width = h_low.shape[1:]
    return comm_call(
        first_kernel,
        "first",
        1,
        [VMEM] + [HBM] * 6,
        [VMEM] + [ANY] * 5,
        [shape((16, 2, half, width), BF16), shape((8, 16, 2, half, width // 8), BF16)]
        + Probes.shapes(probes)
        + [shape((2, 4 * kw.shape[1], width), BF16)],
        [pltpu.VMEM((8, 2, half, width // 8), BF16)]
        + TensorGather.scratch
        + DataSpread.scratch
        + TensorGather.scratch
        + CoreShare.scratch
        + [DMA((2,))]
        + Probes.scratch(LargeGather),
        (h_low,) + probes + (kw, vw),
    )


def between_kernel(*refs):
    (
        (primal, moved, tokens, gains, q, k, v, o),
        (x_out, t_out, h_all, th_all, gq, gkv, go),
        (h_low, th_low),
        sum_refs,
        gather_refs,
        sems,
    ) = taken(refs, 8, 7, 2, 20, 8, 10)
    gain = gains[1:2]
    enter(NEAR)
    lots = taken(sum_refs, 5, 5, 5, 5)
    primals = [TensorSum(r, primal, *lots[r]) for r in range(2)]
    moves = [TensorSum(r, moved, *lots[2 + r]) for r in range(2)]
    sums = [primals[0], moves[0], primals[1], moves[1]]
    lots = taken(gather_refs, 2, 2, 2, 2)
    rows_h = [TensorGather(h_low.at[r], half_slot(h_all, r), *lots[r]) for r in range(2)]
    rows_th = [TensorGather(th_low.at[r], half_slot(th_all, r), *lots[2 + r]) for r in range(2)]
    probes = Probes(DataGather, 1, (q, k, v, o), (gq, gkv, go), sems)
    for one in sums:
        one.start()
    for one in sums:
        one.send()
    probes.start()
    for one in sums[:2]:
        one.middle()
    for r in range(2):
        stream = (tokens[r].astype(F32) + primals[r].total()).astype(BF16)
        x_out[r] = stream
        wide = stream.astype(F32)
        inverse = lax.rsqrt(mean_of(wide * wide) + EPS)
        h_low[r] = (wide * inverse * gain).astype(BF16)
        rows_h[r].start()
        tangent = moves[r].total()
        t_out[r] = tangent
        shift = mean_of(wide * tangent)
        th_low[r] = (
            gain * (tangent * inverse - wide * inverse * inverse * inverse * shift)
        ).astype(BF16)
        rows_th[r].start()
        if r == 0:
            for one in sums[2:]:
                one.middle()
            rows_h[0].relay()
    rows_th[0].relay()
    probes.relay()
    rows_h[1].relay()
    rows_th[1].relay()
    probes.pass_on()
    for one in sums:
        one.finish()
    for rows in rows_h + rows_th:
        rows.finish()
    probes.finish()


def between(primal, moved, tokens, gains, probes):
    half, width = tokens.shape[1:]
    return comm_call(
        between_kernel,
        "between",
        2,
        [VMEM] * 4 + [HBM] * 4,
        [VMEM] * 4 + [ANY] * 3,
        [
            shape((2, half, width), BF16),
            shape((2, half, width), F32),
            shape((16, 2, half, width), BF16),
            shape((16, 2, half, width), BF16),
        ]
        + Probes.shapes(probes),
        [pltpu.VMEM((2, half, width), BF16)] * 2
        + TensorSum.scratch(width) * 4
        + TensorGather.scratch * 4
        + Probes.scratch(DataGather),
        (primal, moved, tokens, gains) + probes,
    )


def turn_kernel(*refs):
    (
        (lengths, moved, t_one, a_zero, a_one, h_one),
        (c_out, cb_all, ga_zero, ga_one, hs_one),
        (c_low,),
        sum_refs,
        gather_refs,
        sems,
    ) = taken(refs, 6, 5, 1, 10, 4, 6)
    d, t = places()
    enter(HOPS)
    lots = taken(sum_refs, 5, 5)
    sums = [TensorSum(r, moved, *lots[r]) for r in range(2)]
    lots = taken(gather_refs, 2, 2)
    rows = [TensorGather(c_low.at[r], half_slot(cb_all, r), *lots[r]) for r in range(2)]
    jobs = [
        DataGather(a_zero, slot_of(ga_zero), *sems[0:2]),
        DataGather(a_one, slot_of(ga_one), *sems[2:4]),
    ]
    swap = DataExchange(h_one, hs_one, *sems[4:6])
    for one in sums:
        one.start()
    for one in sums:
        one.send()
    for job in jobs:
        job.start()
    for one in sums:
        one.middle()
    swap.start()
    half = t_one.shape[1]
    for r in range(2):
        position = (2 * t + r) * half + lax.broadcasted_iota(jnp.int32, t_one.shape[1:], 0)
        mask = jnp.where(position < lengths[d], 1.0, 0.0)
        cotangent = mask * (t_one[r] + sums[r].total())
        c_out[r] = cotangent
        c_low[r] = cotangent.astype(BF16)
        rows[r].start()
    swap.start_pairs()
    for r in range(2):
        rows[r].relay()
        jobs[r].relay()
    for job in jobs:
        job.pass_on()
    for r in range(2):
        sums[r].finish()
        rows[r].finish()
    swap.finish()
    for job in jobs:
        job.finish()


SMEM = pl.BlockSpec(memory_space=pltpu.SMEM)


def turn(lengths, moved, t_one, a_zero, a_one, h_one):
    half, width = t_one.shape[1:]
    return comm_call(
        turn_kernel,
        "turn",
        3,
        [SMEM] + [VMEM] * 2 + [ANY] * 3,
        [VMEM] * 2 + [ANY] * 3,
        [
            shape((2, half, width), F32),
            shape((16, 2, half, width), BF16),
            shape((8,) + a_zero.shape, BF16),
            shape((8,) + a_one.shape, BF16),
            shape((8, h_one.shape[0], h_one.shape[1] // 8), BF16),
        ],
        [pltpu.VMEM((2, half, width), BF16)]
        + TensorSum.scratch(width) * 2
        + TensorGather.scratch * 2
        + DataGather.scratch * 2
        + DataExchange.scratch,
        (lengths, moved, t_one, a_zero, a_one, h_one),
    )


class Cotangents:
    def __init__(self, gq, gkv, gathered, came, merged, sems):
        self.gkv, self.came, self.merged = gkv, came, merged
        width = gq.shape[1]
        self.jobs = [
            DataGather(gq, lambda block: gathered.at[block, :, 0:width], *sems[0:2]),
            DataGather(
                merged,
                lambda block: gathered.at[block, :, width : width + merged.shape[1]],
                *sems[2:4],
            ),
        ]
        self.sends, self.recvs = sems[4:6]

    @staticmethod
    def scratch(gkv):
        return (
            [pltpu.VMEM(gkv.shape[1:], BF16)] * 2
            + DataGather.scratch * 2
            + [DMA((1,)), DMA((1,))]
        )

    def swap(self):
        d, t = places()
        return remote(
            self.gkv.at[1 - lax.rem(t, 2)],
            self.came,
            self.sends,
            self.recvs,
            0,
            (d, other_core(t)),
        )

    def start(self):
        d, t = places()
        self.jobs[0].start()
        self.swap().wait()
        mine = self.gkv[lax.rem(t, 2)].astype(F32) + self.came[...].astype(F32)
        self.merged[...] = mine.astype(BF16)
        self.jobs[1].start()

    def relay(self):
        for job in self.jobs:
            job.relay()

    def pass_on(self):
        for job in self.jobs:
            job.pass_on()

    def finish(self):
        for job in self.jobs:
            job.finish()


def lower_kernel(*refs):
    (
        (part, c_two, x_one, gains, gkv, gq, cb_one),
        (cb_all, gg, cbs, mini),
        (c_low,),
        sum_refs,
        gather_refs,
        (came, merged),
        sems,
        swap_sems,
        spread_sems,
    ) = taken(refs, 7, 4, 1, 10, 4, 2, 6, 2, 2)
    enter(HOPS)
    lots = taken(sum_refs, 5, 5)
    sums = [TensorSum(r, part, *lots[r]) for r in range(2)]
    lots = taken(gather_refs, 2, 2)
    rows = [TensorGather(c_low.at[r], half_slot(cb_all, r), *lots[r]) for r in range(2)]
    jobs = Cotangents(gq, gkv, gg, came, merged, sems)
    swap = DataExchange(cb_one, cbs, *swap_sems)
    jobs.swap().start()
    for one in sums:
        one.start()
    for one in sums:
        one.send()
    jobs.start()
    for one in sums:
        one.middle()
    swap.start()
    for r in range(2):
        scaled = sums[r].total() * gains[1:2]
        wide = x_one[r].astype(F32)
        inverse = lax.rsqrt(mean_of(wide * wide) + EPS)
        shift = mean_of(wide * scaled)
        cotangent = c_two[r] + inverse * (scaled - wide * inverse * inverse * shift)
        c_low[r] = cotangent.astype(BF16)
        rows[r].start()
    spread = DataSpread(c_low, mini, *spread_sems)
    spread.start()
    swap.start_pairs()
    for one in rows:
        one.relay()
    jobs.relay()
    jobs.pass_on()
    for r in range(2):
        sums[r].finish()
        rows[r].finish()
    swap.finish()
    spread.finish()
    jobs.finish()


def lower(part, c_two, x_one, gains, gkv, gq, cb_one):
    half, width = c_two.shape[1:]
    return comm_call(
        lower_kernel,
        "lower",
        4,
        [VMEM] * 5 + [ANY] * 2,
        [VMEM] + [ANY] * 3,
        [
            shape((16, 2, half, width), BF16),
            shape((8, gq.shape[0], gq.shape[1] + gkv.shape[2]), BF16),
            shape((8, cb_one.shape[0], width // 8), BF16),
            shape((8, 2, half, width // 8), BF16),
        ],
        [pltpu.VMEM((2, half, width), BF16)]
        + TensorSum.scratch(width) * 2
        + TensorGather.scratch * 2
        + Cotangents.scratch(gkv)
        + DataExchange.scratch
        + DataSpread.scratch,
        (part, c_two, x_one, gains, gkv, gq, cb_one),
    )


def last_kernel(*refs):
    (gkv, mini, gq), (gg, cbs), (came, merged), sems, slice_sems = taken(refs, 3, 2, 2, 6, 2)
    enter(NEAR)
    slices = TensorGather(mini, lambda block: cbs.at[:, block], *slice_sems)
    jobs = Cotangents(gq, gkv, gg, came, merged, sems)
    jobs.swap().start()
    slices.start()
    jobs.start()
    slices.relay()
    jobs.relay()
    jobs.pass_on()
    slices.finish()
    jobs.finish()


def last(gkv, mini, gq):
    return comm_call(
        last_kernel,
        "last",
        5,
        [VMEM] * 2 + [ANY],
        [ANY] * 2,
        [
            shape((8, gq.shape[0], gq.shape[1] + gkv.shape[2]), BF16),
            shape((8, 16) + mini.shape[1:], BF16),
        ],
        Cotangents.scratch(gkv) + TensorGather.scratch,
        (gkv, mini, gq),
    )


def contract(left_side, right_side, left_dim, right_dim):
    return lax.dot_general(
        left_side,
        right_side,
        (((left_dim,), (right_dim,)), ((), ())),
        preferred_element_type=F32,
    )


def turned(values, cosine, sine):
    return values * cosine + pltpu.roll(values, values.shape[1] // 2, 1) * sine


def attention_weights(q, k, length):
    size = q.shape[0]
    row = lax.broadcasted_iota(jnp.int32, (size, size), 0)
    column = lax.broadcasted_iota(jnp.int32, (size, size), 1)
    allowed = (column <= row) & (column < length)
    scores = contract(q, k, 1, 1) * (1.0 / math.sqrt(q.shape[1]))
    powers = jnp.where(allowed, jnp.exp(scores), 0.0)
    return powers / jnp.sum(powers, axis=-1, keepdims=True)


def forward_kernel(steps, second, *refs):
    more = 1 if second else 0
    (
        (lengths, cosine, sine, wq, kv, pq, pkv, wo, po, h),
        th,
        (q_out, k_out, v_out, a_out, moved),
        primal,
        (q_sum, tq_sum, kv_sum, tkv_sum, ta_low),
    ) = taken(refs, 10, more, 5, 1 - more, 5)
    i = pl.program_id(0)
    sums = (q_sum, tq_sum, kv_sum, tkv_sum)

    @pl.when(i == 0)
    def _():
        for one in sums:
            one[...] = jnp.zeros_like(one)

    @pl.when(i < steps)
    def _():
        normed = h[...]
        q_sum[...] += contract(normed, wq[...], 1, 0)
        kv_sum[...] += contract(normed, kv[...], 1, 1)
        tq = contract(normed, pq[...], 1, 0)
        tkv = contract(normed, pkv[...], 1, 1)
        if second:
            tq = tq + contract(th[0][...], wq[...], 1, 0)
            tkv = tkv + contract(th[0][...], kv[...], 1, 1)
        tq_sum[...] += tq
        tkv_sum[...] += tkv

    @pl.when(i == steps - 1)
    def _():
        length = lengths[lax.axis_index("dp")]
        scaling = 1.0 / math.sqrt(HD)
        cos, sin = cosine[...], sine[...]
        k = turned(kv_sum[:, 0:HD], cos, sin).astype(BF16)
        v = kv_sum[:, HD:].astype(BF16)
        tk = turned(tkv_sum[:, 0:HD], cos, sin).astype(BF16)
        tv = tkv_sum[:, HD:].astype(BF16)
        k_out[...] = k
        v_out[...] = v
        for at in range(0, q_sum.shape[1], HD):
            head = slice(at, at + HD)
            q = turned(q_sum[:, head], cos, sin).astype(BF16)
            tq = turned(tq_sum[:, head], cos, sin).astype(BF16)
            q_out[:, head] = q
            weights = attention_weights(q, k, length)
            low = weights.astype(BF16)
            a_out[:, head] = contract(low, v, 1, 0).astype(BF16)
            scores = (contract(tq, k, 1, 1) + contract(q, tk, 1, 1)) * scaling
            change = weights * (scores - jnp.sum(weights * scores, axis=-1, keepdims=True))
            ta = contract(change.astype(BF16), v, 1, 0) + contract(low, tv, 1, 0)
            ta_low[:, head] = ta.astype(BF16)

    @pl.when(i >= steps)
    def _():
        moved[...] = (
            contract(ta_low[...], wo[...], 1, 0) + contract(a_out[...], po[...], 1, 0)
        ).astype(BF16)
        if not second:
            primal[0][...] = contract(a_out[...], wo[...], 1, 0).astype(BF16)


def whole(dims):
    return pl.BlockSpec(dims, lambda i: (0,) * len(dims))


TILE = 1024


def forward(layer, lengths, tables, wq, kv, pq, pkv, wo, po, h, th=None):
    rows, width = h.shape
    columns = wq.shape[2]
    steps = width // TILE
    second = th is not None

    def now(i):
        return jnp.minimum(i, steps - 1)

    def later(i):
        return jnp.maximum(i - steps, 0)

    into = pl.BlockSpec((rows, TILE), lambda i: (0, now(i)))
    out = pl.BlockSpec((rows, TILE), lambda i: (0, later(i)))
    in_specs = [
        SMEM,
        whole((rows, HD)),
        whole((rows, HD)),
        pl.BlockSpec((None, TILE, columns), lambda i: (layer, now(i), 0)),
        pl.BlockSpec((None, 2 * HD, TILE), lambda i: (layer, 0, now(i))),
        pl.BlockSpec((TILE, columns), lambda i: (now(i), 0)),
        pl.BlockSpec((2 * HD, TILE), lambda i: (0, now(i))),
        pl.BlockSpec((None, columns, TILE), lambda i: (layer, 0, later(i))),
        pl.BlockSpec((columns, TILE), lambda i: (0, later(i))),
        into,
    ] + [into] * second
    out_specs = [
        whole((rows, columns)),
        whole((rows, HD)),
        whole((rows, HD)),
        whole((rows, columns)),
        out,
    ] + [out] * (not second)
    out_shape = [
        shape((rows, columns), BF16),
        shape((rows, HD), BF16),
        shape((rows, HD), BF16),
        shape((rows, columns), BF16),
        shape((rows, width), BF16),
    ] + [shape((rows, width), BF16)] * (not second)
    args = (lengths,) + tables + (wq, kv, pq, pkv, wo, po, h) + ((th,) if second else ())
    return pl.pallas_call(
        functools.partial(forward_kernel, steps, second),
        name=f"forward_{layer}",
        grid=(2 * steps,),
        in_specs=in_specs,
        out_specs=out_specs,
        out_shape=out_shape,
        scratch_shapes=[
            pltpu.VMEM((rows, columns), F32),
            pltpu.VMEM((rows, columns), F32),
            pltpu.VMEM((rows, 2 * HD), F32),
            pltpu.VMEM((rows, 2 * HD), F32),
            pltpu.VMEM((rows, columns), BF16),
        ],
        compiler_params=pltpu.CompilerParams(vmem_limit_bytes=20 * 2**20),
    )(*args)


def backward_kernel(steps, lowest, *refs):
    more = 0 if lowest else 1
    (
        (lengths, cosine, sine, q_in, k_in, v_in, cb, wo),
        weights_in,
        (gq_out, gkv_out),
        part,
        (ga_sum, gkv_low),
    ) = taken(refs, 8, 2 * more, 2, more, 2)
    i = pl.program_id(0)

    @pl.when(i == 0)
    def _():
        ga_sum[...] = jnp.zeros_like(ga_sum)

    @pl.when(i < steps)
    def _():
        ga_sum[...] += contract(cb[...], wo[...], 1, 1)

    @pl.when(i == steps - 1)
    def _():
        length = lengths[lax.axis_index("dp")]
        scaling = 1.0 / math.sqrt(HD)
        cos, sin = cosine[...], -sine[...]
        k, v = k_in[...], v_in[...]
        gk, gv = None, None
        for at in range(0, ga_sum.shape[1], HD):
            head = slice(at, at + HD)
            q = q_in[:, head]
            ga = ga_sum[:, head].astype(BF16)
            weights = attention_weights(q, k, length)
            grads = contract(ga, v, 1, 1)
            value = contract(weights.astype(BF16), ga, 0, 0)
            scores = (
                weights * (grads - jnp.sum(weights * grads, axis=-1, keepdims=True)) * scaling
            ).astype(BF16)
            gq_out[:, head] = turned(contract(scores, k, 1, 0), cos, sin).astype(BF16)
            key = contract(scores, q, 0, 0)
            gk = key if gk is None else gk + key
            gv = value if gv is None else gv + value
        gk = turned(gk, cos, sin).astype(BF16)
        gv = gv.astype(BF16)
        half = HD // 2
        gkv_low[:, 0:HD] = gk
        gkv_low[:, HD:] = gv
        gkv_out[0] = jnp.concatenate([gk[:, 0:half], gv[:, 0:half]], axis=-1)
        gkv_out[1] = jnp.concatenate([gk[:, half:], gv[:, half:]], axis=-1)

    if not lowest:

        @pl.when(i >= steps)
        def _():
            part[0][...] = (
                contract(gq_out[...], weights_in[0][...], 1, 1)
                + contract(gkv_low[...], weights_in[1][...], 1, 0)
            ).astype(BF16)


def backward(layer, lengths, tables, q, k, v, cb, wo, wq, kv):
    rows, width = cb.shape
    columns = wo.shape[1]
    steps = width // TILE
    lowest = layer == 0

    def now(i):
        return jnp.minimum(i, steps - 1)

    def later(i):
        return jnp.maximum(i - steps, 0)

    in_specs = [
        SMEM,
        whole((rows, HD)),
        whole((rows, HD)),
        whole((rows, columns)),
        whole((rows, HD)),
        whole((rows, HD)),
        pl.BlockSpec((rows, TILE), lambda i: (0, now(i))),
        pl.BlockSpec((None, columns, TILE), lambda i: (layer, 0, now(i))),
    ]
    out_specs = [whole((rows, columns)), whole((2, rows, HD))]
    out_shape = [shape((rows, columns), BF16), shape((2, rows, HD), BF16)]
    args = (lengths,) + tables + (q, k, v, cb, wo)
    if not lowest:
        in_specs += [
            pl.BlockSpec((None, TILE, columns), lambda i: (layer, later(i), 0)),
            pl.BlockSpec((None, 2 * HD, TILE), lambda i: (layer, 0, later(i))),
        ]
        out_specs.append(pl.BlockSpec((rows, TILE), lambda i: (0, later(i))))
        out_shape.append(shape((rows, width), BF16))
        args += (wq, kv)
    return pl.pallas_call(
        functools.partial(backward_kernel, steps, lowest),
        name=f"backward_{layer}",
        grid=(steps if lowest else 2 * steps,),
        in_specs=in_specs,
        out_specs=out_specs,
        out_shape=out_shape,
        scratch_shapes=[
            pltpu.VMEM((rows, columns), F32),
            pltpu.VMEM((rows, 2 * HD), BF16),
        ],
        compiler_params=pltpu.CompilerParams(vmem_limit_bytes=20 * 2**20),
    )(*args)


def products_kernel(*refs):
    sides, (q_out, k_out, v_out, o_out), (q_sum,) = taken(refs, 8, 4, 1)
    i = pl.program_id(0)
    columns, half = q_out.shape[2], k_out.shape[1]
    for layer in range(2):
        hs, gg, ga, cs = [ref[...].reshape(-1, ref.shape[-1]) for ref in sides[4 * layer :][:4]]
        g = contract(gg, hs, 0, 0)
        o = contract(ga, cs, 0, 0)

        @pl.when(i == 0)
        def _():
            q_sum[layer] = g[0:columns]
            k_out[layer] = g[columns : columns + half]
            v_out[layer] = g[columns + half :]
            o_out[layer] = o

        @pl.when(i > 0)
        def _():
            q_sum[layer] += g[0:columns]
            k_out[layer] += g[columns : columns + half]
            v_out[layer] += g[columns + half :]
            o_out[layer] += o

    @pl.when(i == pl.num_programs(0) - 1)
    def _():
        for layer in range(2):
            q_out[layer] = q_sum[layer].T


def products(*sides):
    chunk = 2
    columns, share = sides[2].shape[2], sides[0].shape[2]
    half = (sides[1].shape[2] - columns) // 2
    out_shape = [
        shape((2, share, columns), F32),
        shape((2, half, share), F32),
        shape((2, half, share), F32),
        shape((2, columns, share), F32),
    ]
    return pl.pallas_call(
        products_kernel,
        name="products",
        grid=(8 // chunk,),
        in_specs=[
            pl.BlockSpec((chunk,) + side.shape[1:], lambda i: (i, 0, 0)) for side in sides
        ],
        out_specs=[whole(out.shape) for out in out_shape],
        out_shape=out_shape,
        scratch_shapes=[pltpu.VMEM((2, columns, share), F32)],
        compiler_params=pltpu.CompilerParams(vmem_limit_bytes=20 * 2**20),
    )(*sides)


def rope_tables():
    angles = np.arange(LEN)[:, None] * THETA ** (-2.0 * np.arange(HD // 2) / HD)[None, :]
    cosine, sine = np.cos(angles), np.sin(angles)
    return (
        jnp.asarray(np.concatenate([cosine, cosine], axis=1), F32),
        jnp.asarray(np.concatenate([-sine, sine], axis=1), F32),
    )


def body(
    tokens,
    lengths,
    gains,
    query_weight,
    key_weight,
    value_weight,
    out_weight,
    query_probe,
    key_probe,
    value_probe,
    out_probe,
):
    rows, width = tokens.shape
    tables = rope_tables()

    def turned_over(array):
        return jnp.swapaxes(array, 1, 2)

    tokens = tokens.reshape(2, rows // 2, width)

    def by_owner(part):
        return part.reshape(8, 2, 2, rows // 2, width)

    def all_rows(blocks):
        return blocks.reshape(-1, blocks.shape[-1])

    def by_batch(blocks):
        return blocks.reshape(blocks.shape[0], -1, blocks.shape[-1])

    probes = (query_probe, turned_over(key_probe), turned_over(value_probe), out_probe)
    h_zero, hs_zero, pq, pkv, po, kv = first(
        normed(tokens, gains), probes, turned_over(key_weight), turned_over(value_weight)
    )
    q0, k0, v0, a_zero, moved, primal = forward(
        0, lengths, tables, query_weight, kv, all_rows(pq), pkv, out_weight, po, all_rows(h_zero)
    )
    x_one, t_one, h_one, th_one, pq, pkv, po = between(
        by_owner(primal), by_owner(moved), tokens, gains, probes
    )
    h_one = all_rows(h_one)
    q1, k1, v1, a_one, moved = forward(
        1,
        lengths,
        tables,
        query_weight,
        kv,
        all_rows(pq),
        pkv,
        out_weight,
        po,
        h_one,
        all_rows(th_one),
    )
    c_two, cb_one, ga_zero, ga_one, hs_one = turn(
        lengths, by_owner(moved), t_one, a_zero, a_one, h_one
    )
    cb_one = all_rows(cb_one)
    gq, gkv, part = backward(
        1, lengths, tables, q1, k1, v1, cb_one, out_weight, query_weight, kv
    )
    cb_zero, gg_one, cs_one, mini = lower(
        by_owner(part), c_two, x_one, gains, gkv, gq, cb_one
    )
    gq, gkv = backward(
        0, lengths, tables, q0, k0, v0, all_rows(cb_zero), out_weight, query_weight, kv
    )
    gg_zero, cs_zero = last(gkv, mini, gq)
    q, k, v, o = products(
        by_batch(hs_zero), gg_zero, ga_zero, by_batch(cs_zero), hs_one, gg_one, ga_one, cs_one
    )
    return (q, turned_over(k), turned_over(v), o)


def solution(mesh):
    placed = (
        P(("dp", "tensor"), None),
        P(),
        P(),
        P(None, None, "tensor"),
        P(None, None, "tensor"),
        P(None, None, "tensor"),
        P(None, "tensor", None),
        P(None, "dp", "tensor"),
        P(None, "dp", "tensor"),
        P(None, "dp", "tensor"),
        P(None, "tensor", "dp"),
    )
    return jax.shard_map(
        body,
        mesh=mesh,
        in_specs=placed,
        out_specs=(
            P(None, "dp", "tensor"),
            P(None, "dp", "tensor"),
            P(None, "dp", "tensor"),
            P(None, "tensor", "dp"),
        ),
        check_vma=False,
    )
```

```python
import functools
import math

import jax
import jax.numpy as jnp
import numpy as np
from jax import lax
from jax.experimental import pallas as pl
from jax.experimental.pallas import tpu as pltpu
from jax.sharding import PartitionSpec as P

HD = 128
LEN = 256
EPS = 1e-05
THETA = 500000.0

MESH = pl.DeviceIdType.MESH
F32 = jnp.float32
BF16 = jnp.bfloat16
VMEM = pl.BlockSpec(memory_space=pltpu.VMEM)
ANY = pl.BlockSpec(memory_space=pl.ANY)
HBM = pl.BlockSpec(memory_space=pltpu.HBM)
SMEM = pl.BlockSpec(memory_space=pltpu.SMEM)
DMA = pltpu.SemaphoreType.DMA
TILE = 1024

HOPS = ((1, 1), (3, 1), (2, 1), (2, 0), (1, 0), (3, 0), (0, 1))
NEAR = HOPS[3:]


def back(hop):
    return ((4 - hop[0]) % 4, hop[1])


def data_at(d, hop):
    ring, pair = lax.div(d, 2), lax.rem(d, 2)
    return lax.rem(ring + hop[0], 4) * 2 + lax.rem(pair + hop[1], 2)


def chip_at(t, hop):
    return data_at(lax.div(t, 2), hop)


def tensor_at(t, hop):
    return chip_at(t, hop) * 2 + lax.rem(t, 2)


def other_core(t):
    return t + 1 - 2 * lax.rem(t, 2)


def places():
    return lax.axis_index("dp"), lax.axis_index("tensor")


def remote(src, dst, sends, recvs, j, device):
    return pltpu.make_async_remote_copy(
        src_ref=src,
        dst_ref=dst,
        send_sem=sends.at[j],
        recv_sem=recvs.at[j],
        device_id=device,
        device_id_type=MESH,
    )


def enter(data_hops):
    d, t = places()
    barrier = pltpu.get_barrier_semaphore()
    peers = [(d, other_core(t))]
    peers += [(d, tensor_at(t, hop)) for hop in NEAR]
    peers += [(data_at(d, hop), t) for hop in data_hops]
    for peer in peers:
        pl.semaphore_signal(barrier, inc=1, device_id=peer, device_id_type=MESH)
    pl.semaphore_wait(barrier, len(peers))


def half_of(ref, half):
    if half is None:
        return ref
    rows = ref.shape[0] // 2
    return ref.at[pl.ds(half * rows, rows)]


class RingGather:
    ROUTES = ()
    FIRST = 0

    def __init__(self, src, slot, sends, recvs):
        self.src, self.slot, self.sends, self.recvs = src, slot, sends, recvs

    def out(self, j):
        hop, block, unused, half = self.ROUTES[j]
        slot = half_of(self.slot(self.place(block)), half)
        src = self.src if j < self.FIRST else slot
        return remote(src, slot, self.sends, self.recvs, j, self.device(hop))

    def into(self, j):
        slot = half_of(self.slot(self.place(self.ROUTES[j][2])), self.ROUTES[j][3])
        return remote(slot, slot, self.sends, self.recvs, j, self.device((0, 1)))

    def own(self):
        n = len(self.ROUTES)
        return pltpu.make_async_copy(self.src, self.slot(self.place((0, 0))), self.sends.at[n])

    def start(self):
        for j in range(self.FIRST):
            self.out(j).start()
        self.own().start()

    def sent(self):
        for j in range(len(self.ROUTES)):
            self.out(j).wait_send()
        self.own().wait()


class DataGather(RingGather):
    scratch = [DMA((8,)), DMA((7,))]
    FIRST = 4
    ROUTES = (
        ((0, 1), (0, 0), (0, 1), None),
        ((1, 0), (0, 0), (3, 0), None),
        ((3, 0), (0, 0), (1, 0), None),
        ((2, 0), (0, 0), (2, 0), None),
        ((1, 0), (0, 1), (3, 1), None),
        ((3, 0), (0, 1), (1, 1), None),
        ((0, 1), (2, 0), (2, 1), None),
    )

    def place(self, hop):
        d, t = places()
        return data_at(d, hop)

    def device(self, hop):
        d, t = places()
        return (data_at(d, hop), t)

    def relay(self):
        self.into(0).wait_recv()
        self.out(4).start()
        self.out(5).start()

    def pass_on(self):
        self.into(3).wait_recv()
        self.out(6).start()

    def finish(self):
        for j in (1, 2, 4, 5, 6):
            self.into(j).wait_recv()
        self.sent()


class LargeGather(DataGather):
    scratch = [DMA((12,)), DMA((11,))]
    FIRST = 3
    ROUTES = (
        ((0, 1), (0, 0), (0, 1), None),
        ((1, 0), (0, 0), (3, 0), None),
        ((3, 0), (0, 0), (1, 0), None),
        ((1, 0), (0, 1), (3, 1), 0),
        ((3, 0), (0, 1), (1, 1), 1),
        ((1, 0), (3, 0), (2, 0), 0),
        ((0, 1), (3, 0), (3, 1), 1),
        ((3, 0), (1, 0), (2, 0), 1),
        ((0, 1), (1, 0), (1, 1), 0),
        ((1, 0), (3, 1), (2, 1), 0),
        ((3, 0), (1, 1), (2, 1), 1),
    )

    def relay(self):
        for j in range(3):
            self.into(j).wait_recv()
            self.out(3 + 2 * j).start()
            self.out(4 + 2 * j).start()

    def pass_on(self):
        for j in (3, 4):
            self.into(j).wait_recv()
            self.out(6 + j).start()

    def finish(self):
        for j in range(5, 11):
            self.into(j).wait_recv()
        self.sent()


class TensorGather(RingGather):
    scratch = [DMA((16,)), DMA((15,))]
    FIRST = 4
    ROUTES = (
        ((0, 1), (0, 0), (0, 1), None),
        ((1, 0), (0, 0), (3, 0), None),
        ((3, 0), (0, 0), (1, 0), None),
        ((2, 0), (0, 0), (2, 0), None),
        ((1, 0), (0, 1), (3, 1), None),
        ((3, 0), (0, 1), (1, 1), None),
        ((2, 0), (0, 1), (2, 1), None),
    )

    def place(self, hop):
        d, t = places()
        return tensor_at(t, hop)

    def device(self, hop):
        d, t = places()
        return (d, tensor_at(t, hop))

    def handover(self, j, src, block):
        d, t = places()
        return pltpu.make_async_remote_copy(
            src_ref=src,
            dst_ref=self.slot(block),
            send_sem=self.sends.at[8 + j],
            recv_sem=self.recvs.at[7 + j],
            device_id=(d, other_core(t)),
            device_id_type=MESH,
        )

    def hand(self, j):
        block = self.place(self.ROUTES[j][2])
        return self.handover(j, self.slot(block), block)

    def near(self):
        return self.handover(7, self.src, self.place((0, 0)))

    def start(self):
        super().start()
        self.near().start()

    def relay(self):
        self.into(0).wait_recv()
        for j in range(4, 7):
            self.out(j).start()
        self.hand(0).start()

    def finish(self):
        for j in range(1, 7):
            self.into(j).wait_recv()
            self.hand(j).start()
        self.sent()
        d, t = places()
        far = other_core(t)
        self.handover(7, self.slot(far), far).wait_recv()
        self.near().wait_send()
        for j in range(7):
            block = tensor_at(far, self.ROUTES[j][2])
            self.handover(j, self.slot(block), block).wait_recv()
            self.hand(j).wait_send()


class TensorSum:
    STEPS = ((2, 1), (1, 1), (3, 1), (2, 0), (1, 0), (3, 0))
    BLOCKS = STEPS + ((0, 1), (0, 0))

    @staticmethod
    def scratch(columns):
        return [
            pltpu.VMEM((8, 8, columns), BF16),
            pltpu.VMEM((7, 8, columns), BF16),
            pltpu.VMEM((7, 8, columns), BF16),
            DMA((15,)),
            DMA((15,)),
        ]

    def __init__(self, rows, part, near, sent, far, sends, recvs):
        self.rows = rows
        self.part, self.near_, self.sent, self.far = part, near, sent, far
        self.sends, self.recvs = sends, recvs

    def swap(self, j):
        d, t = places()
        k = chip_at(t, self.BLOCKS[j])
        c = lax.rem(t, 2)
        return remote(
            self.part.at[k, 1 - c, self.rows], self.near_.at[k], self.sends, self.recvs, j, (d, other_core(t))
        )

    def cross(self, j):
        d, t = places()
        hop = (self.STEPS[j][0], 0) if j < 6 else (0, 1)
        return remote(
            self.sent.at[j], self.far.at[j], self.sends, self.recvs, 8 + j, (d, tensor_at(t, hop))
        )

    def pair_sum(self, j):
        d, t = places()
        k = chip_at(t, self.BLOCKS[j])
        c = lax.rem(t, 2)
        return self.part[k, c, self.rows].astype(F32) + self.near_[k].astype(F32)

    def start(self):
        for j in range(8):
            self.swap(j).start()

    def send(self):
        for j in range(6):
            self.swap(j).wait_recv()
            self.sent[j] = self.pair_sum(j).astype(BF16)
            self.cross(j).start()

    def middle(self):
        self.swap(6).wait_recv()
        total = self.pair_sum(6)
        for j in (1, 2, 0):
            self.cross(j).wait_recv()
            total = total + self.far[j].astype(F32)
        self.sent[6] = total.astype(BF16)
        self.cross(6).start()

    def total(self):
        self.swap(7).wait_recv()
        total = self.pair_sum(7)
        for j in (4, 5, 3, 6):
            self.cross(j).wait_recv()
            total = total + self.far[j].astype(F32)
        return total

    def finish(self):
        for j in range(8):
            self.swap(j).wait_send()
        for j in range(7):
            self.cross(j).wait_send()


class DataSpread:
    scratch = [DMA((8,)), DMA((7,))]

    def __init__(self, src, out, sends, recvs):
        self.src, self.out_, self.sends, self.recvs = src, out, sends, recvs
        self.share = src.shape[-1] // 8

    def columns(self, d):
        return pl.ds(pl.multiple_of(d * self.share, self.share), self.share)

    def cross(self, j):
        d, t = places()
        peer = data_at(d, HOPS[j])
        return remote(
            self.src.at[:, :, self.columns(peer)],
            self.out_.at[d],
            self.sends,
            self.recvs,
            j,
            (peer, t),
        )

    def arrived(self, j):
        d, t = places()
        slot = self.out_.at[data_at(d, back(HOPS[j]))]
        return remote(slot, slot, self.sends, self.recvs, j, (d, other_core(t)))

    def own(self):
        d, t = places()
        return pltpu.make_async_copy(
            self.src.at[:, :, self.columns(d)], self.out_.at[d], self.sends.at[7]
        )

    def start(self):
        for j in range(7):
            self.cross(j).start()
        self.own().start()

    def finish(self):
        for j in range(7):
            self.arrived(j).wait_recv()
            self.cross(j).wait_send()
        self.own().wait()


class DataExchange:
    scratch = [DMA((15,)), DMA((14,))]

    def __init__(self, src, out, sends, recvs):
        self.src, self.out_, self.sends, self.recvs = src, out, sends, recvs
        self.half = src.shape[0] // 2
        self.share = src.shape[1] // 8

    def rows(self, t):
        return pl.ds(pl.multiple_of(lax.rem(t, 2) * self.half, self.half), self.half)

    def columns(self, d):
        return pl.ds(pl.multiple_of(d * self.share, self.share), self.share)

    def cross(self, j):
        d, t = places()
        peer = data_at(d, HOPS[j])
        return remote(
            self.src.at[self.rows(t), self.columns(peer)],
            self.out_.at[d, self.rows(t)],
            self.sends,
            self.recvs,
            j,
            (peer, t),
        )

    def hand(self, j, t_of):
        d, t = places()
        slot = self.out_.at[data_at(d, back(HOPS[j])), self.rows(t_of)]
        return slot

    def arrived(self, j):
        d, t = places()
        slot = self.hand(j, t)
        return remote(slot, slot, self.sends, self.recvs, j, (d, other_core(t)))

    def handed(self, j):
        d, t = places()
        slot = self.hand(j, t)
        return remote(slot, slot, self.sends, self.recvs, 7 + j, (d, other_core(t)))

    def received(self, j):
        d, t = places()
        slot = self.hand(j, other_core(t))
        return remote(slot, slot, self.sends, self.recvs, 7 + j, (d, other_core(t)))

    def own(self):
        d, t = places()
        return pltpu.make_async_copy(
            self.src.at[:, self.columns(d)], self.out_.at[d], self.sends.at[14]
        )

    def start(self):
        for j in (3, 4, 5):
            self.cross(j).start()
        self.own().start()

    def start_pairs(self):
        for j in (6, 0, 1, 2):
            self.cross(j).start()

    def finish(self):
        for j in (4, 5, 3, 6, 0, 1, 2):
            self.arrived(j).wait_recv()
            self.handed(j).start()
        for j in range(7):
            self.received(j).wait_recv()
            self.cross(j).wait_send()
            self.handed(j).wait_send()
        self.own().wait()


def taken(refs, *counts):
    out, at = [], 0
    for count in counts:
        out.append(refs[at : at + count])
        at += count
    return out


def comm_call(kernel, name, number, in_specs, out_specs, out_shape, scratch, args, limit=12):
    return pl.pallas_call(
        kernel,
        name=name,
        in_specs=in_specs,
        out_specs=out_specs,
        out_shape=out_shape,
        scratch_shapes=scratch,
        cost_estimate=pl.CostEstimate(flops=10**10, bytes_accessed=0, transcendentals=0),
        compiler_params=pltpu.CompilerParams(
            collective_id=number, has_side_effects=True, vmem_limit_bytes=limit * 2**20
        ),
    )(*args)


def shape(dims, dtype):
    return jax.ShapeDtypeStruct(dims, dtype)


def slot_of(ref):
    return lambda block: ref.at[block]


def half_slot(ref, half):
    return lambda block: ref.at[block, half]


def columns_of(ref):
    width = ref.shape[1] // 8
    return lambda block: ref.at[:, pl.ds(pl.multiple_of(block * width, width), width)]


def mean_of(values):
    return jnp.sum(values, axis=-1, keepdims=True) * (1.0 / values.shape[-1])


def strip(which, core):
    return pl.ds(pl.multiple_of(which * 128 + core * 64, 64), 64)


class CoreShare:
    scratch = [DMA((2,)), DMA((2,))]

    def __init__(self, sources, slot, sends, recvs):
        self.sources, self.slot, self.sends, self.recvs = sources, slot, sends, recvs

    def copy(self, j, core):
        d, t = places()
        slot = self.slot(j, core)
        src = slot if self.sources is None else self.sources[j]
        return remote(src, slot, self.sends, self.recvs, j, (d, other_core(t)))

    def start(self):
        d, t = places()
        for j in range(2):
            self.copy(j, lax.rem(t, 2)).start()

    def finish(self):
        d, t = places()
        for j in range(2):
            self.copy(j, 1 - lax.rem(t, 2)).wait_recv()
            self.copy(j, lax.rem(t, 2)).wait_send()


class Probes:
    COUNT = 4
    @staticmethod
    def scratch(kind):
        return kind.scratch * 4 + CoreShare.scratch

    def __init__(self, kind, layer, probes, gathered, sems):
        q, k, v, o = probes
        gq, gkv, go = gathered
        d, t = places()
        core = lax.rem(t, 2)
        width = k.shape[2]

        def part(which):
            return lambda block: gkv.at[
                strip(which, core), pl.ds(pl.multiple_of(block * width, width), width)
            ]

        self.jobs = [
            kind(k.at[layer], part(0), *sems[0:2]),
            kind(v.at[layer], part(1), *sems[2:4]),
            kind(q.at[layer], slot_of(gq), *sems[4:6]),
            kind(o.at[layer], columns_of(go), *sems[6:8]),
        ]
        self.share = CoreShare(None, lambda j, c: gkv.at[strip(j, c)], *sems[8:10])

    @staticmethod
    def shapes(probes):
        q, k, v, o = probes
        return [
            shape((8,) + q.shape[1:], BF16),
            shape((4 * k.shape[1], 8 * k.shape[2]), BF16),
            shape((o.shape[1], 8 * o.shape[2]), BF16),
        ]

    def start(self):
        for job in self.jobs:
            job.start()

    def relay(self):
        for job in self.jobs:
            job.relay()

    def pass_on(self):
        for job in self.jobs:
            job.pass_on()

    def finish(self):
        for job in self.jobs[:2]:
            job.finish()
        self.share.start()
        for job in self.jobs[2:]:
            job.finish()
        self.share.finish()


def contract(left_side, right_side, left_dim, right_dim):
    return lax.dot_general(
        left_side,
        right_side,
        (((left_dim,), (right_dim,)), ((), ())),
        preferred_element_type=F32,
    )


def turned(values, cosine, sine):
    return values * cosine + pltpu.roll(values, values.shape[1] // 2, 1) * sine


def attention_weights(q, k, length):
    size = q.shape[0]
    row = lax.broadcasted_iota(jnp.int32, (size, size), 0)
    column = lax.broadcasted_iota(jnp.int32, (size, size), 1)
    allowed = (column <= row) & (column < length)
    scores = contract(q, k, 1, 1) * (1.0 / math.sqrt(q.shape[1]))
    powers = jnp.where(allowed, jnp.exp(scores), 0.0)
    return powers / jnp.sum(powers, axis=-1, keepdims=True)


def attend(length, cos, sin, sums, q_out, k_out, v_out, a_out, ta_out):
    q_sum, tq_sum, kv_sum, tkv_sum = sums
    scaling = 1.0 / math.sqrt(HD)
    k = turned(kv_sum[:, 0:HD], cos, sin).astype(BF16)
    v = kv_sum[:, HD:].astype(BF16)
    tk = turned(tkv_sum[:, 0:HD], cos, sin).astype(BF16)
    tv = tkv_sum[:, HD:].astype(BF16)
    k_out[...] = k
    v_out[...] = v
    for at in range(0, q_sum.shape[1], HD):
        head = slice(at, at + HD)
        q = turned(q_sum[:, head], cos, sin).astype(BF16)
        tq = turned(tq_sum[:, head], cos, sin).astype(BF16)
        q_out[:, head] = q
        weights = attention_weights(q, k, length)
        low = weights.astype(BF16)
        a_out[:, head] = contract(low, v, 1, 0).astype(BF16)
        scores = (contract(tq, k, 1, 1) + contract(q, tk, 1, 1)) * scaling
        change = weights * (scores - jnp.sum(weights * scores, axis=-1, keepdims=True))
        ta = contract(change.astype(BF16), v, 1, 0) + contract(low, tv, 1, 0)
        ta_out[:, head] = ta.astype(BF16)


def attend_back(length, cos, sin, q_in, k, v, ga_sum, gq_out, gkv_out, gkv_low):
    scaling = 1.0 / math.sqrt(HD)
    gk, gv = None, None
    for at in range(0, ga_sum.shape[1], HD):
        head = slice(at, at + HD)
        q = q_in[:, head]
        ga = ga_sum[:, head].astype(BF16)
        weights = attention_weights(q, k, length)
        grads = contract(ga, v, 1, 1)
        value = contract(weights.astype(BF16), ga, 0, 0)
        scores = (
            weights * (grads - jnp.sum(weights * grads, axis=-1, keepdims=True)) * scaling
        ).astype(BF16)
        gq_out[:, head] = turned(contract(scores, k, 1, 0), cos, -sin).astype(BF16)
        key = contract(scores, q, 0, 0)
        gk = key if gk is None else gk + key
        gv = value if gv is None else gv + value
    gk = turned(gk, cos, -sin).astype(BF16)
    gv = gv.astype(BF16)
    half = HD // 2
    if gkv_low is not None:
        gkv_low[:, 0:HD] = gk
        gkv_low[:, HD:] = gv
    gkv_out[0] = jnp.concatenate([gk[:, 0:half], gv[:, 0:half]], axis=-1)
    gkv_out[1] = jnp.concatenate([gk[:, half:], gv[:, half:]], axis=-1)


def tiles(width, size):
    def over(function):
        @pl.loop(0, width // size)
        def _(i):
            function(pl.ds(pl.multiple_of(i * size, size), size))

    return over


def store_by_owner(part, columns, values):
    dims = part.shape[:-1] + (values.shape[1],)
    part[:, :, :, :, columns] = values.reshape(dims).astype(BF16)


def normed_kernel(tokens, gains, h_low):
    wide = tokens[...].astype(F32)
    inverse = lax.rsqrt(mean_of(wide * wide) + EPS)
    h_low[...] = (wide * inverse * gains[0:1]).astype(BF16)


def normed(tokens, gains):
    return pl.pallas_call(
        normed_kernel,
        name="normed",
        in_specs=[VMEM, VMEM],
        out_specs=VMEM,
        out_shape=shape(tokens.shape, BF16),
        cost_estimate=pl.CostEstimate(flops=10**9, bytes_accessed=0, transcendentals=0),
        compiler_params=pltpu.CompilerParams(vmem_limit_bytes=8 * 2**20),
    )(tokens, gains)


def first_kernel(*refs):
    (
        (h_low, q, k, v, o, kw, vw),
        (h_all, hs, gq, gkv, go, kv),
        (mini,),
        row_sems,
        spread_sems,
        slice_sems,
        share_sems,
        own_sems,
        probe_sems,
    ) = taken(refs, 7, 6, 1, 2, 2, 2, 2, 1, 10)
    d, t = places()
    core = lax.rem(t, 2)
    enter(HOPS)
    spread = DataSpread(h_low, mini, *spread_sems)
    rows = TensorGather(h_low, slot_of(h_all), *row_sems)
    slices = TensorGather(mini, lambda block: hs.at[:, block], *slice_sems)
    share = CoreShare((kw, vw), lambda j, c: kv.at[:, strip(j, c)], *share_sems)
    probes = Probes(LargeGather, 0, (q, k, v, o), (gq, gkv, go), probe_sems)
    own = [
        pltpu.make_async_copy(src, kv.at[:, strip(j, core)], own_sems[0].at[j])
        for j, src in enumerate((kw, vw))
    ]
    spread.start()
    rows.start()
    probes.start()
    rows.relay()
    spread.finish()
    slices.start()
    share.start()
    for copy in own:
        copy.start()
    rows.finish()
    probes.relay()
    slices.relay()
    probes.pass_on()
    slices.finish()
    share.finish()
    for copy in own:
        copy.wait()
    probes.finish()


def first(h_low, probes, kw, vw):
    half, width = h_low.shape[1:]
    return comm_call(
        first_kernel,
        "first",
        1,
        [VMEM] + [HBM] * 6,
        [VMEM] + [ANY] * 5,
        [shape((16, 2, half, width), BF16), shape((8, 16, 2, half, width // 8), BF16)]
        + Probes.shapes(probes)
        + [shape((2, 4 * kw.shape[1], width), BF16)],
        [pltpu.VMEM((8, 2, half, width // 8), BF16)]
        + TensorGather.scratch
        + DataSpread.scratch
        + TensorGather.scratch
        + CoreShare.scratch
        + [DMA((2,))]
        + Probes.scratch(LargeGather),
        (h_low,) + probes + (kw, vw),
    )


def between_kernel(*refs):
    (
        (lengths, cosine, sine, wq, kv, pq, pkv, wo, po, h_zero, tokens, gains, q, k, v, o),
        (q_out, k_out, v_out, a_out, x_out, t_out, h_all, th_all, gq, gkv, go),
        (ta_low, primal, moved, h_low, th_low),
        sums_f32,
        sum_refs,
        gather_refs,
        sems,
    ) = taken(refs, 16, 11, 5, 4, 20, 8, 10)
    d, t = places()
    width = h_zero.shape[1]
    gain = gains[1:2]
    enter(NEAR)
    lots = taken(sum_refs, 5, 5, 5, 5)
    primals = [TensorSum(r, primal, *lots[r]) for r in range(2)]
    moves = [TensorSum(r, moved, *lots[2 + r]) for r in range(2)]
    sums = [primals[0], moves[0], primals[1], moves[1]]
    lots = taken(gather_refs, 2, 2, 2, 2)
    rows_h = [TensorGather(h_low.at[r], half_slot(h_all, r), *lots[r]) for r in range(2)]
    rows_th = [TensorGather(th_low.at[r], half_slot(th_all, r), *lots[2 + r]) for r in range(2)]
    probes = Probes(DataGather, 1, (q, k, v, o), (gq, gkv, go), sems)
    probes.start()
    q_sum, tq_sum, kv_sum, tkv_sum = sums_f32
    for one in sums_f32:
        one[...] = jnp.zeros_like(one)

    @tiles(width, TILE)
    def _(at):
        h = h_zero[:, at]
        q_sum[...] += contract(h, wq[0, at], 1, 0)
        kv_sum[...] += contract(h, kv[0, :, at], 1, 1)
        tq_sum[...] += contract(h, pq[at], 1, 0)
        tkv_sum[...] += contract(h, pkv[:, at], 1, 1)

    attend(lengths[d], cosine[...], sine[...], sums_f32, q_out, k_out, v_out, a_out, ta_low)

    @tiles(width, TILE)
    def _(at):
        w = wo[0, :, at]
        store_by_owner(primal, at, contract(a_out[...], w, 1, 0))
        store_by_owner(
            moved, at, contract(ta_low[...], w, 1, 0) + contract(a_out[...], po[:, at], 1, 0)
        )

    for one in sums:
        one.start()
    for job in probes.jobs[:2]:
        job.relay()
    for one in sums:
        one.send()
    for one in sums[:2]:
        one.middle()
    for job in probes.jobs[2:]:
        job.relay()
    for r in range(2):
        stream = (tokens[r].astype(F32) + primals[r].total()).astype(BF16)
        x_out[r] = stream
        wide = stream.astype(F32)
        inverse = lax.rsqrt(mean_of(wide * wide) + EPS)
        h_low[r] = (wide * inverse * gain).astype(BF16)
        rows_h[r].start()
        tangent = moves[r].total()
        t_out[r] = tangent
        shift = mean_of(wide * tangent)
        th_low[r] = (
            gain * (tangent * inverse - wide * inverse * inverse * inverse * shift)
        ).astype(BF16)
        rows_th[r].start()
        if r == 0:
            for one in sums[2:]:
                one.middle()
            rows_h[0].relay()
    rows_th[0].relay()
    rows_h[1].relay()
    rows_th[1].relay()
    probes.pass_on()
    for one in sums:
        one.finish()
    for rows in rows_h + rows_th:
        rows.finish()
    probes.finish()


def between(lengths, tables, wq, kv, pq, pkv, wo, po, h_zero, tokens, gains, probes):
    half, width = tokens.shape[1:]
    length, columns = h_zero.shape[0], wq.shape[2]
    return comm_call(
        between_kernel,
        "between",
        2,
        [SMEM] + [VMEM] * 11 + [HBM] * 4,
        [VMEM] * 8 + [ANY] * 3,
        [
            shape((length, columns), BF16),
            shape((length, HD), BF16),
            shape((length, HD), BF16),
            shape((length, columns), BF16),
            shape((2, half, width), BF16),
            shape((2, half, width), F32),
            shape((16, 2, half, width), BF16),
            shape((16, 2, half, width), BF16),
        ]
        + Probes.shapes(probes),
        [
            pltpu.VMEM((length, columns), BF16),
            pltpu.VMEM((8, 2, 2, half, width), BF16),
            pltpu.VMEM((8, 2, 2, half, width), BF16),
            pltpu.VMEM((2, half, width), BF16),
            pltpu.VMEM((2, half, width), BF16),
            pltpu.VMEM((length, columns), F32),
            pltpu.VMEM((length, columns), F32),
            pltpu.VMEM((length, 2 * HD), F32),
            pltpu.VMEM((length, 2 * HD), F32),
        ]
        + TensorSum.scratch(width) * 4
        + TensorGather.scratch * 4
        + Probes.scratch(DataGather),
        (lengths,) + tables + (wq, kv, pq, pkv, wo, po, h_zero, tokens, gains) + probes,
        limit=16,
    )


def turn_kernel(*refs):
    (
        (lengths, cosine, sine, wq, kv, pq, pkv, wo, po, h_one, th_one, t_one, a_zero),
        (q_out, k_out, v_out, c_out, cb_all, ga_zero, ga_one, hs_one),
        (a_one, ta_low, part, c_low),
        sums_f32,
        sum_refs,
        gather_refs,
        sems,
    ) = taken(refs, 13, 8, 4, 4, 10, 4, 6)
    d, t = places()
    width = h_one.shape[1]
    enter(HOPS)
    lots = taken(sum_refs, 5, 5)
    sums = [TensorSum(r, part, *lots[r]) for r in range(2)]
    lots = taken(gather_refs, 2, 2)
    rows = [TensorGather(c_low.at[r], half_slot(cb_all, r), *lots[r]) for r in range(2)]
    jobs = [
        DataGather(a_zero, slot_of(ga_zero), *sems[0:2]),
        DataGather(a_one, slot_of(ga_one), *sems[2:4]),
    ]
    swap = DataExchange(h_one, hs_one, *sems[4:6])
    jobs[0].start()
    swap.start()
    swap.start_pairs()
    q_sum, tq_sum, kv_sum, tkv_sum = sums_f32
    for one in sums_f32:
        one[...] = jnp.zeros_like(one)

    @tiles(width, TILE)
    def _(at):
        h, th = h_one[:, at], th_one[:, at]
        w, k = wq[1, at], kv[1, :, at]
        q_sum[...] += contract(h, w, 1, 0)
        kv_sum[...] += contract(h, k, 1, 1)
        tq_sum[...] += contract(h, pq[at], 1, 0) + contract(th, w, 1, 0)
        tkv_sum[...] += contract(h, pkv[:, at], 1, 1) + contract(th, k, 1, 1)

    attend(lengths[d], cosine[...], sine[...], sums_f32, q_out, k_out, v_out, a_one, ta_low)
    jobs[1].start()
    jobs[0].relay()

    @tiles(width, TILE)
    def _(at):
        moved = contract(ta_low[...], wo[1, :, at], 1, 0) + contract(a_one[...], po[:, at], 1, 0)
        store_by_owner(part, at, moved)

    for one in sums:
        one.start()
    for one in sums:
        one.send()
    for one in sums:
        one.middle()
    half = t_one.shape[1]
    for r in range(2):
        position = (2 * t + r) * half + lax.broadcasted_iota(jnp.int32, t_one.shape[1:], 0)
        mask = jnp.where(position < lengths[d], 1.0, 0.0)
        cotangent = mask * (t_one[r] + sums[r].total())
        c_out[r] = cotangent
        c_low[r] = cotangent.astype(BF16)
        rows[r].start()
    rows[0].relay()
    jobs[1].relay()
    rows[1].relay()
    for job in jobs:
        job.pass_on()
    for r in range(2):
        sums[r].finish()
        rows[r].finish()
    swap.finish()
    for job in jobs:
        job.finish()


def turn(lengths, tables, wq, kv, pq, pkv, wo, po, h_one, th_one, t_one, a_zero):
    half, width = t_one.shape[1:]
    length, columns = a_zero.shape
    return comm_call(
        turn_kernel,
        "turn",
        3,
        [SMEM] + [VMEM] * 12,
        [VMEM] * 5 + [ANY] * 3,
        [
            shape((length, columns), BF16),
            shape((length, HD), BF16),
            shape((length, HD), BF16),
            shape((2, half, width), F32),
            shape((16, 2, half, width), BF16),
            shape((8,) + a_zero.shape, BF16),
            shape((8,) + a_zero.shape, BF16),
            shape((8, length, width // 8), BF16),
        ],
        [
            pltpu.VMEM((length, columns), BF16),
            pltpu.VMEM((length, columns), BF16),
            pltpu.VMEM((8, 2, 2, half, width), BF16),
            pltpu.VMEM((2, half, width), BF16),
            pltpu.VMEM((length, columns), F32),
            pltpu.VMEM((length, columns), F32),
            pltpu.VMEM((length, 2 * HD), F32),
            pltpu.VMEM((length, 2 * HD), F32),
        ]
        + TensorSum.scratch(width) * 2
        + TensorGather.scratch * 2
        + DataGather.scratch * 2
        + DataExchange.scratch,
        (lengths,) + tables + (wq, kv, pq, pkv, wo, po, h_one, th_one, t_one, a_zero),
    )


class Cotangents:
    def __init__(self, gq, gkv, gathered, came, merged, sems):
        self.gkv, self.came, self.merged = gkv, came, merged
        width = gq.shape[1]
        self.jobs = [
            DataGather(gq, lambda block: gathered.at[block, :, 0:width], *sems[0:2]),
            DataGather(
                merged,
                lambda block: gathered.at[block, :, width : width + merged.shape[1]],
                *sems[2:4],
            ),
        ]
        self.sends, self.recvs = sems[4:6]

    @staticmethod
    def scratch(gkv):
        return (
            [pltpu.VMEM(gkv.shape[1:], BF16)] * 2
            + DataGather.scratch * 2
            + [DMA((1,)), DMA((1,))]
        )

    def swap(self):
        d, t = places()
        return remote(
            self.gkv.at[1 - lax.rem(t, 2)],
            self.came,
            self.sends,
            self.recvs,
            0,
            (d, other_core(t)),
        )

    def start(self):
        self.swap().start()
        self.jobs[0].start()

    def merge(self):
        d, t = places()
        self.swap().wait()
        mine = self.gkv[lax.rem(t, 2)].astype(F32) + self.came[...].astype(F32)
        self.merged[...] = mine.astype(BF16)
        self.jobs[1].start()

    def relay(self):
        for job in self.jobs:
            job.relay()

    def pass_on(self):
        for job in self.jobs:
            job.pass_on()

    def finish(self):
        for job in self.jobs:
            job.finish()


def lower_kernel(*refs):
    (
        (lengths, cosine, sine, q, k, v, cb_one, wo, wq, kv, c_two, x_one, gains),
        (cb_all, gg, cbs, mini),
        (ga_sum, gq, gkv, gkv_low, part, c_low),
        sum_refs,
        gather_refs,
        (came, merged),
        sems,
        swap_sems,
        spread_sems,
    ) = taken(refs, 13, 4, 6, 10, 4, 2, 6, 2, 2)
    d, t = places()
    width = cb_one.shape[1]
    enter(HOPS)
    lots = taken(sum_refs, 5, 5)
    sums = [TensorSum(r, part, *lots[r]) for r in range(2)]
    lots = taken(gather_refs, 2, 2)
    rows = [TensorGather(c_low.at[r], half_slot(cb_all, r), *lots[r]) for r in range(2)]
    jobs = Cotangents(gq, gkv, gg, came, merged, sems)
    swap = DataExchange(cb_one, cbs, *swap_sems)
    swap.start()
    swap.start_pairs()
    ga_sum[...] = jnp.zeros_like(ga_sum)

    @tiles(width, TILE)
    def _(at):
        ga_sum[...] += contract(cb_one[:, at], wo[1, :, at], 1, 1)

    attend_back(
        lengths[d], cosine[...], sine[...], q, k[...], v[...], ga_sum, gq, gkv, gkv_low
    )
    jobs.start()

    @tiles(width, TILE)
    def _(at):
        term = contract(gq[...], wq[1, at], 1, 1) + contract(gkv_low[...], kv[1, :, at], 1, 0)
        store_by_owner(part, at, term)

    for one in sums:
        one.start()
    jobs.merge()
    for one in sums:
        one.send()
    for one in sums:
        one.middle()
    for r in range(2):
        scaled = sums[r].total() * gains[1:2]
        wide = x_one[r].astype(F32)
        inverse = lax.rsqrt(mean_of(wide * wide) + EPS)
        shift = mean_of(wide * scaled)
        cotangent = c_two[r] + inverse * (scaled - wide * inverse * inverse * shift)
        c_low[r] = cotangent.astype(BF16)
        rows[r].start()
    spread = DataSpread(c_low, mini, *spread_sems)
    spread.start()
    for one in rows:
        one.relay()
    jobs.relay()
    jobs.pass_on()
    for r in range(2):
        sums[r].finish()
        rows[r].finish()
    swap.finish()
    spread.finish()
    jobs.finish()


def lower(lengths, tables, q, k, v, cb_one, wo, wq, kv, c_two, x_one, gains):
    half, width = c_two.shape[1:]
    length, columns = q.shape
    gkv = shape((2, length, HD), BF16)
    return comm_call(
        lower_kernel,
        "lower",
        4,
        [SMEM] + [VMEM] * 12,
        [VMEM] + [ANY] * 3,
        [
            shape((16, 2, half, width), BF16),
            shape((8, length, columns + HD), BF16),
            shape((8, length, width // 8), BF16),
            shape((8, 2, half, width // 8), BF16),
        ],
        [
            pltpu.VMEM((length, columns), F32),
            pltpu.VMEM((length, columns), BF16),
            pltpu.VMEM(gkv.shape, BF16),
            pltpu.VMEM((length, 2 * HD), BF16),
            pltpu.VMEM((8, 2, 2, half, width), BF16),
            pltpu.VMEM((2, half, width), BF16),
        ]
        + TensorSum.scratch(width) * 2
        + TensorGather.scratch * 2
        + Cotangents.scratch(gkv)
        + DataExchange.scratch
        + DataSpread.scratch,
        (lengths,) + tables + (q, k, v, cb_one, wo, wq, kv, c_two, x_one, gains),
    )


def inner(hs, gathered, g_sum):
    g_sum[...] = jnp.zeros_like(g_sum)

    @pl.loop(0, 4)
    def _(i):
        g = gathered[pl.ds(2 * i, 2)].reshape(-1, gathered.shape[2])
        h = hs[pl.ds(2 * i, 2)].reshape(-1, hs.shape[2])
        g_sum[...] += contract(g, h, 0, 0)


def outer(ga, cs, o_sum):
    o_sum[...] = jnp.zeros_like(o_sum)

    @pl.loop(0, 4)
    def _(i):
        a = ga[pl.ds(2 * i, 2)].reshape(-1, ga.shape[2])
        c = cs[pl.ds(2 * i, 2)].reshape(-1, cs.shape[2])
        o_sum[...] += contract(a, c, 0, 0)


def last_kernel(*refs):
    (
        (lengths, cosine, sine, q, k, v, cb, wo, mini, hs, gg_one, ga, cs),
        (gg, cs_zero, q_out, g_sum, o_sum),
        (ga_sum, gq, gkv),
        (came, merged),
        sems,
        slice_sems,
    ) = taken(refs, 13, 5, 3, 2, 6, 2)
    d, t = places()
    width, columns = cb.shape[1], gq.shape[1]
    enter(NEAR)
    slices = TensorGather(mini, lambda block: cs_zero.at[:, block], *slice_sems)
    jobs = Cotangents(gq, gkv, gg, came, merged, sems)
    slices.start()
    ga_sum[...] = jnp.zeros_like(ga_sum)

    @tiles(width, TILE)
    def _(at):
        ga_sum[...] += contract(cb[:, at], wo[0, :, at], 1, 1)

    attend_back(lengths[d], cosine[...], sine[...], q, k[...], v[...], ga_sum, gq, gkv, None)
    jobs.start()
    slices.relay()
    jobs.merge()
    inner(hs, gg_one, g_sum)
    q_out[...] = g_sum[0:columns].T
    jobs.relay()
    outer(ga, cs, o_sum)
    jobs.pass_on()
    slices.finish()
    jobs.finish()


def last(lengths, tables, q, k, v, cb, wo, mini, *sides):
    length, columns = q.shape
    share = mini.shape[3]
    gkv = shape((2, length, HD), BF16)
    return comm_call(
        last_kernel,
        "last",
        5,
        [SMEM] + [VMEM] * 12,
        [ANY] * 2 + [VMEM] * 3,
        [
            shape((8, length, columns + HD), BF16),
            shape((8, 16) + mini.shape[1:], BF16),
            shape((share, columns), F32),
            shape((columns + HD, share), F32),
            shape((columns, share), F32),
        ],
        [
            pltpu.VMEM((length, columns), F32),
            pltpu.VMEM((length, columns), BF16),
            pltpu.VMEM(gkv.shape, BF16),
        ]
        + Cotangents.scratch(gkv)
        + TensorGather.scratch,
        (lengths,) + tables + (q, k, v, cb, wo, mini) + sides,
    )


def products_kernel(hs, gg, ga, cs, q_one, g_one, o_one, q_out, k_out, v_out, o_out, g_sum):
    columns, half = q_out.shape[2], k_out.shape[1]
    inner(hs, gg, g_sum)
    outer(ga, cs, o_out.at[0])
    q_out[0] = g_sum[0:columns].T
    q_out[1] = q_one[...]
    o_out[1] = o_one[...]
    for layer, one in ((0, g_sum), (1, g_one)):
        k_out[layer] = one[columns : columns + half]
        v_out[layer] = one[columns + half :]


def products(*operands):
    share, columns = operands[4].shape
    half = (operands[1].shape[2] - columns) // 2
    return pl.pallas_call(
        products_kernel,
        name="products",
        in_specs=[VMEM] * 7,
        out_specs=[VMEM] * 4,
        out_shape=[
            shape((2, share, columns), F32),
            shape((2, half, share), F32),
            shape((2, half, share), F32),
            shape((2, columns, share), F32),
        ],
        scratch_shapes=[pltpu.VMEM(operands[5].shape, F32)],
        compiler_params=pltpu.CompilerParams(vmem_limit_bytes=14 * 2**20),
    )(*operands)


def rope_tables():
    angles = np.arange(LEN)[:, None] * THETA ** (-2.0 * np.arange(HD // 2) / HD)[None, :]
    cosine, sine = np.cos(angles), np.sin(angles)
    return (
        jnp.asarray(np.concatenate([cosine, cosine], axis=1), F32),
        jnp.asarray(np.concatenate([-sine, sine], axis=1), F32),
    )


def body(
    tokens,
    lengths,
    gains,
    query_weight,
    key_weight,
    value_weight,
    out_weight,
    query_probe,
    key_probe,
    value_probe,
    out_probe,
):
    rows, width = tokens.shape
    tables = rope_tables()

    def turned_over(array):
        return jnp.swapaxes(array, 1, 2)

    tokens = tokens.reshape(2, rows // 2, width)

    def all_rows(blocks):
        return blocks.reshape(-1, blocks.shape[-1])

    def by_batch(blocks):
        return blocks.reshape(blocks.shape[0], -1, blocks.shape[-1])

    probes = (query_probe, turned_over(key_probe), turned_over(value_probe), out_probe)
    h_zero, hs_zero, pq, pkv, po, kv = first(
        normed(tokens, gains), probes, turned_over(key_weight), turned_over(value_weight)
    )
    q0, k0, v0, a_zero, x_one, t_one, h_one, th_one, pq, pkv, po = between(
        lengths,
        tables,
        query_weight,
        kv,
        all_rows(pq),
        pkv,
        out_weight,
        po,
        all_rows(h_zero),
        tokens,
        gains,
        probes,
    )
    q1, k1, v1, c_two, cb_one, ga_zero, ga_one, hs_one = turn(
        lengths,
        tables,
        query_weight,
        kv,
        all_rows(pq),
        pkv,
        out_weight,
        po,
        all_rows(h_one),
        all_rows(th_one),
        t_one,
        a_zero,
    )
    cb_zero, gg_one, cs_one, mini = lower(
        lengths,
        tables,
        q1,
        k1,
        v1,
        all_rows(cb_one),
        out_weight,
        query_weight,
        kv,
        c_two,
        x_one,
        gains,
    )
    gg_zero, cs_zero, q_one, g_one, o_one = last(
        lengths,
        tables,
        q0,
        k0,
        v0,
        all_rows(cb_zero),
        out_weight,
        mini,
        hs_one,
        gg_one,
        ga_one,
        cs_one,
    )
    q, k, v, o = products(
        by_batch(hs_zero), gg_zero, ga_zero, by_batch(cs_zero), q_one, g_one, o_one
    )
    return (q, turned_over(k), turned_over(v), o)


def solution(mesh):
    placed = (
        P(("dp", "tensor"), None),
        P(),
        P(),
        P(None, None, "tensor"),
        P(None, None, "tensor"),
        P(None, None, "tensor"),
        P(None, "tensor", None),
        P(None, "dp", "tensor"),
        P(None, "dp", "tensor"),
        P(None, "dp", "tensor"),
        P(None, "tensor", "dp"),
    )
    return jax.shard_map(
        body,
        mesh=mesh,
        in_specs=placed,
        out_specs=(
            P(None, "dp", "tensor"),
            P(None, "dp", "tensor"),
            P(None, "dp", "tensor"),
            P(None, "tensor", "dp"),
        ),
        check_vma=False,
    )
```

```python
import functools
import math

import jax
import jax.numpy as jnp
import numpy as np
from jax import lax
from jax.experimental import pallas as pl
from jax.experimental.pallas import tpu as pltpu
from jax.sharding import PartitionSpec as P

HD = 128
LEN = 256
EPS = 1e-05
THETA = 500000.0

MESH = pl.DeviceIdType.MESH
F32 = jnp.float32
BF16 = jnp.bfloat16
VMEM = pl.BlockSpec(memory_space=pltpu.VMEM)
ANY = pl.BlockSpec(memory_space=pl.ANY)
HBM = pl.BlockSpec(memory_space=pltpu.HBM)
SMEM = pl.BlockSpec(memory_space=pltpu.SMEM)
DMA = pltpu.SemaphoreType.DMA
TILE = 1024

HOPS = ((1, 1), (3, 1), (2, 1), (2, 0), (1, 0), (3, 0), (0, 1))
NEAR = HOPS[3:]


def back(hop):
    return ((4 - hop[0]) % 4, hop[1])


def data_at(d, hop):
    ring, pair = lax.div(d, 2), lax.rem(d, 2)
    return lax.rem(ring + hop[0], 4) * 2 + lax.rem(pair + hop[1], 2)


def chip_at(t, hop):
    return data_at(lax.div(t, 2), hop)


def tensor_at(t, hop):
    return chip_at(t, hop) * 2 + lax.rem(t, 2)


def other_core(t):
    return t + 1 - 2 * lax.rem(t, 2)


def places():
    return lax.axis_index("dp"), lax.axis_index("tensor")


def remote(src, dst, sends, recvs, j, device):
    return pltpu.make_async_remote_copy(
        src_ref=src,
        dst_ref=dst,
        send_sem=sends.at[j],
        recv_sem=recvs.at[j],
        device_id=device,
        device_id_type=MESH,
    )


def enter(data_hops):
    d, t = places()
    barrier = pltpu.get_barrier_semaphore()
    peers = [(d, other_core(t))]
    peers += [(d, tensor_at(t, hop)) for hop in NEAR]
    peers += [(data_at(d, hop), t) for hop in data_hops]
    for peer in peers:
        pl.semaphore_signal(barrier, inc=1, device_id=peer, device_id_type=MESH)
    pl.semaphore_wait(barrier, len(peers))


def half_of(ref, half):
    if half is None:
        return ref
    rows = ref.shape[0] // 2
    return ref.at[pl.ds(half * rows, rows)]


class RingGather:
    ROUTES = ()
    FIRST = 0

    def __init__(self, src, slot, sends, recvs):
        self.src, self.slot, self.sends, self.recvs = src, slot, sends, recvs

    def out(self, j):
        hop, block, unused, half = self.ROUTES[j]
        slot = half_of(self.slot(self.place(block)), half)
        src = self.src if j < self.FIRST else slot
        return remote(src, slot, self.sends, self.recvs, j, self.device(hop))

    def into(self, j):
        slot = half_of(self.slot(self.place(self.ROUTES[j][2])), self.ROUTES[j][3])
        return remote(slot, slot, self.sends, self.recvs, j, self.device((0, 1)))

    def own(self):
        n = len(self.ROUTES)
        return pltpu.make_async_copy(self.src, self.slot(self.place((0, 0))), self.sends.at[n])

    def start(self):
        for j in range(self.FIRST):
            self.out(j).start()
        self.own().start()

    def sent(self):
        for j in range(len(self.ROUTES)):
            self.out(j).wait_send()
        self.own().wait()


class DataGather(RingGather):
    scratch = [DMA((8,)), DMA((7,))]
    FIRST = 4
    ROUTES = (
        ((0, 1), (0, 0), (0, 1), None),
        ((1, 0), (0, 0), (3, 0), None),
        ((3, 0), (0, 0), (1, 0), None),
        ((2, 0), (0, 0), (2, 0), None),
        ((1, 0), (0, 1), (3, 1), None),
        ((3, 0), (0, 1), (1, 1), None),
        ((0, 1), (2, 0), (2, 1), None),
    )

    def place(self, hop):
        d, t = places()
        return data_at(d, hop)

    def device(self, hop):
        d, t = places()
        return (data_at(d, hop), t)

    def relay(self):
        self.into(0).wait_recv()
        self.out(4).start()
        self.out(5).start()

    def pass_on(self):
        self.into(3).wait_recv()
        self.out(6).start()

    def finish(self):
        for j in (1, 2, 4, 5, 6):
            self.into(j).wait_recv()
        self.sent()


class LargeGather(DataGather):
    scratch = [DMA((12,)), DMA((11,))]
    FIRST = 3
    ROUTES = (
        ((0, 1), (0, 0), (0, 1), None),
        ((1, 0), (0, 0), (3, 0), None),
        ((3, 0), (0, 0), (1, 0), None),
        ((1, 0), (0, 1), (3, 1), 0),
        ((3, 0), (0, 1), (1, 1), 1),
        ((1, 0), (3, 0), (2, 0), 0),
        ((0, 1), (3, 0), (3, 1), 1),
        ((3, 0), (1, 0), (2, 0), 1),
        ((0, 1), (1, 0), (1, 1), 0),
        ((1, 0), (3, 1), (2, 1), 0),
        ((3, 0), (1, 1), (2, 1), 1),
    )

    def start_ring(self):
        self.out(1).start()
        self.out(2).start()
        self.own().start()

    def start_pair(self):
        self.out(0).start()

    def relay_ring(self):
        self.into(0).wait_recv()
        self.out(3).start()
        self.out(4).start()
        self.into(1).wait_recv()
        self.out(5).start()
        self.into(2).wait_recv()
        self.out(7).start()

    def relay_pair(self):
        self.out(6).start()
        self.out(8).start()

    def relay(self):
        self.relay_ring()
        self.relay_pair()

    def pass_on(self):
        for j in (3, 4):
            self.into(j).wait_recv()
            self.out(6 + j).start()

    def finish(self):
        for j in range(5, 11):
            self.into(j).wait_recv()
        self.sent()


class TensorGather(RingGather):
    scratch = [DMA((16,)), DMA((15,))]
    FIRST = 4
    ROUTES = (
        ((0, 1), (0, 0), (0, 1), None),
        ((1, 0), (0, 0), (3, 0), None),
        ((3, 0), (0, 0), (1, 0), None),
        ((2, 0), (0, 0), (2, 0), None),
        ((1, 0), (0, 1), (3, 1), None),
        ((3, 0), (0, 1), (1, 1), None),
        ((2, 0), (0, 1), (2, 1), None),
    )

    def place(self, hop):
        d, t = places()
        return tensor_at(t, hop)

    def device(self, hop):
        d, t = places()
        return (d, tensor_at(t, hop))

    def handover(self, j, src, block):
        d, t = places()
        return pltpu.make_async_remote_copy(
            src_ref=src,
            dst_ref=self.slot(block),
            send_sem=self.sends.at[8 + j],
            recv_sem=self.recvs.at[7 + j],
            device_id=(d, other_core(t)),
            device_id_type=MESH,
        )

    def hand(self, j):
        block = self.place(self.ROUTES[j][2])
        return self.handover(j, self.slot(block), block)

    def near(self):
        return self.handover(7, self.src, self.place((0, 0)))

    def start(self):
        super().start()
        self.near().start()

    def relay(self):
        self.into(0).wait_recv()
        for j in range(4, 7):
            self.out(j).start()
        self.hand(0).start()

    def finish(self):
        for j in range(1, 7):
            self.into(j).wait_recv()
            self.hand(j).start()
        self.sent()
        d, t = places()
        far = other_core(t)
        self.handover(7, self.slot(far), far).wait_recv()
        self.near().wait_send()
        for j in range(7):
            block = tensor_at(far, self.ROUTES[j][2])
            self.handover(j, self.slot(block), block).wait_recv()
            self.hand(j).wait_send()


class TensorSum:
    STEPS = ((2, 1), (1, 1), (3, 1), (2, 0), (1, 0), (3, 0))
    BLOCKS = STEPS + ((0, 1), (0, 0))

    @staticmethod
    def scratch(columns):
        return [
            pltpu.VMEM((8, 8, columns), BF16),
            pltpu.VMEM((7, 8, columns), BF16),
            pltpu.VMEM((7, 8, columns), BF16),
            DMA((15,)),
            DMA((15,)),
        ]

    def __init__(self, rows, part, near, sent, far, sends, recvs):
        self.rows = rows
        self.part, self.near_, self.sent, self.far = part, near, sent, far
        self.sends, self.recvs = sends, recvs

    def swap(self, j):
        d, t = places()
        k = chip_at(t, self.BLOCKS[j])
        c = lax.rem(t, 2)
        return remote(
            self.part.at[k, 1 - c, self.rows], self.near_.at[k], self.sends, self.recvs, j, (d, other_core(t))
        )

    def cross(self, j):
        d, t = places()
        hop = (self.STEPS[j][0], 0) if j < 6 else (0, 1)
        return remote(
            self.sent.at[j], self.far.at[j], self.sends, self.recvs, 8 + j, (d, tensor_at(t, hop))
        )

    def pair_sum(self, j):
        d, t = places()
        k = chip_at(t, self.BLOCKS[j])
        c = lax.rem(t, 2)
        return self.part[k, c, self.rows].astype(F32) + self.near_[k].astype(F32)

    def start(self):
        for j in range(8):
            self.swap(j).start()

    def send(self):
        for j in range(6):
            self.swap(j).wait_recv()
            self.sent[j] = self.pair_sum(j).astype(BF16)
            self.cross(j).start()

    def middle(self):
        self.swap(6).wait_recv()
        total = self.pair_sum(6)
        for j in (1, 2, 0):
            self.cross(j).wait_recv()
            total = total + self.far[j].astype(F32)
        self.sent[6] = total.astype(BF16)
        self.cross(6).start()

    def total(self):
        self.swap(7).wait_recv()
        total = self.pair_sum(7)
        for j in (4, 5, 3, 6):
            self.cross(j).wait_recv()
            total = total + self.far[j].astype(F32)
        return total

    def finish(self):
        for j in range(8):
            self.swap(j).wait_send()
        for j in range(7):
            self.cross(j).wait_send()


class DataSpread:
    scratch = [DMA((8,)), DMA((7,))]

    def __init__(self, src, out, sends, recvs):
        self.src, self.out_, self.sends, self.recvs = src, out, sends, recvs
        self.share = src.shape[-1] // 8

    def columns(self, d):
        return pl.ds(pl.multiple_of(d * self.share, self.share), self.share)

    def cut(self, d):
        return self.src.at[(slice(None),) * (len(self.src.shape) - 1) + (self.columns(d),)]

    def cross(self, j):
        d, t = places()
        peer = data_at(d, HOPS[j])
        return remote(
            self.cut(peer),
            self.out_.at[d],
            self.sends,
            self.recvs,
            j,
            (peer, t),
        )

    def arrived(self, j):
        d, t = places()
        slot = self.out_.at[data_at(d, back(HOPS[j]))]
        return remote(slot, slot, self.sends, self.recvs, j, (d, other_core(t)))

    def own(self):
        d, t = places()
        return pltpu.make_async_copy(
            self.cut(d), self.out_.at[d], self.sends.at[7]
        )

    def start(self):
        for j in range(7):
            self.cross(j).start()
        self.own().start()

    def finish(self):
        for j in range(7):
            self.arrived(j).wait_recv()
            self.cross(j).wait_send()
        self.own().wait()


class DataExchange:
    scratch = [DMA((15,)), DMA((14,))]

    def __init__(self, src, out, sends, recvs):
        self.src, self.out_, self.sends, self.recvs = src, out, sends, recvs
        self.half = src.shape[0] // 2
        self.share = src.shape[1] // 8

    def rows(self, t):
        return pl.ds(pl.multiple_of(lax.rem(t, 2) * self.half, self.half), self.half)

    def columns(self, d):
        return pl.ds(pl.multiple_of(d * self.share, self.share), self.share)

    def cross(self, j):
        d, t = places()
        peer = data_at(d, HOPS[j])
        return remote(
            self.src.at[self.rows(t), self.columns(peer)],
            self.out_.at[d, self.rows(t)],
            self.sends,
            self.recvs,
            j,
            (peer, t),
        )

    def hand(self, j, t_of):
        d, t = places()
        slot = self.out_.at[data_at(d, back(HOPS[j])), self.rows(t_of)]
        return slot

    def arrived(self, j):
        d, t = places()
        slot = self.hand(j, t)
        return remote(slot, slot, self.sends, self.recvs, j, (d, other_core(t)))

    def handed(self, j):
        d, t = places()
        slot = self.hand(j, t)
        return remote(slot, slot, self.sends, self.recvs, 7 + j, (d, other_core(t)))

    def received(self, j):
        d, t = places()
        slot = self.hand(j, other_core(t))
        return remote(slot, slot, self.sends, self.recvs, 7 + j, (d, other_core(t)))

    def own(self):
        d, t = places()
        return pltpu.make_async_copy(
            self.src.at[:, self.columns(d)], self.out_.at[d], self.sends.at[14]
        )

    def start(self):
        for j in (3, 4, 5):
            self.cross(j).start()
        self.own().start()

    def start_pairs(self):
        for j in (6, 0, 1, 2):
            self.cross(j).start()

    def finish(self):
        for j in (4, 5, 3, 6, 0, 1, 2):
            self.arrived(j).wait_recv()
            self.handed(j).start()
        for j in range(7):
            self.received(j).wait_recv()
            self.cross(j).wait_send()
            self.handed(j).wait_send()
        self.own().wait()


def taken(refs, *counts):
    out, at = [], 0
    for count in counts:
        out.append(refs[at : at + count])
        at += count
    return out


def comm_call(kernel, name, number, in_specs, out_specs, out_shape, scratch, args, limit=12):
    return pl.pallas_call(
        kernel,
        name=name,
        in_specs=in_specs,
        out_specs=out_specs,
        out_shape=out_shape,
        scratch_shapes=scratch,
        cost_estimate=pl.CostEstimate(flops=10**10, bytes_accessed=0, transcendentals=0),
        compiler_params=pltpu.CompilerParams(
            collective_id=number, has_side_effects=True, vmem_limit_bytes=limit * 2**20
        ),
    )(*args)


def shape(dims, dtype):
    return jax.ShapeDtypeStruct(dims, dtype)


def slot_of(ref):
    return lambda block: ref.at[block]


def rows_of(ref, count):
    size = ref.shape[0] // count
    return lambda block: ref.at[pl.ds(pl.multiple_of(block * size, size), size)]


def half_slot(ref, half):
    return lambda block: ref.at[block, half]


def columns_of(ref):
    width = ref.shape[1] // 8
    return lambda block: ref.at[:, pl.ds(pl.multiple_of(block * width, width), width)]


def mean_of(values):
    return jnp.sum(values, axis=-1, keepdims=True) * (1.0 / values.shape[-1])


def strip(which, core):
    return pl.ds(pl.multiple_of(which * 128 + core * 64, 64), 64)


class CoreShare:
    scratch = [DMA((2,)), DMA((2,))]

    def __init__(self, sources, slot, sends, recvs):
        self.sources, self.slot, self.sends, self.recvs = sources, slot, sends, recvs

    def copy(self, j, core):
        d, t = places()
        slot = self.slot(j, core)
        src = slot if self.sources is None else self.sources[j]
        return remote(src, slot, self.sends, self.recvs, j, (d, other_core(t)))

    def start(self):
        d, t = places()
        for j in range(2):
            self.copy(j, lax.rem(t, 2)).start()

    def finish(self):
        d, t = places()
        for j in range(2):
            self.copy(j, 1 - lax.rem(t, 2)).wait_recv()
            self.copy(j, lax.rem(t, 2)).wait_send()


class Probes:
    COUNT = 4
    @staticmethod
    def scratch(kind):
        return kind.scratch * 4 + CoreShare.scratch

    def __init__(self, kind, layer, probes, gathered, sems):
        q, k, v, o = probes
        gq, gkv, go = gathered
        d, t = places()
        core = lax.rem(t, 2)
        width = k.shape[2]

        def part(which):
            return lambda block: gkv.at[
                strip(which, core), pl.ds(pl.multiple_of(block * width, width), width)
            ]

        self.jobs = [
            kind(k.at[layer], part(0), *sems[0:2]),
            kind(v.at[layer], part(1), *sems[2:4]),
            kind(q.at[layer], rows_of(gq, 8), *sems[4:6]),
            kind(o.at[layer], columns_of(go), *sems[6:8]),
        ]
        self.share = CoreShare(None, lambda j, c: gkv.at[strip(j, c)], *sems[8:10])

    @staticmethod
    def shapes(probes):
        q, k, v, o = probes
        return [
            shape((8 * q.shape[1], q.shape[2]), BF16),
            shape((4 * k.shape[1], 8 * k.shape[2]), BF16),
            shape((o.shape[1], 8 * o.shape[2]), BF16),
        ]

    def start(self):
        for job in self.jobs:
            job.start()

    def relay(self):
        for job in self.jobs:
            job.relay()

    def pass_on(self):
        for job in self.jobs:
            job.pass_on()

    def finish(self):
        for job in self.jobs[:2]:
            job.finish()
        self.share.start()
        for job in self.jobs[2:]:
            job.finish()
        self.share.finish()


def contract(left_side, right_side, left_dim, right_dim):
    return lax.dot_general(
        left_side,
        right_side,
        (((left_dim,), (right_dim,)), ((), ())),
        preferred_element_type=F32,
    )


def turned(values, cosine, sine):
    return values * cosine + pltpu.roll(values, values.shape[1] // 2, 1) * sine


def attention_weights(q, k, length):
    size = q.shape[0]
    row = lax.broadcasted_iota(jnp.int32, (size, size), 0)
    column = lax.broadcasted_iota(jnp.int32, (size, size), 1)
    allowed = (column <= row) & (column < length)
    scores = contract(q, k, 1, 1) * (1.0 / math.sqrt(q.shape[1]))
    powers = jnp.where(allowed, jnp.exp(scores), 0.0)
    return powers / jnp.sum(powers, axis=-1, keepdims=True)


def attend(length, cos, sin, sums, q_out, k_out, v_out, a_out, ta_out):
    q_sum, tq_sum, kv_sum, tkv_sum = sums
    scaling = 1.0 / math.sqrt(HD)
    k = turned(kv_sum[:, 0:HD], cos, sin).astype(BF16)
    v = kv_sum[:, HD:].astype(BF16)
    tk = turned(tkv_sum[:, 0:HD], cos, sin).astype(BF16)
    tv = tkv_sum[:, HD:].astype(BF16)
    k_out[...] = k
    v_out[...] = v
    for at in range(0, q_sum.shape[1], HD):
        head = slice(at, at + HD)
        q = turned(q_sum[:, head], cos, sin).astype(BF16)
        tq = turned(tq_sum[:, head], cos, sin).astype(BF16)
        q_out[:, head] = q
        weights = attention_weights(q, k, length)
        low = weights.astype(BF16)
        a_out[:, head] = contract(low, v, 1, 0).astype(BF16)
        scores = (contract(tq, k, 1, 1) + contract(q, tk, 1, 1)) * scaling
        change = weights * (scores - jnp.sum(weights * scores, axis=-1, keepdims=True))
        ta = contract(change.astype(BF16), v, 1, 0) + contract(low, tv, 1, 0)
        ta_out[:, head] = ta.astype(BF16)


def attend_primal(length, cos, sin, q_sum, kv_sum, q_out, k_out, v_out, a_out, w_out):
    k = turned(kv_sum[:, 0:HD], cos, sin).astype(BF16)
    v = kv_sum[:, HD:].astype(BF16)
    k_out[...] = k
    v_out[...] = v
    for n, at in enumerate(range(0, q_sum.shape[1], HD)):
        head = slice(at, at + HD)
        q = turned(q_sum[:, head], cos, sin).astype(BF16)
        q_out[:, head] = q
        weights = attention_weights(q, k, length)
        w_out[n] = weights
        a_out[:, head] = contract(weights.astype(BF16), v, 1, 0).astype(BF16)


def attend_tangent(cos, sin, tq_sum, tkv_sum, q_in, k, v, w_in, ta_out):
    scaling = 1.0 / math.sqrt(HD)
    tk = turned(tkv_sum[:, 0:HD], cos, sin).astype(BF16)
    tv = tkv_sum[:, HD:].astype(BF16)
    for n, at in enumerate(range(0, tq_sum.shape[1], HD)):
        head = slice(at, at + HD)
        tq = turned(tq_sum[:, head], cos, sin).astype(BF16)
        weights = w_in[n]
        low = weights.astype(BF16)
        scores = (contract(tq, k, 1, 1) + contract(q_in[:, head], tk, 1, 1)) * scaling
        change = weights * (scores - jnp.sum(weights * scores, axis=-1, keepdims=True))
        ta = contract(change.astype(BF16), v, 1, 0) + contract(low, tv, 1, 0)
        ta_out[:, head] = ta.astype(BF16)


def attend_back(length, cos, sin, q_in, k, v, ga_sum, gq_out, gkv_out, gkv_low):
    scaling = 1.0 / math.sqrt(HD)
    gk, gv = None, None
    for at in range(0, ga_sum.shape[1], HD):
        head = slice(at, at + HD)
        q = q_in[:, head]
        ga = ga_sum[:, head].astype(BF16)
        weights = attention_weights(q, k, length)
        grads = contract(ga, v, 1, 1)
        value = contract(weights.astype(BF16), ga, 0, 0)
        scores = (
            weights * (grads - jnp.sum(weights * grads, axis=-1, keepdims=True)) * scaling
        ).astype(BF16)
        gq_out[:, head] = turned(contract(scores, k, 1, 0), cos, -sin).astype(BF16)
        key = contract(scores, q, 0, 0)
        gk = key if gk is None else gk + key
        gv = value if gv is None else gv + value
    gk = turned(gk, cos, -sin).astype(BF16)
    gv = gv.astype(BF16)
    half = HD // 2
    if gkv_low is not None:
        gkv_low[:, 0:HD] = gk
        gkv_low[:, HD:] = gv
    gkv_out[0] = jnp.concatenate([gk[:, 0:half], gv[:, 0:half]], axis=-1)
    gkv_out[1] = jnp.concatenate([gk[:, half:], gv[:, half:]], axis=-1)


def tiles(width, size):
    def over(function):
        @pl.loop(0, width // size)
        def _(i):
            function(pl.ds(pl.multiple_of(i * size, size), size))

    return over


def store_by_owner(part, columns, values):
    dims = part.shape[:-1] + (values.shape[1],)
    part[:, :, :, :, columns] = values.reshape(dims).astype(BF16)


def normed_kernel(tokens, gains, h_low):
    wide = tokens[...].astype(F32)
    inverse = lax.rsqrt(mean_of(wide * wide) + EPS)
    h_low[...] = (wide * inverse * gains[0:1]).astype(BF16)


def normed(tokens, gains):
    return pl.pallas_call(
        normed_kernel,
        name="normed",
        in_specs=[VMEM, VMEM],
        out_specs=VMEM,
        out_shape=shape(tokens.shape, BF16),
        cost_estimate=pl.CostEstimate(flops=10**10, bytes_accessed=0, transcendentals=0),
        compiler_params=pltpu.CompilerParams(vmem_limit_bytes=8 * 2**20),
    )(tokens, gains)


def head_kernel(*refs):
    (
        (lengths, cosine, sine, h_low, wq, wo, tokens, gains, kw, vw, q, k, v, o),
        (q_out, k_out, v_out, a_out, x_out, t_out, h_all, th_all, kv, hs, gq, gkv, go),
        (mini, h_zero, pq, pkv, po, weights, ta_low, part, h_one, th_one),
        sums_f32,
        sum_refs,
        gather_refs,
        spread_sems,
        share_sems,
        own_sems,
        zero_sems,
        one_sems,
    ) = taken(refs, 14, 13, 10, 4, 20, 12, 2, 2, 1, 10, 10)
    d, t = places()
    core = lax.rem(t, 2)
    width = h_zero.shape[1]
    gain = gains[1:2]
    cos, sin = cosine[...], sine[...]
    enter(HOPS)
    lots = taken(sum_refs, 5, 5, 5, 5)
    primals = [TensorSum(r, part, *lots[r]) for r in range(2)]
    moves = [TensorSum(r, part, *lots[2 + r]) for r in range(2)]
    lots = taken(gather_refs, 2, 2, 2, 2, 2, 2)
    rows = TensorGather(h_low, rows_of(h_zero, 16), *lots[0])
    slices = TensorGather(mini, lambda block: hs.at[:, block], *lots[1])
    rows_h = [TensorGather(h_one.at[r], half_slot(h_all, r), *lots[2 + r]) for r in range(2)]
    rows_th = [TensorGather(th_one.at[r], half_slot(th_all, r), *lots[4 + r]) for r in range(2)]
    spread = DataSpread(h_low, mini, *spread_sems)
    share = CoreShare((kw, vw), lambda j, c: kv.at[:, strip(j, c)], *share_sems)
    own = [
        pltpu.make_async_copy(src, kv.at[:, strip(j, core)], own_sems[0].at[j])
        for j, src in enumerate((kw, vw))
    ]
    zeros = Probes(LargeGather, 0, (q, k, v, o), (pq, pkv, po), zero_sems)
    ones = Probes(LargeGather, 1, (q, k, v, o), (gq, gkv, go), one_sems)

    spread.start()
    rows.start()
    zeros.start()
    share.start()
    for copy in own:
        copy.start()
    q_sum, tq_sum, kv_sum, tkv_sum = sums_f32
    for one in sums_f32:
        one[...] = jnp.zeros_like(one)
    rows.relay()
    spread.finish()
    slices.start()
    for job in zeros.jobs[:3]:
        job.relay()
    rows.finish()
    zeros.jobs[3].relay()
    slices.relay()
    share.finish()
    for copy in own:
        copy.wait()

    @tiles(width, TILE)
    def _(at):
        h = h_zero[:, at]
        q_sum[...] += contract(h, wq[0, at], 1, 0)
        kv_sum[...] += contract(h, kv[0, :, at], 1, 1)

    attend_primal(lengths[d], cos, sin, q_sum, kv_sum, q_out, k_out, v_out, a_out, weights)

    @tiles(width, TILE)
    def _(at):
        store_by_owner(part, at, contract(a_out[...], wo[0, :, at], 1, 0))

    for one in primals:
        one.start()
    for job in zeros.jobs[:2]:
        job.pass_on()
    for one in primals:
        one.send()
    for job in zeros.jobs[2:]:
        job.pass_on()
    for job in ones.jobs:
        job.start_ring()
    for one in primals:
        one.middle()
    for r in range(2):
        stream = (tokens[r].astype(F32) + primals[r].total()).astype(BF16)
        x_out[r] = stream
        wide = stream.astype(F32)
        inverse = lax.rsqrt(mean_of(wide * wide) + EPS)
        h_one[r] = (wide * inverse * gain).astype(BF16)
        rows_h[r].start()
    for job in ones.jobs:
        job.start_pair()
    for one in primals:
        one.finish()
    zeros.finish()

    @tiles(width, TILE)
    def _(at):
        h = h_zero[:, at]
        tq_sum[...] += contract(h, pq[at], 1, 0)
        tkv_sum[...] += contract(h, pkv[:, at], 1, 1)

    for one in rows_h:
        one.relay()
    attend_tangent(cos, sin, tq_sum, tkv_sum, q_out, k_out[...], v_out[...], weights, ta_low)

    @tiles(width, TILE)
    def _(at):
        term = contract(ta_low[...], wo[0, :, at], 1, 0) + contract(a_out[...], po[:, at], 1, 0)
        store_by_owner(part, at, term)

    for one in moves:
        one.start()
    for one in moves:
        one.send()
    for job in ones.jobs:
        job.relay_ring()
    for one in moves:
        one.middle()
    for r in range(2):
        tangent = moves[r].total()
        t_out[r] = tangent
        wide = x_out[r].astype(F32)
        inverse = lax.rsqrt(mean_of(wide * wide) + EPS)
        shift = mean_of(wide * tangent)
        th_one[r] = (
            gain * (tangent * inverse - wide * inverse * inverse * inverse * shift)
        ).astype(BF16)
        rows_th[r].start()
    for job in ones.jobs:
        job.relay_pair()
    for one in rows_th:
        one.relay()
    ones.pass_on()
    for one in moves:
        one.finish()
    slices.finish()
    for one in rows_h + rows_th:
        one.finish()
    ones.finish()


def head(lengths, tables, h_low, wq, wo, tokens, gains, kw, vw, probes):
    half, width = tokens.shape[1:]
    columns = wq.shape[2]
    wide = pltpu.VMEM((LEN, columns), F32)
    return comm_call(
        head_kernel,
        "head",
        1,
        [SMEM] + [VMEM] * 7 + [HBM] * 6,
        [VMEM] * 9 + [ANY] * 4,
        [
            shape((LEN, columns), BF16),
            shape((LEN, HD), BF16),
            shape((LEN, HD), BF16),
            shape((LEN, columns), BF16),
            shape((2, half, width), BF16),
            shape((2, half, width), F32),
            shape((16, 2, half, width), BF16),
            shape((16, 2, half, width), BF16),
            shape((2, 4 * kw.shape[1], width), BF16),
            shape((8, 16, 2 * half, width // 8), BF16),
        ]
        + Probes.shapes(probes),
        [pltpu.VMEM((8, 2 * half, width // 8), BF16), pltpu.VMEM((LEN, width), BF16)]
        + [pltpu.VMEM(one.shape, BF16) for one in Probes.shapes(probes)]
        + [pltpu.VMEM((columns // HD, LEN, LEN), F32), pltpu.VMEM((LEN, columns), BF16)]
        + [pltpu.VMEM((8, 2, 2, half, width), BF16)]
        + [pltpu.VMEM((2, half, width), BF16)] * 2
        + [wide] * 4
        + TensorSum.scratch(width) * 4
        + TensorGather.scratch * 6
        + DataSpread.scratch
        + CoreShare.scratch
        + [DMA((2,))]
        + Probes.scratch(LargeGather) * 2,
        (lengths,) + tables + (h_low, wq, wo, tokens, gains, kw, vw) + probes,
        limit=19,
    )


def turn_kernel(*refs):
    (
        (lengths, cosine, sine, wq, kv, pq, pkv, wo, po, h_one, th_one, t_one, a_zero),
        (q_out, k_out, v_out, c_out, cb_all, ga_zero, ga_one, hs_one),
        (a_one, ta_low, part, c_low),
        sums_f32,
        sum_refs,
        gather_refs,
        sems,
    ) = taken(refs, 13, 8, 4, 4, 10, 4, 6)
    d, t = places()
    width = h_one.shape[1]
    enter(HOPS)
    lots = taken(sum_refs, 5, 5)
    sums = [TensorSum(r, part, *lots[r]) for r in range(2)]
    lots = taken(gather_refs, 2, 2)
    rows = [TensorGather(c_low.at[r], half_slot(cb_all, r), *lots[r]) for r in range(2)]
    jobs = [
        DataGather(a_zero, slot_of(ga_zero), *sems[0:2]),
        DataGather(a_one, slot_of(ga_one), *sems[2:4]),
    ]
    swap = DataExchange(h_one, hs_one, *sems[4:6])
    jobs[0].start()
    swap.start()
    swap.start_pairs()
    q_sum, tq_sum, kv_sum, tkv_sum = sums_f32
    for one in sums_f32:
        one[...] = jnp.zeros_like(one)

    @tiles(width, TILE)
    def _(at):
        h, th = h_one[:, at], th_one[:, at]
        w, k = wq[1, at], kv[1, :, at]
        q_sum[...] += contract(h, w, 1, 0)
        kv_sum[...] += contract(h, k, 1, 1)
        tq_sum[...] += contract(h, pq[at], 1, 0) + contract(th, w, 1, 0)
        tkv_sum[...] += contract(h, pkv[:, at], 1, 1) + contract(th, k, 1, 1)

    attend(lengths[d], cosine[...], sine[...], sums_f32, q_out, k_out, v_out, a_one, ta_low)
    jobs[1].start()
    jobs[0].relay()

    @tiles(width, TILE)
    def _(at):
        moved = contract(ta_low[...], wo[1, :, at], 1, 0) + contract(a_one[...], po[:, at], 1, 0)
        store_by_owner(part, at, moved)

    for one in sums:
        one.start()
    for one in sums:
        one.send()
    for one in sums:
        one.middle()
    half = t_one.shape[1]
    for r in range(2):
        position = (2 * t + r) * half + lax.broadcasted_iota(jnp.int32, t_one.shape[1:], 0)
        mask = jnp.where(position < lengths[d], 1.0, 0.0)
        cotangent = mask * (t_one[r] + sums[r].total())
        c_out[r] = cotangent
        c_low[r] = cotangent.astype(BF16)
        rows[r].start()
    rows[0].relay()
    jobs[1].relay()
    rows[1].relay()
    for job in jobs:
        job.pass_on()
    for r in range(2):
        sums[r].finish()
        rows[r].finish()
    swap.finish()
    for job in jobs:
        job.finish()


def turn(lengths, tables, wq, kv, pq, pkv, wo, po, h_one, th_one, t_one, a_zero):
    half, width = t_one.shape[1:]
    length, columns = a_zero.shape
    return comm_call(
        turn_kernel,
        "turn",
        3,
        [SMEM] + [VMEM] * 12,
        [VMEM] * 5 + [ANY] * 3,
        [
            shape((length, columns), BF16),
            shape((length, HD), BF16),
            shape((length, HD), BF16),
            shape((2, half, width), F32),
            shape((16, 2, half, width), BF16),
            shape((8,) + a_zero.shape, BF16),
            shape((8,) + a_zero.shape, BF16),
            shape((8, length, width // 8), BF16),
        ],
        [
            pltpu.VMEM((length, columns), BF16),
            pltpu.VMEM((length, columns), BF16),
            pltpu.VMEM((8, 2, 2, half, width), BF16),
            pltpu.VMEM((2, half, width), BF16),
            pltpu.VMEM((length, columns), F32),
            pltpu.VMEM((length, columns), F32),
            pltpu.VMEM((length, 2 * HD), F32),
            pltpu.VMEM((length, 2 * HD), F32),
        ]
        + TensorSum.scratch(width) * 2
        + TensorGather.scratch * 2
        + DataGather.scratch * 2
        + DataExchange.scratch,
        (lengths,) + tables + (wq, kv, pq, pkv, wo, po, h_one, th_one, t_one, a_zero),
    )


class Cotangents:
    def __init__(self, gq, gkv, gathered, came, merged, sems):
        self.gkv, self.came, self.merged = gkv, came, merged
        width = gq.shape[1]
        self.jobs = [
            DataGather(gq, lambda block: gathered.at[block, :, 0:width], *sems[0:2]),
            DataGather(
                merged,
                lambda block: gathered.at[block, :, width : width + merged.shape[1]],
                *sems[2:4],
            ),
        ]
        self.sends, self.recvs = sems[4:6]

    @staticmethod
    def scratch(gkv):
        return (
            [pltpu.VMEM(gkv.shape[1:], BF16)] * 2
            + DataGather.scratch * 2
            + [DMA((1,)), DMA((1,))]
        )

    def swap(self):
        d, t = places()
        return remote(
            self.gkv.at[1 - lax.rem(t, 2)],
            self.came,
            self.sends,
            self.recvs,
            0,
            (d, other_core(t)),
        )

    def start(self):
        self.swap().start()
        self.jobs[0].start()

    def merge(self):
        d, t = places()
        self.swap().wait()
        mine = self.gkv[lax.rem(t, 2)].astype(F32) + self.came[...].astype(F32)
        self.merged[...] = mine.astype(BF16)
        self.jobs[1].start()

    def relay(self):
        for job in self.jobs:
            job.relay()

    def pass_on(self):
        for job in self.jobs:
            job.pass_on()

    def finish(self):
        for job in self.jobs:
            job.finish()


def lower_kernel(*refs):
    (
        (lengths, cosine, sine, q, k, v, cb_one, wo, wq, kv, c_two, x_one, gains),
        (cb_all, gg, cbs, mini),
        (ga_sum, gq, gkv, gkv_low, part, c_low),
        sum_refs,
        gather_refs,
        (came, merged),
        sems,
        swap_sems,
        spread_sems,
    ) = taken(refs, 13, 4, 6, 10, 4, 2, 6, 2, 2)
    d, t = places()
    width = cb_one.shape[1]
    enter(HOPS)
    lots = taken(sum_refs, 5, 5)
    sums = [TensorSum(r, part, *lots[r]) for r in range(2)]
    lots = taken(gather_refs, 2, 2)
    rows = [TensorGather(c_low.at[r], half_slot(cb_all, r), *lots[r]) for r in range(2)]
    jobs = Cotangents(gq, gkv, gg, came, merged, sems)
    swap = DataExchange(cb_one, cbs, *swap_sems)
    swap.start()
    swap.start_pairs()
    ga_sum[...] = jnp.zeros_like(ga_sum)

    @tiles(width, TILE)
    def _(at):
        ga_sum[...] += contract(cb_one[:, at], wo[1, :, at], 1, 1)

    attend_back(
        lengths[d], cosine[...], sine[...], q, k[...], v[...], ga_sum, gq, gkv, gkv_low
    )
    jobs.start()

    @tiles(width, TILE)
    def _(at):
        term = contract(gq[...], wq[1, at], 1, 1) + contract(gkv_low[...], kv[1, :, at], 1, 0)
        store_by_owner(part, at, term)

    for one in sums:
        one.start()
    jobs.merge()
    for one in sums:
        one.send()
    for one in sums:
        one.middle()
    for r in range(2):
        scaled = sums[r].total() * gains[1:2]
        wide = x_one[r].astype(F32)
        inverse = lax.rsqrt(mean_of(wide * wide) + EPS)
        shift = mean_of(wide * scaled)
        cotangent = c_two[r] + inverse * (scaled - wide * inverse * inverse * shift)
        c_low[r] = cotangent.astype(BF16)
        rows[r].start()
    spread = DataSpread(c_low, mini, *spread_sems)
    spread.start()
    for one in rows:
        one.relay()
    jobs.relay()
    jobs.pass_on()
    for r in range(2):
        sums[r].finish()
        rows[r].finish()
    swap.finish()
    spread.finish()
    jobs.finish()


def lower(lengths, tables, q, k, v, cb_one, wo, wq, kv, c_two, x_one, gains):
    half, width = c_two.shape[1:]
    length, columns = q.shape
    gkv = shape((2, length, HD), BF16)
    return comm_call(
        lower_kernel,
        "lower",
        4,
        [SMEM] + [VMEM] * 12,
        [VMEM] + [ANY] * 3,
        [
            shape((16, 2, half, width), BF16),
            shape((8, length, columns + HD), BF16),
            shape((8, length, width // 8), BF16),
            shape((8, 2, half, width // 8), BF16),
        ],
        [
            pltpu.VMEM((length, columns), F32),
            pltpu.VMEM((length, columns), BF16),
            pltpu.VMEM(gkv.shape, BF16),
            pltpu.VMEM((length, 2 * HD), BF16),
            pltpu.VMEM((8, 2, 2, half, width), BF16),
            pltpu.VMEM((2, half, width), BF16),
        ]
        + TensorSum.scratch(width) * 2
        + TensorGather.scratch * 2
        + Cotangents.scratch(gkv)
        + DataExchange.scratch
        + DataSpread.scratch,
        (lengths,) + tables + (q, k, v, cb_one, wo, wq, kv, c_two, x_one, gains),
    )


def inner(hs, gathered, g_sum):
    g_sum[...] = jnp.zeros_like(g_sum)

    @pl.loop(0, 4)
    def _(i):
        g = gathered[pl.ds(2 * i, 2)].reshape(-1, gathered.shape[2])
        h = hs[pl.ds(2 * i, 2)].reshape(-1, hs.shape[2])
        g_sum[...] += contract(g, h, 0, 0)


def outer(ga, cs, o_sum):
    o_sum[...] = jnp.zeros_like(o_sum)

    @pl.loop(0, 4)
    def _(i):
        a = ga[pl.ds(2 * i, 2)].reshape(-1, ga.shape[2])
        c = cs[pl.ds(2 * i, 2)].reshape(-1, cs.shape[2])
        o_sum[...] += contract(a, c, 0, 0)


def last_kernel(*refs):
    (
        (lengths, cosine, sine, q, k, v, cb, wo, mini, hs, gg_one, ga, cs),
        (gg, cs_zero, q_out, g_sum, o_sum),
        (ga_sum, gq, gkv),
        (came, merged),
        sems,
        slice_sems,
    ) = taken(refs, 13, 5, 3, 2, 6, 2)
    d, t = places()
    width, columns = cb.shape[1], gq.shape[1]
    enter(NEAR)
    slices = TensorGather(mini, lambda block: cs_zero.at[:, block], *slice_sems)
    jobs = Cotangents(gq, gkv, gg, came, merged, sems)
    slices.start()
    ga_sum[...] = jnp.zeros_like(ga_sum)

    @tiles(width, TILE)
    def _(at):
        ga_sum[...] += contract(cb[:, at], wo[0, :, at], 1, 1)

    attend_back(lengths[d], cosine[...], sine[...], q, k[...], v[...], ga_sum, gq, gkv, None)
    jobs.start()
    slices.relay()
    jobs.merge()
    inner(hs, gg_one, g_sum)
    q_out[...] = g_sum[0:columns].T
    jobs.relay()
    outer(ga, cs, o_sum)
    jobs.pass_on()
    slices.finish()
    jobs.finish()


def last(lengths, tables, q, k, v, cb, wo, mini, *sides):
    length, columns = q.shape
    share = mini.shape[3]
    gkv = shape((2, length, HD), BF16)
    return comm_call(
        last_kernel,
        "last",
        5,
        [SMEM] + [VMEM] * 12,
        [ANY] * 2 + [VMEM] * 3,
        [
            shape((8, length, columns + HD), BF16),
            shape((8, 16) + mini.shape[1:], BF16),
            shape((share, columns), F32),
            shape((columns + HD, share), F32),
            shape((columns, share), F32),
        ],
        [
            pltpu.VMEM((length, columns), F32),
            pltpu.VMEM((length, columns), BF16),
            pltpu.VMEM(gkv.shape, BF16),
        ]
        + Cotangents.scratch(gkv)
        + TensorGather.scratch,
        (lengths,) + tables + (q, k, v, cb, wo, mini) + sides,
    )


def products_kernel(hs, gg, ga, cs, q_one, g_one, o_one, q_out, k_out, v_out, o_out, g_sum):
    columns, half = q_out.shape[2], k_out.shape[1]
    inner(hs, gg, g_sum)
    outer(ga, cs, o_out.at[0])
    q_out[0] = g_sum[0:columns].T
    q_out[1] = q_one[...]
    o_out[1] = o_one[...]
    for layer, one in ((0, g_sum), (1, g_one)):
        k_out[layer] = one[columns : columns + half]
        v_out[layer] = one[columns + half :]


def products(*operands):
    share, columns = operands[4].shape
    half = (operands[1].shape[2] - columns) // 2
    return pl.pallas_call(
        products_kernel,
        name="products",
        in_specs=[VMEM] * 7,
        out_specs=[VMEM] * 4,
        out_shape=[
            shape((2, share, columns), F32),
            shape((2, half, share), F32),
            shape((2, half, share), F32),
            shape((2, columns, share), F32),
        ],
        scratch_shapes=[pltpu.VMEM(operands[5].shape, F32)],
        compiler_params=pltpu.CompilerParams(vmem_limit_bytes=12 * 2**20),
    )(*operands)


def rope_tables():
    angles = np.arange(LEN)[:, None] * THETA ** (-2.0 * np.arange(HD // 2) / HD)[None, :]
    cosine, sine = np.cos(angles), np.sin(angles)
    return (
        jnp.asarray(np.concatenate([cosine, cosine], axis=1), F32),
        jnp.asarray(np.concatenate([-sine, sine], axis=1), F32),
    )


def body(
    tokens,
    lengths,
    gains,
    query_weight,
    key_weight,
    value_weight,
    out_weight,
    query_probe,
    key_probe,
    value_probe,
    out_probe,
):
    rows, width = tokens.shape
    tables = rope_tables()

    def turned_over(array):
        return jnp.swapaxes(array, 1, 2)

    def all_rows(blocks):
        return blocks.reshape(-1, blocks.shape[-1])

    def by_batch(blocks):
        return blocks.reshape(blocks.shape[0], -1, blocks.shape[-1])

    probes = (query_probe, turned_over(key_probe), turned_over(value_probe), out_probe)
    q0, k0, v0, a_zero, x_one, t_one, h_one, th_one, kv, hs_zero, pq, pkv, po = head(
        lengths,
        tables,
        normed(tokens, gains),
        query_weight,
        out_weight,
        tokens.reshape(2, rows // 2, width),
        gains,
        turned_over(key_weight),
        turned_over(value_weight),
        probes,
    )
    q1, k1, v1, c_two, cb_one, ga_zero, ga_one, hs_one = turn(
        lengths,
        tables,
        query_weight,
        kv,
        pq,
        pkv,
        out_weight,
        po,
        all_rows(h_one),
        all_rows(th_one),
        t_one,
        a_zero,
    )
    cb_zero, gg_one, cs_one, mini = lower(
        lengths,
        tables,
        q1,
        k1,
        v1,
        all_rows(cb_one),
        out_weight,
        query_weight,
        kv,
        c_two,
        x_one,
        gains,
    )
    gg_zero, cs_zero, q_one, g_one, o_one = last(
        lengths,
        tables,
        q0,
        k0,
        v0,
        all_rows(cb_zero),
        out_weight,
        mini,
        hs_one,
        gg_one,
        ga_one,
        cs_one,
    )
    q, k, v, o = products(
        by_batch(hs_zero), gg_zero, ga_zero, by_batch(cs_zero), q_one, g_one, o_one
    )
    return (q, turned_over(k), turned_over(v), o)


def solution(mesh):
    placed = (
        P(("dp", "tensor"), None),
        P(),
        P(),
        P(None, None, "tensor"),
        P(None, None, "tensor"),
        P(None, None, "tensor"),
        P(None, "tensor", None),
        P(None, "dp", "tensor"),
        P(None, "dp", "tensor"),
        P(None, "dp", "tensor"),
        P(None, "tensor", "dp"),
    )
    return jax.shard_map(
        body,
        mesh=mesh,
        in_specs=placed,
        out_specs=(
            P(None, "dp", "tensor"),
            P(None, "dp", "tensor"),
            P(None, "dp", "tensor"),
            P(None, "tensor", "dp"),
        ),
        check_vma=False,
    )
```

```python
import functools
import math

import jax
import jax.numpy as jnp
import numpy as np
from jax import lax
from jax.experimental import pallas as pl
from jax.experimental.pallas import tpu as pltpu
from jax.sharding import PartitionSpec as P

HD = 128
LEN = 256
EPS = 1e-05
THETA = 500000.0

MESH = pl.DeviceIdType.MESH
F32 = jnp.float32
BF16 = jnp.bfloat16
VMEM = pl.BlockSpec(memory_space=pltpu.VMEM)
ANY = pl.BlockSpec(memory_space=pl.ANY)
HBM = pl.BlockSpec(memory_space=pltpu.HBM)
SMEM = pl.BlockSpec(memory_space=pltpu.SMEM)
DMA = pltpu.SemaphoreType.DMA
TILE = 1024

HOPS = ((1, 1), (3, 1), (2, 1), (2, 0), (1, 0), (3, 0), (0, 1))
NEAR = HOPS[3:]


def back(hop):
    return ((4 - hop[0]) % 4, hop[1])


def data_at(d, hop):
    ring, pair = lax.div(d, 2), lax.rem(d, 2)
    return lax.rem(ring + hop[0], 4) * 2 + lax.rem(pair + hop[1], 2)


def chip_at(t, hop):
    return data_at(lax.div(t, 2), hop)


def tensor_at(t, hop):
    return chip_at(t, hop) * 2 + lax.rem(t, 2)


def other_core(t):
    return t + 1 - 2 * lax.rem(t, 2)


def places():
    return lax.axis_index("dp"), lax.axis_index("tensor")


def remote(src, dst, sends, recvs, j, device):
    return pltpu.make_async_remote_copy(
        src_ref=src,
        dst_ref=dst,
        send_sem=sends.at[j],
        recv_sem=recvs.at[j],
        device_id=device,
        device_id_type=MESH,
    )


def enter(data_hops):
    d, t = places()
    barrier = pltpu.get_barrier_semaphore()
    peers = [(d, other_core(t))]
    peers += [(d, tensor_at(t, hop)) for hop in NEAR]
    peers += [(data_at(d, hop), t) for hop in data_hops]
    for peer in peers:
        pl.semaphore_signal(barrier, inc=1, device_id=peer, device_id_type=MESH)
    pl.semaphore_wait(barrier, len(peers))


def half_of(ref, half):
    if half is None:
        return ref
    rows = ref.shape[0] // 2
    return ref.at[pl.ds(half * rows, rows)]


class RingGather:
    ROUTES = ()
    FIRST = 0

    def __init__(self, src, slot, sends, recvs):
        self.src, self.slot, self.sends, self.recvs = src, slot, sends, recvs

    def out(self, j):
        hop, block, unused, half = self.ROUTES[j]
        slot = half_of(self.slot(self.place(block)), half)
        src = self.src if j < self.FIRST else slot
        return remote(src, slot, self.sends, self.recvs, j, self.device(hop))

    def into(self, j):
        slot = half_of(self.slot(self.place(self.ROUTES[j][2])), self.ROUTES[j][3])
        return remote(slot, slot, self.sends, self.recvs, j, self.device((0, 1)))

    def own(self):
        n = len(self.ROUTES)
        return pltpu.make_async_copy(self.src, self.slot(self.place((0, 0))), self.sends.at[n])

    def start(self):
        for j in range(self.FIRST):
            self.out(j).start()
        self.own().start()

    def sent(self):
        for j in range(len(self.ROUTES)):
            self.out(j).wait_send()
        self.own().wait()


class DataGather(RingGather):
    scratch = [DMA((8,)), DMA((7,))]
    FIRST = 4
    ROUTES = (
        ((0, 1), (0, 0), (0, 1), None),
        ((1, 0), (0, 0), (3, 0), None),
        ((3, 0), (0, 0), (1, 0), None),
        ((2, 0), (0, 0), (2, 0), None),
        ((1, 0), (0, 1), (3, 1), None),
        ((3, 0), (0, 1), (1, 1), None),
        ((0, 1), (2, 0), (2, 1), None),
    )

    def place(self, hop):
        d, t = places()
        return data_at(d, hop)

    def device(self, hop):
        d, t = places()
        return (data_at(d, hop), t)

    def relay(self):
        self.into(0).wait_recv()
        self.out(4).start()
        self.out(5).start()

    def pass_on(self):
        self.into(3).wait_recv()
        self.out(6).start()

    def finish(self):
        for j in (1, 2, 4, 5, 6):
            self.into(j).wait_recv()
        self.sent()


class LargeGather(DataGather):
    scratch = [DMA((12,)), DMA((11,))]
    FIRST = 3
    ROUTES = (
        ((0, 1), (0, 0), (0, 1), None),
        ((1, 0), (0, 0), (3, 0), None),
        ((3, 0), (0, 0), (1, 0), None),
        ((1, 0), (0, 1), (3, 1), 0),
        ((3, 0), (0, 1), (1, 1), 1),
        ((1, 0), (3, 0), (2, 0), 0),
        ((0, 1), (3, 0), (3, 1), 1),
        ((3, 0), (1, 0), (2, 0), 1),
        ((0, 1), (1, 0), (1, 1), 0),
        ((1, 0), (3, 1), (2, 1), 0),
        ((3, 0), (1, 1), (2, 1), 1),
    )

    def start_ring(self):
        self.out(1).start()
        self.out(2).start()
        self.own().start()

    def start_pair(self):
        self.out(0).start()

    def relay_ring(self):
        self.into(0).wait_recv()
        self.out(3).start()
        self.out(4).start()
        self.into(1).wait_recv()
        self.out(5).start()
        self.into(2).wait_recv()
        self.out(7).start()

    def relay_pair(self):
        self.out(6).start()
        self.out(8).start()

    def relay(self):
        self.relay_ring()
        self.relay_pair()

    def pass_on(self):
        for j in (3, 4):
            self.into(j).wait_recv()
            self.out(6 + j).start()

    def finish(self):
        for j in range(5, 11):
            self.into(j).wait_recv()
        self.sent()


class TensorGather(RingGather):
    scratch = [DMA((16,)), DMA((15,))]
    FIRST = 4
    ROUTES = (
        ((0, 1), (0, 0), (0, 1), None),
        ((1, 0), (0, 0), (3, 0), None),
        ((3, 0), (0, 0), (1, 0), None),
        ((2, 0), (0, 0), (2, 0), None),
        ((1, 0), (0, 1), (3, 1), None),
        ((3, 0), (0, 1), (1, 1), None),
        ((2, 0), (0, 1), (2, 1), None),
    )

    def place(self, hop):
        d, t = places()
        return tensor_at(t, hop)

    def device(self, hop):
        d, t = places()
        return (d, tensor_at(t, hop))

    def handover(self, j, src, block):
        d, t = places()
        return pltpu.make_async_remote_copy(
            src_ref=src,
            dst_ref=self.slot(block),
            send_sem=self.sends.at[8 + j],
            recv_sem=self.recvs.at[7 + j],
            device_id=(d, other_core(t)),
            device_id_type=MESH,
        )

    def hand(self, j):
        block = self.place(self.ROUTES[j][2])
        return self.handover(j, self.slot(block), block)

    def near(self):
        return self.handover(7, self.src, self.place((0, 0)))

    def start(self):
        super().start()
        self.near().start()

    def relay(self):
        self.into(0).wait_recv()
        for j in range(4, 7):
            self.out(j).start()
        self.hand(0).start()

    def collect(self):
        for j in range(1, 7):
            self.into(j).wait_recv()
            self.hand(j).start()

    def close(self):
        self.sent()
        d, t = places()
        far = other_core(t)
        self.handover(7, self.slot(far), far).wait_recv()
        self.near().wait_send()
        for j in range(7):
            block = tensor_at(far, self.ROUTES[j][2])
            self.handover(j, self.slot(block), block).wait_recv()
            self.hand(j).wait_send()

    def finish(self):
        self.collect()
        self.close()


class TensorSum:
    STEPS = ((2, 1), (1, 1), (3, 1), (2, 0), (1, 0), (3, 0))
    BLOCKS = STEPS + ((0, 1), (0, 0))

    @staticmethod
    def scratch(columns):
        return [
            pltpu.VMEM((8, 8, columns), BF16),
            pltpu.VMEM((7, 8, columns), BF16),
            pltpu.VMEM((7, 8, columns), BF16),
            DMA((15,)),
            DMA((15,)),
        ]

    def __init__(self, rows, part, near, sent, far, sends, recvs):
        self.rows = rows
        self.part, self.near_, self.sent, self.far = part, near, sent, far
        self.sends, self.recvs = sends, recvs

    def swap(self, j):
        d, t = places()
        k = chip_at(t, self.BLOCKS[j])
        c = lax.rem(t, 2)
        return remote(
            self.part.at[k, 1 - c, self.rows], self.near_.at[k], self.sends, self.recvs, j, (d, other_core(t))
        )

    def cross(self, j):
        d, t = places()
        hop = (self.STEPS[j][0], 0) if j < 6 else (0, 1)
        return remote(
            self.sent.at[j], self.far.at[j], self.sends, self.recvs, 8 + j, (d, tensor_at(t, hop))
        )

    def pair_sum(self, j):
        d, t = places()
        k = chip_at(t, self.BLOCKS[j])
        c = lax.rem(t, 2)
        return self.part[k, c, self.rows].astype(F32) + self.near_[k].astype(F32)

    def start(self):
        for j in range(8):
            self.swap(j).start()

    def send(self):
        for j in range(6):
            self.swap(j).wait_recv()
            self.sent[j] = self.pair_sum(j).astype(BF16)
            self.cross(j).start()

    def middle(self):
        self.swap(6).wait_recv()
        total = self.pair_sum(6)
        for j in (1, 2, 0):
            self.cross(j).wait_recv()
            total = total + self.far[j].astype(F32)
        self.sent[6] = total.astype(BF16)
        self.cross(6).start()

    def total(self):
        self.swap(7).wait_recv()
        total = self.pair_sum(7)
        for j in (4, 5, 3, 6):
            self.cross(j).wait_recv()
            total = total + self.far[j].astype(F32)
        return total

    def finish(self):
        for j in range(8):
            self.swap(j).wait_send()
        for j in range(7):
            self.cross(j).wait_send()


class DataSpread:
    scratch = [DMA((8,)), DMA((7,))]

    def __init__(self, src, out, sends, recvs):
        self.src, self.out_, self.sends, self.recvs = src, out, sends, recvs
        self.share = src.shape[-1] // 8

    def columns(self, d):
        return pl.ds(pl.multiple_of(d * self.share, self.share), self.share)

    def cut(self, d):
        return self.src.at[(slice(None),) * (len(self.src.shape) - 1) + (self.columns(d),)]

    def cross(self, j):
        d, t = places()
        peer = data_at(d, HOPS[j])
        return remote(
            self.cut(peer),
            self.out_.at[d],
            self.sends,
            self.recvs,
            j,
            (peer, t),
        )

    def arrived(self, j):
        d, t = places()
        slot = self.out_.at[data_at(d, back(HOPS[j]))]
        return remote(slot, slot, self.sends, self.recvs, j, (d, other_core(t)))

    def own(self):
        d, t = places()
        return pltpu.make_async_copy(
            self.cut(d), self.out_.at[d], self.sends.at[7]
        )

    def start(self):
        for j in range(7):
            self.cross(j).start()
        self.own().start()

    def finish(self):
        for j in range(7):
            self.arrived(j).wait_recv()
            self.cross(j).wait_send()
        self.own().wait()


class DataExchange:
    scratch = [DMA((15,)), DMA((14,))]

    def __init__(self, src, out, sends, recvs):
        self.src, self.out_, self.sends, self.recvs = src, out, sends, recvs
        self.half = src.shape[0] // 2
        self.share = src.shape[1] // 8

    def rows(self, t):
        return pl.ds(pl.multiple_of(lax.rem(t, 2) * self.half, self.half), self.half)

    def columns(self, d):
        return pl.ds(pl.multiple_of(d * self.share, self.share), self.share)

    def cross(self, j):
        d, t = places()
        peer = data_at(d, HOPS[j])
        return remote(
            self.src.at[self.rows(t), self.columns(peer)],
            self.out_.at[d, self.rows(t)],
            self.sends,
            self.recvs,
            j,
            (peer, t),
        )

    def landing(self, j, t_of):
        d, t = places()
        slot = self.out_.at[data_at(d, back(HOPS[j])), self.rows(t_of)]
        return slot

    def arrived(self, j):
        d, t = places()
        slot = self.landing(j, t)
        return remote(slot, slot, self.sends, self.recvs, j, (d, other_core(t)))

    def handed(self, j):
        d, t = places()
        slot = self.landing(j, t)
        return remote(slot, slot, self.sends, self.recvs, 7 + j, (d, other_core(t)))

    def received(self, j):
        d, t = places()
        slot = self.landing(j, other_core(t))
        return remote(slot, slot, self.sends, self.recvs, 7 + j, (d, other_core(t)))

    def own(self):
        d, t = places()
        return pltpu.make_async_copy(
            self.src.at[:, self.columns(d)], self.out_.at[d], self.sends.at[14]
        )

    def start(self):
        for j in (3, 4, 5):
            self.cross(j).start()
        self.own().start()

    def start_pairs(self):
        for j in (6, 0, 1, 2):
            self.cross(j).start()

    def collect(self):
        for j in (4, 5, 3, 6, 0, 1, 2):
            self.arrived(j).wait_recv()
            self.handed(j).start()

    def finish(self):
        for j in range(7):
            self.received(j).wait_recv()
            self.cross(j).wait_send()
            self.handed(j).wait_send()
        self.own().wait()


def taken(refs, *counts):
    out, at = [], 0
    for count in counts:
        out.append(refs[at : at + count])
        at += count
    return out


def comm_call(kernel, name, number, in_specs, out_specs, out_shape, scratch, args, limit=12):
    return pl.pallas_call(
        kernel,
        name=name,
        in_specs=in_specs,
        out_specs=out_specs,
        out_shape=out_shape,
        scratch_shapes=scratch,
        cost_estimate=pl.CostEstimate(flops=10**10, bytes_accessed=0, transcendentals=0),
        compiler_params=pltpu.CompilerParams(
            collective_id=number, has_side_effects=True, vmem_limit_bytes=limit * 2**20
        ),
    )(*args)


def shape(dims, dtype):
    return jax.ShapeDtypeStruct(dims, dtype)


def slot_of(ref):
    return lambda block: ref.at[block]


def rows_of(ref, count):
    size = ref.shape[0] // count
    return lambda block: ref.at[pl.ds(pl.multiple_of(block * size, size), size)]


def half_slot(ref, half):
    return lambda block: ref.at[block, half]


def columns_of(ref):
    width = ref.shape[1] // 8
    return lambda block: ref.at[:, pl.ds(pl.multiple_of(block * width, width), width)]


def mean_of(values):
    return jnp.sum(values, axis=-1, keepdims=True) * (1.0 / values.shape[-1])


def strip(which, core):
    return pl.ds(pl.multiple_of(which * 128 + core * 64, 64), 64)


class CoreShare:
    scratch = [DMA((2,)), DMA((2,))]

    def __init__(self, sources, slot, sends, recvs):
        self.sources, self.slot, self.sends, self.recvs = sources, slot, sends, recvs

    def copy(self, j, core):
        d, t = places()
        slot = self.slot(j, core)
        src = slot if self.sources is None else self.sources[j]
        return remote(src, slot, self.sends, self.recvs, j, (d, other_core(t)))

    def start(self):
        d, t = places()
        for j in range(2):
            self.copy(j, lax.rem(t, 2)).start()

    def finish(self):
        d, t = places()
        for j in range(2):
            self.copy(j, 1 - lax.rem(t, 2)).wait_recv()
            self.copy(j, lax.rem(t, 2)).wait_send()


class Probes:
    COUNT = 4
    @staticmethod
    def scratch(kind):
        return kind.scratch * 4 + CoreShare.scratch

    def __init__(self, kind, layer, probes, gathered, sems):
        q, k, v, o = probes
        gq, gkv, go = gathered
        d, t = places()
        core = lax.rem(t, 2)
        width = k.shape[2]

        def part(which):
            return lambda block: gkv.at[
                strip(which, core), pl.ds(pl.multiple_of(block * width, width), width)
            ]

        self.jobs = [
            kind(k.at[layer], part(0), *sems[0:2]),
            kind(v.at[layer], part(1), *sems[2:4]),
            kind(q.at[layer], rows_of(gq, 8), *sems[4:6]),
            kind(o.at[layer], columns_of(go), *sems[6:8]),
        ]
        self.share = CoreShare(None, lambda j, c: gkv.at[strip(j, c)], *sems[8:10])

    @staticmethod
    def shapes(probes):
        q, k, v, o = probes
        return [
            shape((8 * q.shape[1], q.shape[2]), BF16),
            shape((4 * k.shape[1], 8 * k.shape[2]), BF16),
            shape((o.shape[1], 8 * o.shape[2]), BF16),
        ]

    def start(self):
        for job in self.jobs:
            job.start()

    def relay(self):
        for job in self.jobs:
            job.relay()

    def pass_on(self):
        for job in self.jobs:
            job.pass_on()

    def finish(self):
        for job in self.jobs[:2]:
            job.finish()
        self.share.start()
        for job in self.jobs[2:]:
            job.finish()
        self.share.finish()


def contract(left_side, right_side, left_dim, right_dim):
    return lax.dot_general(
        left_side,
        right_side,
        (((left_dim,), (right_dim,)), ((), ())),
        preferred_element_type=F32,
    )


def turned(values, cosine, sine):
    return values * cosine + pltpu.roll(values, values.shape[1] // 2, 1) * sine


def attention_weights(q, k, length):
    size = q.shape[0]
    row = lax.broadcasted_iota(jnp.int32, (size, size), 0)
    column = lax.broadcasted_iota(jnp.int32, (size, size), 1)
    allowed = (column <= row) & (column < length)
    scores = contract(q, k, 1, 1) * (1.0 / math.sqrt(q.shape[1]))
    powers = jnp.where(allowed, jnp.exp(scores), 0.0)
    return powers / jnp.sum(powers, axis=-1, keepdims=True)


def attend(length, cos, sin, sums, q_out, k_out, v_out, a_out, ta_out):
    q_sum, tq_sum, kv_sum, tkv_sum = sums
    scaling = 1.0 / math.sqrt(HD)
    k = turned(kv_sum[:, 0:HD], cos, sin).astype(BF16)
    v = kv_sum[:, HD:].astype(BF16)
    tk = turned(tkv_sum[:, 0:HD], cos, sin).astype(BF16)
    tv = tkv_sum[:, HD:].astype(BF16)
    k_out[...] = k
    v_out[...] = v
    for at in range(0, q_sum.shape[1], HD):
        head = slice(at, at + HD)
        q = turned(q_sum[:, head], cos, sin).astype(BF16)
        tq = turned(tq_sum[:, head], cos, sin).astype(BF16)
        q_out[:, head] = q
        weights = attention_weights(q, k, length)
        low = weights.astype(BF16)
        a_out[:, head] = contract(low, v, 1, 0).astype(BF16)
        scores = (contract(tq, k, 1, 1) + contract(q, tk, 1, 1)) * scaling
        change = weights * (scores - jnp.sum(weights * scores, axis=-1, keepdims=True))
        ta = contract(change.astype(BF16), v, 1, 0) + contract(low, tv, 1, 0)
        ta_out[:, head] = ta.astype(BF16)


def attend_primal(length, cos, sin, q_sum, kv_sum, q_out, k_out, v_out, a_out, w_out):
    k = turned(kv_sum[:, 0:HD], cos, sin).astype(BF16)
    v = kv_sum[:, HD:].astype(BF16)
    k_out[...] = k
    v_out[...] = v
    for n, at in enumerate(range(0, q_sum.shape[1], HD)):
        head = slice(at, at + HD)
        q = turned(q_sum[:, head], cos, sin).astype(BF16)
        q_out[:, head] = q
        weights = attention_weights(q, k, length)
        w_out[n] = weights
        a_out[:, head] = contract(weights.astype(BF16), v, 1, 0).astype(BF16)


def attend_tangent(cos, sin, tq_sum, tkv_sum, q_in, k, v, w_in, ta_out):
    scaling = 1.0 / math.sqrt(HD)
    tk = turned(tkv_sum[:, 0:HD], cos, sin).astype(BF16)
    tv = tkv_sum[:, HD:].astype(BF16)
    for n, at in enumerate(range(0, tq_sum.shape[1], HD)):
        head = slice(at, at + HD)
        tq = turned(tq_sum[:, head], cos, sin).astype(BF16)
        weights = w_in[n]
        low = weights.astype(BF16)
        scores = (contract(tq, k, 1, 1) + contract(q_in[:, head], tk, 1, 1)) * scaling
        change = weights * (scores - jnp.sum(weights * scores, axis=-1, keepdims=True))
        ta = contract(change.astype(BF16), v, 1, 0) + contract(low, tv, 1, 0)
        ta_out[:, head] = ta.astype(BF16)


def attend_back(length, cos, sin, q_in, k, v, ga_sum, gq_out, gkv_out, gkv_low):
    scaling = 1.0 / math.sqrt(HD)
    gk, gv = None, None
    for at in range(0, ga_sum.shape[1], HD):
        head = slice(at, at + HD)
        q = q_in[:, head]
        ga = ga_sum[:, head].astype(BF16)
        weights = attention_weights(q, k, length)
        grads = contract(ga, v, 1, 1)
        value = contract(weights.astype(BF16), ga, 0, 0)
        scores = (
            weights * (grads - jnp.sum(weights * grads, axis=-1, keepdims=True)) * scaling
        ).astype(BF16)
        gq_out[:, head] = turned(contract(scores, k, 1, 0), cos, -sin).astype(BF16)
        key = contract(scores, q, 0, 0)
        gk = key if gk is None else gk + key
        gv = value if gv is None else gv + value
    gk = turned(gk, cos, -sin).astype(BF16)
    gv = gv.astype(BF16)
    half = HD // 2
    if gkv_low is not None:
        gkv_low[:, 0:HD] = gk
        gkv_low[:, HD:] = gv
    gkv_out[0] = jnp.concatenate([gk[:, 0:half], gv[:, 0:half]], axis=-1)
    gkv_out[1] = jnp.concatenate([gk[:, half:], gv[:, half:]], axis=-1)


def tiles(width, size):
    def over(function):
        @pl.loop(0, width // size)
        def _(i):
            function(pl.ds(pl.multiple_of(i * size, size), size))

    return over


def store_by_owner(part, columns, values):
    dims = part.shape[:-1] + (values.shape[1],)
    part[:, :, :, :, columns] = values.reshape(dims).astype(BF16)


def normed_kernel(tokens, gains, h_low):
    wide = tokens[...].astype(F32)
    inverse = lax.rsqrt(mean_of(wide * wide) + EPS)
    h_low[...] = (wide * inverse * gains[0:1]).astype(BF16)


def normed(tokens, gains):
    return pl.pallas_call(
        normed_kernel,
        name="normed",
        in_specs=[VMEM, VMEM],
        out_specs=VMEM,
        out_shape=shape(tokens.shape, BF16),
        cost_estimate=pl.CostEstimate(flops=10**10, bytes_accessed=0, transcendentals=0),
        compiler_params=pltpu.CompilerParams(vmem_limit_bytes=8 * 2**20),
    )(tokens, gains)


def head_kernel(*refs):
    (
        (lengths, cosine, sine, h_low, wq, wo, tokens, gains, kw, vw, q, k, v, o),
        (q_out, k_out, v_out, a_out, x_out, t_out, h_all, th_all, kv, hs, gq, gkv, go),
        (mini, h_zero, pq, pkv, po, weights, ta_low, part, h_one, th_one),
        sums_f32,
        sum_refs,
        gather_refs,
        spread_sems,
        share_sems,
        own_sems,
        zero_sems,
        one_sems,
    ) = taken(refs, 14, 13, 10, 4, 20, 12, 2, 2, 1, 10, 10)
    d, t = places()
    core = lax.rem(t, 2)
    width = h_zero.shape[1]
    gain = gains[1:2]
    cos, sin = cosine[...], sine[...]
    enter(HOPS)
    lots = taken(sum_refs, 5, 5, 5, 5)
    primals = [TensorSum(r, part, *lots[r]) for r in range(2)]
    moves = [TensorSum(r, part, *lots[2 + r]) for r in range(2)]
    lots = taken(gather_refs, 2, 2, 2, 2, 2, 2)
    rows = TensorGather(h_low, rows_of(h_zero, 16), *lots[0])
    slices = TensorGather(mini, lambda block: hs.at[:, block], *lots[1])
    rows_h = [TensorGather(h_one.at[r], half_slot(h_all, r), *lots[2 + r]) for r in range(2)]
    rows_th = [TensorGather(th_one.at[r], half_slot(th_all, r), *lots[4 + r]) for r in range(2)]
    spread = DataSpread(h_low, mini, *spread_sems)
    share = CoreShare((kw, vw), lambda j, c: kv.at[:, strip(j, c)], *share_sems)
    own = [
        pltpu.make_async_copy(src, kv.at[:, strip(j, core)], own_sems[0].at[j])
        for j, src in enumerate((kw, vw))
    ]
    zeros = Probes(LargeGather, 0, (q, k, v, o), (pq, pkv, po), zero_sems)
    ones = Probes(LargeGather, 1, (q, k, v, o), (gq, gkv, go), one_sems)

    spread.start()
    rows.start()
    zeros.start()
    share.start()
    for copy in own:
        copy.start()
    q_sum, tq_sum, kv_sum, tkv_sum = sums_f32
    for one in sums_f32:
        one[...] = jnp.zeros_like(one)
    rows.relay()
    spread.finish()
    slices.start()
    for job in zeros.jobs[:3]:
        job.relay()
    rows.finish()
    zeros.jobs[3].relay()
    slices.relay()
    share.finish()
    for copy in own:
        copy.wait()

    @tiles(width, TILE)
    def _(at):
        h = h_zero[:, at]
        q_sum[...] += contract(h, wq[0, at], 1, 0)
        kv_sum[...] += contract(h, kv[0, :, at], 1, 1)

    attend_primal(lengths[d], cos, sin, q_sum, kv_sum, q_out, k_out, v_out, a_out, weights)

    @tiles(width, TILE)
    def _(at):
        store_by_owner(part, at, contract(a_out[...], wo[0, :, at], 1, 0))

    for one in primals:
        one.start()
    for job in zeros.jobs[:2]:
        job.pass_on()
    for one in primals:
        one.send()
    for job in zeros.jobs[2:]:
        job.pass_on()
    for job in ones.jobs:
        job.start_ring()
    for one in primals:
        one.middle()
    for r in range(2):
        stream = (tokens[r].astype(F32) + primals[r].total()).astype(BF16)
        x_out[r] = stream
        wide = stream.astype(F32)
        inverse = lax.rsqrt(mean_of(wide * wide) + EPS)
        h_one[r] = (wide * inverse * gain).astype(BF16)
        rows_h[r].start()
    for job in ones.jobs:
        job.start_pair()
    for one in primals:
        one.finish()
    zeros.finish()

    @tiles(width, TILE)
    def _(at):
        h = h_zero[:, at]
        tq_sum[...] += contract(h, pq[at], 1, 0)
        tkv_sum[...] += contract(h, pkv[:, at], 1, 1)

    for one in rows_h:
        one.relay()
    attend_tangent(cos, sin, tq_sum, tkv_sum, q_out, k_out[...], v_out[...], weights, ta_low)

    @tiles(width, TILE)
    def _(at):
        term = contract(ta_low[...], wo[0, :, at], 1, 0) + contract(a_out[...], po[:, at], 1, 0)
        store_by_owner(part, at, term)

    for one in moves:
        one.start()
    for one in moves:
        one.send()
    for job in ones.jobs:
        job.relay_ring()
    for one in moves:
        one.middle()
    for r in range(2):
        tangent = moves[r].total()
        t_out[r] = tangent
        wide = x_out[r].astype(F32)
        inverse = lax.rsqrt(mean_of(wide * wide) + EPS)
        shift = mean_of(wide * tangent)
        th_one[r] = (
            gain * (tangent * inverse - wide * inverse * inverse * inverse * shift)
        ).astype(BF16)
        rows_th[r].start()
    for job in ones.jobs:
        job.relay_pair()
    for one in rows_th:
        one.relay()
    ones.pass_on()
    slices.collect()
    for one in rows_h + rows_th:
        one.collect()
    for one in moves:
        one.finish()
    slices.close()
    for one in rows_h + rows_th:
        one.close()
    ones.finish()


def head(lengths, tables, h_low, wq, wo, tokens, gains, kw, vw, probes):
    half, width = tokens.shape[1:]
    columns = wq.shape[2]
    wide = pltpu.VMEM((LEN, columns), F32)
    return comm_call(
        head_kernel,
        "head",
        1,
        [SMEM] + [VMEM] * 7 + [HBM] * 6,
        [VMEM] * 9 + [ANY] * 4,
        [
            shape((LEN, columns), BF16),
            shape((LEN, HD), BF16),
            shape((LEN, HD), BF16),
            shape((LEN, columns), BF16),
            shape((2, half, width), BF16),
            shape((2, half, width), F32),
            shape((16, 2, half, width), BF16),
            shape((16, 2, half, width), BF16),
            shape((2, 4 * kw.shape[1], width), BF16),
            shape((8, 16, 2 * half, width // 8), BF16),
        ]
        + Probes.shapes(probes),
        [pltpu.VMEM((8, 2 * half, width // 8), BF16), pltpu.VMEM((LEN, width), BF16)]
        + [pltpu.VMEM(one.shape, BF16) for one in Probes.shapes(probes)]
        + [pltpu.VMEM((columns // HD, LEN, LEN), F32), pltpu.VMEM((LEN, columns), BF16)]
        + [pltpu.VMEM((8, 2, 2, half, width), BF16)]
        + [pltpu.VMEM((2, half, width), BF16)] * 2
        + [wide] * 4
        + TensorSum.scratch(width) * 4
        + TensorGather.scratch * 6
        + DataSpread.scratch
        + CoreShare.scratch
        + [DMA((2,))]
        + Probes.scratch(LargeGather) * 2,
        (lengths,) + tables + (h_low, wq, wo, tokens, gains, kw, vw) + probes,
        limit=19,
    )


def turn_kernel(*refs):
    (
        (lengths, cosine, sine, wq, kv, pq, pkv, wo, po, h_one, th_one, t_one, a_zero),
        (q_out, k_out, v_out, c_out, cb_all, ga_zero, ga_one, hs_one),
        (a_one, ta_low, part, c_low),
        sums_f32,
        sum_refs,
        gather_refs,
        sems,
    ) = taken(refs, 13, 8, 4, 4, 10, 4, 6)
    d, t = places()
    width = h_one.shape[1]
    enter(HOPS)
    lots = taken(sum_refs, 5, 5)
    sums = [TensorSum(r, part, *lots[r]) for r in range(2)]
    lots = taken(gather_refs, 2, 2)
    rows = [TensorGather(c_low.at[r], half_slot(cb_all, r), *lots[r]) for r in range(2)]
    jobs = [
        DataGather(a_zero, slot_of(ga_zero), *sems[0:2]),
        DataGather(a_one, slot_of(ga_one), *sems[2:4]),
    ]
    swap = DataExchange(h_one, hs_one, *sems[4:6])
    jobs[0].start()
    swap.start()
    swap.start_pairs()
    q_sum, tq_sum, kv_sum, tkv_sum = sums_f32
    for one in sums_f32:
        one[...] = jnp.zeros_like(one)

    @tiles(width, TILE)
    def _(at):
        h, th = h_one[:, at], th_one[:, at]
        w, k = wq[1, at], kv[1, :, at]
        q_sum[...] += contract(h, w, 1, 0)
        kv_sum[...] += contract(h, k, 1, 1)
        tq_sum[...] += contract(h, pq[at], 1, 0) + contract(th, w, 1, 0)
        tkv_sum[...] += contract(h, pkv[:, at], 1, 1) + contract(th, k, 1, 1)

    attend(lengths[d], cosine[...], sine[...], sums_f32, q_out, k_out, v_out, a_one, ta_low)
    jobs[1].start()
    jobs[0].relay()

    @tiles(width, TILE)
    def _(at):
        moved = contract(ta_low[...], wo[1, :, at], 1, 0) + contract(a_one[...], po[:, at], 1, 0)
        store_by_owner(part, at, moved)

    for one in sums:
        one.start()
    for one in sums:
        one.send()
    for one in sums:
        one.middle()
    half = t_one.shape[1]
    for r in range(2):
        position = (2 * t + r) * half + lax.broadcasted_iota(jnp.int32, t_one.shape[1:], 0)
        mask = jnp.where(position < lengths[d], 1.0, 0.0)
        cotangent = mask * (t_one[r] + sums[r].total())
        c_out[r] = cotangent
        c_low[r] = cotangent.astype(BF16)
        rows[r].start()
    swap.collect()
    rows[0].relay()
    rows[1].relay()
    jobs[1].relay()
    for job in jobs:
        job.pass_on()
    for one in rows:
        one.collect()
    for one in sums:
        one.finish()
    swap.finish()
    for one in rows:
        one.close()
    for job in jobs:
        job.finish()


def turn(lengths, tables, wq, kv, pq, pkv, wo, po, h_one, th_one, t_one, a_zero):
    half, width = t_one.shape[1:]
    length, columns = a_zero.shape
    return comm_call(
        turn_kernel,
        "turn",
        3,
        [SMEM] + [VMEM] * 12,
        [VMEM] * 5 + [ANY] * 3,
        [
            shape((length, columns), BF16),
            shape((length, HD), BF16),
            shape((length, HD), BF16),
            shape((2, half, width), F32),
            shape((16, 2, half, width), BF16),
            shape((8,) + a_zero.shape, BF16),
            shape((8,) + a_zero.shape, BF16),
            shape((8, length, width // 8), BF16),
        ],
        [
            pltpu.VMEM((length, columns), BF16),
            pltpu.VMEM((length, columns), BF16),
            pltpu.VMEM((8, 2, 2, half, width), BF16),
            pltpu.VMEM((2, half, width), BF16),
            pltpu.VMEM((length, columns), F32),
            pltpu.VMEM((length, columns), F32),
            pltpu.VMEM((length, 2 * HD), F32),
            pltpu.VMEM((length, 2 * HD), F32),
        ]
        + TensorSum.scratch(width) * 2
        + TensorGather.scratch * 2
        + DataGather.scratch * 2
        + DataExchange.scratch,
        (lengths,) + tables + (wq, kv, pq, pkv, wo, po, h_one, th_one, t_one, a_zero),
    )


class Cotangents:
    def __init__(self, gq, gkv, gathered, came, merged, sems):
        self.gkv, self.came, self.merged = gkv, came, merged
        width = gq.shape[1]
        self.jobs = [
            DataGather(gq, lambda block: gathered.at[block, :, 0:width], *sems[0:2]),
            DataGather(
                merged,
                lambda block: gathered.at[block, :, width : width + merged.shape[1]],
                *sems[2:4],
            ),
        ]
        self.sends, self.recvs = sems[4:6]

    @staticmethod
    def scratch(gkv):
        return (
            [pltpu.VMEM(gkv.shape[1:], BF16)] * 2
            + DataGather.scratch * 2
            + [DMA((1,)), DMA((1,))]
        )

    def swap(self):
        d, t = places()
        return remote(
            self.gkv.at[1 - lax.rem(t, 2)],
            self.came,
            self.sends,
            self.recvs,
            0,
            (d, other_core(t)),
        )

    def start(self):
        self.swap().start()
        self.jobs[0].start()

    def merge(self):
        d, t = places()
        self.swap().wait()
        mine = self.gkv[lax.rem(t, 2)].astype(F32) + self.came[...].astype(F32)
        self.merged[...] = mine.astype(BF16)
        self.jobs[1].start()

    def relay(self):
        for job in self.jobs:
            job.relay()

    def pass_on(self):
        for job in self.jobs:
            job.pass_on()

    def finish(self):
        for job in self.jobs:
            job.finish()


def lower_kernel(*refs):
    (
        (lengths, cosine, sine, q, k, v, cb_one, wo, wq, kv, c_two, x_one, gains),
        (cb_all, gg, cbs, mini),
        (ga_sum, gq, gkv, gkv_low, part, c_low),
        sum_refs,
        gather_refs,
        (came, merged),
        sems,
        swap_sems,
        spread_sems,
    ) = taken(refs, 13, 4, 6, 10, 4, 2, 6, 2, 2)
    d, t = places()
    width = cb_one.shape[1]
    enter(HOPS)
    lots = taken(sum_refs, 5, 5)
    sums = [TensorSum(r, part, *lots[r]) for r in range(2)]
    lots = taken(gather_refs, 2, 2)
    rows = [TensorGather(c_low.at[r], half_slot(cb_all, r), *lots[r]) for r in range(2)]
    jobs = Cotangents(gq, gkv, gg, came, merged, sems)
    swap = DataExchange(cb_one, cbs, *swap_sems)
    swap.start()
    swap.start_pairs()
    ga_sum[...] = jnp.zeros_like(ga_sum)

    @tiles(width, TILE)
    def _(at):
        ga_sum[...] += contract(cb_one[:, at], wo[1, :, at], 1, 1)

    attend_back(
        lengths[d], cosine[...], sine[...], q, k[...], v[...], ga_sum, gq, gkv, gkv_low
    )
    jobs.start()

    @tiles(width, TILE)
    def _(at):
        term = contract(gq[...], wq[1, at], 1, 1) + contract(gkv_low[...], kv[1, :, at], 1, 0)
        store_by_owner(part, at, term)

    for one in sums:
        one.start()
    jobs.merge()
    for one in sums:
        one.send()
    for one in sums:
        one.middle()
    for r in range(2):
        scaled = sums[r].total() * gains[1:2]
        wide = x_one[r].astype(F32)
        inverse = lax.rsqrt(mean_of(wide * wide) + EPS)
        shift = mean_of(wide * scaled)
        cotangent = c_two[r] + inverse * (scaled - wide * inverse * inverse * shift)
        c_low[r] = cotangent.astype(BF16)
        rows[r].start()
    spread = DataSpread(c_low, mini, *spread_sems)
    spread.start()
    swap.collect()
    for one in rows:
        one.relay()
    jobs.relay()
    jobs.pass_on()
    for one in rows:
        one.collect()
    for one in sums:
        one.finish()
    swap.finish()
    spread.finish()
    for one in rows:
        one.close()
    jobs.finish()


def lower(lengths, tables, q, k, v, cb_one, wo, wq, kv, c_two, x_one, gains):
    half, width = c_two.shape[1:]
    length, columns = q.shape
    gkv = shape((2, length, HD), BF16)
    return comm_call(
        lower_kernel,
        "lower",
        4,
        [SMEM] + [VMEM] * 12,
        [VMEM] + [ANY] * 3,
        [
            shape((16, 2, half, width), BF16),
            shape((8, length, columns + HD), BF16),
            shape((8, length, width // 8), BF16),
            shape((8, 2, half, width // 8), BF16),
        ],
        [
            pltpu.VMEM((length, columns), F32),
            pltpu.VMEM((length, columns), BF16),
            pltpu.VMEM(gkv.shape, BF16),
            pltpu.VMEM((length, 2 * HD), BF16),
            pltpu.VMEM((8, 2, 2, half, width), BF16),
            pltpu.VMEM((2, half, width), BF16),
        ]
        + TensorSum.scratch(width) * 2
        + TensorGather.scratch * 2
        + Cotangents.scratch(gkv)
        + DataExchange.scratch
        + DataSpread.scratch,
        (lengths,) + tables + (q, k, v, cb_one, wo, wq, kv, c_two, x_one, gains),
    )


def inner(hs, gathered, g_sum):
    g_sum[...] = jnp.zeros_like(g_sum)

    @pl.loop(0, 4)
    def _(i):
        g = gathered[pl.ds(2 * i, 2)].reshape(-1, gathered.shape[2])
        h = hs[pl.ds(2 * i, 2)].reshape(-1, hs.shape[2])
        g_sum[...] += contract(g, h, 0, 0)


def outer(ga, cs, o_sum):
    o_sum[...] = jnp.zeros(o_sum.shape, F32)

    @pl.loop(0, 4)
    def _(i):
        a = ga[pl.ds(2 * i, 2)].reshape(-1, ga.shape[-1])
        c = cs[pl.ds(2 * i, 2)].reshape(-1, cs.shape[-1])
        o_sum[...] += contract(a, c, 0, 0)


def last_kernel(*refs):
    (
        (lengths, cosine, sine, q, k, v, cb, wo, mini, ga_zero, hs, gg_one, ga, cs),
        (gg, cs_zero, q_out, g_sum, o_sum),
        (ga_sum, gq, gkv),
        (came, merged),
        sems,
        slice_sems,
    ) = taken(refs, 14, 5, 3, 2, 6, 2)
    d, t = places()
    width, columns = cb.shape[1], gq.shape[1]
    enter(NEAR)
    slices = TensorGather(mini, lambda block: cs_zero.at[:, block], *slice_sems)
    jobs = Cotangents(gq, gkv, gg, came, merged, sems)
    slices.start()
    ga_sum[...] = jnp.zeros_like(ga_sum)

    @tiles(width, TILE)
    def _(at):
        ga_sum[...] += contract(cb[:, at], wo[0, :, at], 1, 1)

    attend_back(lengths[d], cosine[...], sine[...], q, k[...], v[...], ga_sum, gq, gkv, None)
    jobs.start()
    slices.relay()
    jobs.merge()
    inner(hs, gg_one, g_sum)
    q_out[...] = g_sum[0:columns].T
    jobs.relay()
    outer(ga, cs, o_sum.at[1])
    jobs.pass_on()
    slices.finish()
    outer(ga_zero, cs_zero, o_sum.at[0])
    jobs.finish()


def last(lengths, tables, q, k, v, cb, wo, mini, *sides):
    length, columns = q.shape
    share = mini.shape[3]
    gkv = shape((2, length, HD), BF16)
    return comm_call(
        last_kernel,
        "last",
        5,
        [SMEM] + [VMEM] * 13,
        [ANY] + [VMEM] * 4,
        [
            shape((8, length, columns + HD), BF16),
            shape((8, 16) + mini.shape[1:], BF16),
            shape((share, columns), F32),
            shape((columns + HD, share), F32),
            shape((2, columns, share), F32),
        ],
        [
            pltpu.VMEM((length, columns), F32),
            pltpu.VMEM((length, columns), BF16),
            pltpu.VMEM(gkv.shape, BF16),
        ]
        + Cotangents.scratch(gkv)
        + TensorGather.scratch,
        (lengths,) + tables + (q, k, v, cb, wo, mini) + sides,
    )


def products_kernel(hs, gg, q_one, g_one, o_both, q_out, k_out, v_out, o_out, g_sum):
    columns, half = q_out.shape[2], k_out.shape[1]
    o_out[...] = o_both[...]
    inner(hs, gg, g_sum)
    q_out[0] = g_sum[0:columns].T
    q_out[1] = q_one[...]
    for layer, one in ((0, g_sum), (1, g_one)):
        k_out[layer] = one[columns : columns + half]
        v_out[layer] = one[columns + half :]


def products(*operands):
    share, columns = operands[2].shape
    half = (operands[1].shape[2] - columns) // 2
    return pl.pallas_call(
        products_kernel,
        name="products",
        in_specs=[VMEM] * 5,
        out_specs=[VMEM] * 4,
        out_shape=[
            shape((2, share, columns), F32),
            shape((2, half, share), F32),
            shape((2, half, share), F32),
            shape((2, columns, share), F32),
        ],
        scratch_shapes=[pltpu.VMEM(operands[3].shape, F32)],
        compiler_params=pltpu.CompilerParams(vmem_limit_bytes=12 * 2**20),
    )(*operands)


def rope_tables():
    angles = np.arange(LEN)[:, None] * THETA ** (-2.0 * np.arange(HD // 2) / HD)[None, :]
    cosine, sine = np.cos(angles), np.sin(angles)
    return (
        jnp.asarray(np.concatenate([cosine, cosine], axis=1), F32),
        jnp.asarray(np.concatenate([-sine, sine], axis=1), F32),
    )


def body(
    tokens,
    lengths,
    gains,
    query_weight,
    key_weight,
    value_weight,
    out_weight,
    query_probe,
    key_probe,
    value_probe,
    out_probe,
):
    rows, width = tokens.shape
    tables = rope_tables()

    def turned_over(array):
        return jnp.swapaxes(array, 1, 2)

    def all_rows(blocks):
        return blocks.reshape(-1, blocks.shape[-1])

    def by_batch(blocks):
        return blocks.reshape(blocks.shape[0], -1, blocks.shape[-1])

    probes = (query_probe, turned_over(key_probe), turned_over(value_probe), out_probe)
    q0, k0, v0, a_zero, x_one, t_one, h_one, th_one, kv, hs_zero, pq, pkv, po = head(
        lengths,
        tables,
        normed(tokens, gains),
        query_weight,
        out_weight,
        tokens.reshape(2, rows // 2, width),
        gains,
        turned_over(key_weight),
        turned_over(value_weight),
        probes,
    )
    q1, k1, v1, c_two, cb_one, ga_zero, ga_one, hs_one = turn(
        lengths,
        tables,
        query_weight,
        kv,
        pq,
        pkv,
        out_weight,
        po,
        all_rows(h_one),
        all_rows(th_one),
        t_one,
        a_zero,
    )
    cb_zero, gg_one, cs_one, mini = lower(
        lengths,
        tables,
        q1,
        k1,
        v1,
        all_rows(cb_one),
        out_weight,
        query_weight,
        kv,
        c_two,
        x_one,
        gains,
    )
    gg_zero, unused, q_one, g_one, o_both = last(
        lengths,
        tables,
        q0,
        k0,
        v0,
        all_rows(cb_zero),
        out_weight,
        mini,
        ga_zero,
        hs_one,
        gg_one,
        ga_one,
        cs_one,
    )
    q, k, v, o = products(by_batch(hs_zero), gg_zero, q_one, g_one, o_both)
    return (q, turned_over(k), turned_over(v), o)


def solution(mesh):
    placed = (
        P(("dp", "tensor"), None),
        P(),
        P(),
        P(None, None, "tensor"),
        P(None, None, "tensor"),
        P(None, None, "tensor"),
        P(None, "tensor", None),
        P(None, "dp", "tensor"),
        P(None, "dp", "tensor"),
        P(None, "dp", "tensor"),
        P(None, "tensor", "dp"),
    )
    return jax.shard_map(
        body,
        mesh=mesh,
        in_specs=placed,
        out_specs=(
            P(None, "dp", "tensor"),
            P(None, "dp", "tensor"),
            P(None, "dp", "tensor"),
            P(None, "tensor", "dp"),
        ),
        check_vma=False,
    )
```

```python
import functools
import math

import jax
import jax.numpy as jnp
import numpy as np
from jax import lax
from jax.experimental import pallas as pl
from jax.experimental.pallas import tpu as pltpu
from jax.sharding import PartitionSpec as P

HD = 128
LEN = 256
EPS = 1e-05
THETA = 500000.0

MESH = pl.DeviceIdType.MESH
F32 = jnp.float32
BF16 = jnp.bfloat16
VMEM = pl.BlockSpec(memory_space=pltpu.VMEM)
ANY = pl.BlockSpec(memory_space=pl.ANY)
HBM = pl.BlockSpec(memory_space=pltpu.HBM)
SMEM = pl.BlockSpec(memory_space=pltpu.SMEM)
DMA = pltpu.SemaphoreType.DMA
TILE = 1024

HOPS = ((1, 1), (3, 1), (2, 1), (2, 0), (1, 0), (3, 0), (0, 1))
NEAR = HOPS[3:]


def back(hop):
    return ((4 - hop[0]) % 4, hop[1])


def data_at(d, hop):
    ring, pair = lax.div(d, 2), lax.rem(d, 2)
    return lax.rem(ring + hop[0], 4) * 2 + lax.rem(pair + hop[1], 2)


def chip_at(t, hop):
    return data_at(lax.div(t, 2), hop)


def tensor_at(t, hop):
    return chip_at(t, hop) * 2 + lax.rem(t, 2)


def other_core(t):
    return t + 1 - 2 * lax.rem(t, 2)


def places():
    return lax.axis_index("dp"), lax.axis_index("tensor")


def remote(src, dst, sends, recvs, j, device):
    return pltpu.make_async_remote_copy(
        src_ref=src,
        dst_ref=dst,
        send_sem=sends.at[j],
        recv_sem=recvs.at[j],
        device_id=device,
        device_id_type=MESH,
    )


def enter(data_hops):
    d, t = places()
    barrier = pltpu.get_barrier_semaphore()
    peers = [(d, other_core(t))]
    peers += [(d, tensor_at(t, hop)) for hop in NEAR]
    peers += [(data_at(d, hop), t) for hop in data_hops]
    for peer in peers:
        pl.semaphore_signal(barrier, inc=1, device_id=peer, device_id_type=MESH)
    pl.semaphore_wait(barrier, len(peers))


def half_of(ref, half):
    if half is None:
        return ref
    rows = ref.shape[0] // 2
    return ref.at[pl.ds(half * rows, rows)]


class RingGather:
    ROUTES = ()
    FIRST = 0

    def __init__(self, src, slot, sends, recvs):
        self.src, self.slot, self.sends, self.recvs = src, slot, sends, recvs

    def out(self, j):
        hop, block, unused, half = self.ROUTES[j]
        slot = half_of(self.slot(self.place(block)), half)
        src = self.src if j < self.FIRST else slot
        return remote(src, slot, self.sends, self.recvs, j, self.device(hop))

    def into(self, j):
        slot = half_of(self.slot(self.place(self.ROUTES[j][2])), self.ROUTES[j][3])
        return remote(slot, slot, self.sends, self.recvs, j, self.device((0, 1)))

    def own(self):
        n = len(self.ROUTES)
        return pltpu.make_async_copy(self.src, self.slot(self.place((0, 0))), self.sends.at[n])

    def start(self):
        for j in range(self.FIRST):
            self.out(j).start()
        self.own().start()

    def sent(self):
        for j in range(len(self.ROUTES)):
            self.out(j).wait_send()
        self.own().wait()


class DataGather(RingGather):
    scratch = [DMA((8,)), DMA((7,))]
    FIRST = 4
    ROUTES = (
        ((0, 1), (0, 0), (0, 1), None),
        ((1, 0), (0, 0), (3, 0), None),
        ((3, 0), (0, 0), (1, 0), None),
        ((2, 0), (0, 0), (2, 0), None),
        ((1, 0), (0, 1), (3, 1), None),
        ((3, 0), (0, 1), (1, 1), None),
        ((0, 1), (2, 0), (2, 1), None),
    )

    def place(self, hop):
        d, t = places()
        return data_at(d, hop)

    def device(self, hop):
        d, t = places()
        return (data_at(d, hop), t)

    def relay(self):
        self.into(0).wait_recv()
        self.out(4).start()
        self.out(5).start()

    def pass_on(self):
        self.into(3).wait_recv()
        self.out(6).start()

    def finish(self):
        for j in (1, 2, 4, 5, 6):
            self.into(j).wait_recv()
        self.sent()


class LargeGather(DataGather):
    scratch = [DMA((12,)), DMA((11,))]
    FIRST = 3
    ROUTES = (
        ((0, 1), (0, 0), (0, 1), None),
        ((1, 0), (0, 0), (3, 0), None),
        ((3, 0), (0, 0), (1, 0), None),
        ((1, 0), (0, 1), (3, 1), 0),
        ((3, 0), (0, 1), (1, 1), 1),
        ((1, 0), (3, 0), (2, 0), 0),
        ((0, 1), (3, 0), (3, 1), 1),
        ((3, 0), (1, 0), (2, 0), 1),
        ((0, 1), (1, 0), (1, 1), 0),
        ((1, 0), (3, 1), (2, 1), 0),
        ((3, 0), (1, 1), (2, 1), 1),
    )

    def start_ring(self):
        self.out(1).start()
        self.out(2).start()
        self.own().start()

    def start_pair(self):
        self.out(0).start()

    def relay_ring(self):
        self.into(0).wait_recv()
        self.out(3).start()
        self.out(4).start()
        self.into(1).wait_recv()
        self.out(5).start()
        self.into(2).wait_recv()
        self.out(7).start()

    def relay_pair(self):
        self.out(6).start()
        self.out(8).start()

    def relay(self):
        self.relay_ring()
        self.relay_pair()

    def pass_on(self):
        for j in (3, 4):
            self.into(j).wait_recv()
            self.out(6 + j).start()

    def finish(self):
        for j in range(5, 11):
            self.into(j).wait_recv()
        self.sent()


class TensorGather(RingGather):
    scratch = [DMA((16,)), DMA((15,))]
    FIRST = 4
    ROUTES = (
        ((0, 1), (0, 0), (0, 1), None),
        ((1, 0), (0, 0), (3, 0), None),
        ((3, 0), (0, 0), (1, 0), None),
        ((2, 0), (0, 0), (2, 0), None),
        ((1, 0), (0, 1), (3, 1), None),
        ((3, 0), (0, 1), (1, 1), None),
        ((2, 0), (0, 1), (2, 1), None),
    )

    def place(self, hop):
        d, t = places()
        return tensor_at(t, hop)

    def device(self, hop):
        d, t = places()
        return (d, tensor_at(t, hop))

    def handover(self, j, src, block):
        d, t = places()
        return pltpu.make_async_remote_copy(
            src_ref=src,
            dst_ref=self.slot(block),
            send_sem=self.sends.at[8 + j],
            recv_sem=self.recvs.at[7 + j],
            device_id=(d, other_core(t)),
            device_id_type=MESH,
        )

    def hand(self, j):
        block = self.place(self.ROUTES[j][2])
        return self.handover(j, self.slot(block), block)

    def near(self):
        return self.handover(7, self.src, self.place((0, 0)))

    def start(self):
        super().start()
        self.near().start()

    def relay(self):
        self.into(0).wait_recv()
        for j in range(4, 7):
            self.out(j).start()
        self.hand(0).start()

    def collect(self):
        for j in range(1, 7):
            self.into(j).wait_recv()
            self.hand(j).start()

    def close(self):
        self.sent()
        d, t = places()
        far = other_core(t)
        self.handover(7, self.slot(far), far).wait_recv()
        self.near().wait_send()
        for j in range(7):
            block = tensor_at(far, self.ROUTES[j][2])
            self.handover(j, self.slot(block), block).wait_recv()
            self.hand(j).wait_send()

    def finish(self):
        self.collect()
        self.close()


class TensorSum:
    STEPS = ((2, 1), (1, 1), (3, 1), (2, 0), (1, 0), (3, 0))
    BLOCKS = STEPS + ((0, 1), (0, 0))

    @staticmethod
    def scratch(columns):
        return [
            pltpu.VMEM((8, 8, columns), BF16),
            pltpu.VMEM((7, 8, columns), BF16),
            pltpu.VMEM((7, 8, columns), BF16),
            DMA((15,)),
            DMA((15,)),
        ]

    def __init__(self, rows, part, near, sent, far, sends, recvs):
        self.rows = rows
        self.part, self.near_, self.sent, self.far = part, near, sent, far
        self.sends, self.recvs = sends, recvs

    def swap(self, j):
        d, t = places()
        k = chip_at(t, self.BLOCKS[j])
        c = lax.rem(t, 2)
        return remote(
            self.part.at[k, 1 - c, self.rows], self.near_.at[k], self.sends, self.recvs, j, (d, other_core(t))
        )

    def cross(self, j):
        d, t = places()
        hop = (self.STEPS[j][0], 0) if j < 6 else (0, 1)
        return remote(
            self.sent.at[j], self.far.at[j], self.sends, self.recvs, 8 + j, (d, tensor_at(t, hop))
        )

    def pair_sum(self, j):
        d, t = places()
        k = chip_at(t, self.BLOCKS[j])
        c = lax.rem(t, 2)
        return self.part[k, c, self.rows].astype(F32) + self.near_[k].astype(F32)

    def start(self):
        for j in range(8):
            self.swap(j).start()

    def send(self):
        for j in range(6):
            self.swap(j).wait_recv()
            self.sent[j] = self.pair_sum(j).astype(BF16)
            self.cross(j).start()

    def middle(self):
        self.swap(6).wait_recv()
        total = self.pair_sum(6)
        for j in (1, 2, 0):
            self.cross(j).wait_recv()
            total = total + self.far[j].astype(F32)
        self.sent[6] = total.astype(BF16)
        self.cross(6).start()

    def total(self):
        self.swap(7).wait_recv()
        total = self.pair_sum(7)
        for j in (4, 5, 3, 6):
            self.cross(j).wait_recv()
            total = total + self.far[j].astype(F32)
        return total

    def finish(self):
        for j in range(8):
            self.swap(j).wait_send()
        for j in range(7):
            self.cross(j).wait_send()


class DataSpread:
    scratch = [DMA((8,)), DMA((7,))]

    def __init__(self, src, out, sends, recvs):
        self.src, self.out_, self.sends, self.recvs = src, out, sends, recvs
        self.share = src.shape[-1] // 8

    def columns(self, d):
        return pl.ds(pl.multiple_of(d * self.share, self.share), self.share)

    def cut(self, d):
        return self.src.at[(slice(None),) * (len(self.src.shape) - 1) + (self.columns(d),)]

    def cross(self, j):
        d, t = places()
        peer = data_at(d, HOPS[j])
        return remote(
            self.cut(peer),
            self.out_.at[d],
            self.sends,
            self.recvs,
            j,
            (peer, t),
        )

    def arrived(self, j):
        d, t = places()
        slot = self.out_.at[data_at(d, back(HOPS[j]))]
        return remote(slot, slot, self.sends, self.recvs, j, (d, other_core(t)))

    def own(self):
        d, t = places()
        return pltpu.make_async_copy(
            self.cut(d), self.out_.at[d], self.sends.at[7]
        )

    def start(self):
        for j in range(7):
            self.cross(j).start()
        self.own().start()

    def finish(self):
        for j in range(7):
            self.arrived(j).wait_recv()
            self.cross(j).wait_send()
        self.own().wait()


class DataExchange:
    scratch = [DMA((15,)), DMA((14,))]

    def __init__(self, src, out, sends, recvs):
        self.src, self.out_, self.sends, self.recvs = src, out, sends, recvs
        self.half = src.shape[0] // 2
        self.share = src.shape[1] // 8

    def rows(self, t):
        return pl.ds(pl.multiple_of(lax.rem(t, 2) * self.half, self.half), self.half)

    def columns(self, d):
        return pl.ds(pl.multiple_of(d * self.share, self.share), self.share)

    def cross(self, j):
        d, t = places()
        peer = data_at(d, HOPS[j])
        return remote(
            self.src.at[self.rows(t), self.columns(peer)],
            self.out_.at[d, self.rows(t)],
            self.sends,
            self.recvs,
            j,
            (peer, t),
        )

    def landing(self, j, t_of):
        d, t = places()
        slot = self.out_.at[data_at(d, back(HOPS[j])), self.rows(t_of)]
        return slot

    def arrived(self, j):
        d, t = places()
        slot = self.landing(j, t)
        return remote(slot, slot, self.sends, self.recvs, j, (d, other_core(t)))

    def handed(self, j):
        d, t = places()
        slot = self.landing(j, t)
        return remote(slot, slot, self.sends, self.recvs, 7 + j, (d, other_core(t)))

    def received(self, j):
        d, t = places()
        slot = self.landing(j, other_core(t))
        return remote(slot, slot, self.sends, self.recvs, 7 + j, (d, other_core(t)))

    def own(self):
        d, t = places()
        return pltpu.make_async_copy(
            self.src.at[:, self.columns(d)], self.out_.at[d], self.sends.at[14]
        )

    def start(self):
        for j in (3, 4, 5):
            self.cross(j).start()
        self.own().start()

    def start_pairs(self):
        for j in (6, 0, 1, 2):
            self.cross(j).start()

    def collect(self):
        for j in (4, 5, 3, 6, 0, 1, 2):
            self.arrived(j).wait_recv()
            self.handed(j).start()

    def finish(self):
        for j in range(7):
            self.received(j).wait_recv()
            self.cross(j).wait_send()
            self.handed(j).wait_send()
        self.own().wait()


def taken(refs, *counts):
    out, at = [], 0
    for count in counts:
        out.append(refs[at : at + count])
        at += count
    return out


def comm_call(kernel, name, number, in_specs, out_specs, out_shape, scratch, args, limit=12):
    return pl.pallas_call(
        kernel,
        name=name,
        in_specs=in_specs,
        out_specs=out_specs,
        out_shape=out_shape,
        scratch_shapes=scratch,
        cost_estimate=pl.CostEstimate(flops=10**10, bytes_accessed=0, transcendentals=0),
        compiler_params=pltpu.CompilerParams(
            collective_id=number, has_side_effects=True, vmem_limit_bytes=limit * 2**20
        ),
    )(*args)


def shape(dims, dtype):
    return jax.ShapeDtypeStruct(dims, dtype)


def slot_of(ref):
    return lambda block: ref.at[block]


def rows_of(ref, count):
    size = ref.shape[0] // count
    return lambda block: ref.at[pl.ds(pl.multiple_of(block * size, size), size)]


def half_slot(ref, half):
    return lambda block: ref.at[block, half]


def columns_of(ref):
    width = ref.shape[1] // 8
    return lambda block: ref.at[:, pl.ds(pl.multiple_of(block * width, width), width)]


def mean_of(values):
    return jnp.sum(values, axis=-1, keepdims=True) * (1.0 / values.shape[-1])


def strip(which, core):
    return pl.ds(pl.multiple_of(which * 128 + core * 64, 64), 64)


class CoreShare:
    scratch = [DMA((2,)), DMA((2,))]

    def __init__(self, sources, slot, sends, recvs):
        self.sources, self.slot, self.sends, self.recvs = sources, slot, sends, recvs

    def copy(self, j, core):
        d, t = places()
        slot = self.slot(j, core)
        src = slot if self.sources is None else self.sources[j]
        return remote(src, slot, self.sends, self.recvs, j, (d, other_core(t)))

    def start(self):
        d, t = places()
        for j in range(2):
            self.copy(j, lax.rem(t, 2)).start()

    def finish(self):
        d, t = places()
        for j in range(2):
            self.copy(j, 1 - lax.rem(t, 2)).wait_recv()
            self.copy(j, lax.rem(t, 2)).wait_send()


class Probes:
    COUNT = 4
    @staticmethod
    def scratch(kind):
        return kind.scratch * 4 + CoreShare.scratch

    def __init__(self, kind, layer, probes, gathered, sems):
        q, k, v, o = probes
        gq, gkv, go = gathered
        d, t = places()
        core = lax.rem(t, 2)
        width = k.shape[2]

        def part(which):
            return lambda block: gkv.at[
                strip(which, core), pl.ds(pl.multiple_of(block * width, width), width)
            ]

        self.jobs = [
            kind(k.at[layer], part(0), *sems[0:2]),
            kind(v.at[layer], part(1), *sems[2:4]),
            kind(q.at[layer], rows_of(gq, 8), *sems[4:6]),
            kind(o.at[layer], columns_of(go), *sems[6:8]),
        ]
        self.share = CoreShare(None, lambda j, c: gkv.at[strip(j, c)], *sems[8:10])

    @staticmethod
    def shapes(probes):
        q, k, v, o = probes
        return [
            shape((8 * q.shape[1], q.shape[2]), BF16),
            shape((4 * k.shape[1], 8 * k.shape[2]), BF16),
            shape((o.shape[1], 8 * o.shape[2]), BF16),
        ]

    def start(self):
        for job in self.jobs:
            job.start()

    def relay(self):
        for job in self.jobs:
            job.relay()

    def pass_on(self):
        for job in self.jobs:
            job.pass_on()

    def finish(self):
        for job in self.jobs[:2]:
            job.finish()
        self.share.start()
        for job in self.jobs[2:]:
            job.finish()
        self.share.finish()


def contract(left_side, right_side, left_dim, right_dim):
    return lax.dot_general(
        left_side,
        right_side,
        (((left_dim,), (right_dim,)), ((), ())),
        preferred_element_type=F32,
    )


def turned(values, cosine, sine):
    return values * cosine + pltpu.roll(values, values.shape[1] // 2, 1) * sine


def attention_weights(q, k, length):
    size = q.shape[0]
    row = lax.broadcasted_iota(jnp.int32, (size, size), 0)
    column = lax.broadcasted_iota(jnp.int32, (size, size), 1)
    allowed = (column <= row) & (column < length)
    scores = contract(q, k, 1, 1) * (1.0 / math.sqrt(q.shape[1]))
    powers = jnp.where(allowed, jnp.exp(scores), 0.0)
    return powers / jnp.sum(powers, axis=-1, keepdims=True)


def attend(length, cos, sin, sums, q_out, k_out, v_out, a_out, ta_out):
    q_sum, tq_sum, kv_sum, tkv_sum = sums
    scaling = 1.0 / math.sqrt(HD)
    k = turned(kv_sum[:, 0:HD], cos, sin).astype(BF16)
    v = kv_sum[:, HD:].astype(BF16)
    tk = turned(tkv_sum[:, 0:HD], cos, sin).astype(BF16)
    tv = tkv_sum[:, HD:].astype(BF16)
    k_out[...] = k
    v_out[...] = v
    for at in range(0, q_sum.shape[1], HD):
        head = slice(at, at + HD)
        q = turned(q_sum[:, head], cos, sin).astype(BF16)
        tq = turned(tq_sum[:, head], cos, sin).astype(BF16)
        q_out[:, head] = q
        weights = attention_weights(q, k, length)
        low = weights.astype(BF16)
        a_out[:, head] = contract(low, v, 1, 0).astype(BF16)
        scores = (contract(tq, k, 1, 1) + contract(q, tk, 1, 1)) * scaling
        change = weights * (scores - jnp.sum(weights * scores, axis=-1, keepdims=True))
        ta = contract(change.astype(BF16), v, 1, 0) + contract(low, tv, 1, 0)
        ta_out[:, head] = ta.astype(BF16)


def attend_primal(length, cos, sin, q_sum, kv_sum, q_out, k_out, v_out, a_out, w_out):
    k = turned(kv_sum[:, 0:HD], cos, sin).astype(BF16)
    v = kv_sum[:, HD:].astype(BF16)
    k_out[...] = k
    v_out[...] = v
    for n, at in enumerate(range(0, q_sum.shape[1], HD)):
        head = slice(at, at + HD)
        q = turned(q_sum[:, head], cos, sin).astype(BF16)
        q_out[:, head] = q
        weights = attention_weights(q, k, length)
        w_out[n] = weights
        a_out[:, head] = contract(weights.astype(BF16), v, 1, 0).astype(BF16)


def attend_tangent(cos, sin, tq_sum, tkv_sum, q_in, k, v, w_in, ta_out):
    scaling = 1.0 / math.sqrt(HD)
    tk = turned(tkv_sum[:, 0:HD], cos, sin).astype(BF16)
    tv = tkv_sum[:, HD:].astype(BF16)
    for n, at in enumerate(range(0, tq_sum.shape[1], HD)):
        head = slice(at, at + HD)
        tq = turned(tq_sum[:, head], cos, sin).astype(BF16)
        weights = w_in[n]
        low = weights.astype(BF16)
        scores = (contract(tq, k, 1, 1) + contract(q_in[:, head], tk, 1, 1)) * scaling
        change = weights * (scores - jnp.sum(weights * scores, axis=-1, keepdims=True))
        ta = contract(change.astype(BF16), v, 1, 0) + contract(low, tv, 1, 0)
        ta_out[:, head] = ta.astype(BF16)


def attend_back(length, cos, sin, q_in, k, v, ga_sum, gq_out, gkv_out, gkv_low):
    scaling = 1.0 / math.sqrt(HD)
    gk, gv = None, None
    for at in range(0, ga_sum.shape[1], HD):
        head = slice(at, at + HD)
        q = q_in[:, head]
        ga = ga_sum[:, head].astype(BF16)
        weights = attention_weights(q, k, length)
        grads = contract(ga, v, 1, 1)
        value = contract(weights.astype(BF16), ga, 0, 0)
        scores = (
            weights * (grads - jnp.sum(weights * grads, axis=-1, keepdims=True)) * scaling
        ).astype(BF16)
        gq_out[:, head] = turned(contract(scores, k, 1, 0), cos, -sin).astype(BF16)
        key = contract(scores, q, 0, 0)
        gk = key if gk is None else gk + key
        gv = value if gv is None else gv + value
    gk = turned(gk, cos, -sin).astype(BF16)
    gv = gv.astype(BF16)
    half = HD // 2
    if gkv_low is not None:
        gkv_low[:, 0:HD] = gk
        gkv_low[:, HD:] = gv
    gkv_out[0] = jnp.concatenate([gk[:, 0:half], gv[:, 0:half]], axis=-1)
    gkv_out[1] = jnp.concatenate([gk[:, half:], gv[:, half:]], axis=-1)


def tiles(width, size):
    def over(function):
        @pl.loop(0, width // size)
        def _(i):
            function(pl.ds(pl.multiple_of(i * size, size), size))

    return over


def store_by_owner(part, columns, values):
    dims = part.shape[:-1] + (values.shape[1],)
    part[:, :, :, :, columns] = values.reshape(dims).astype(BF16)


def normed_kernel(tokens, gains, h_low):
    wide = tokens[...].astype(F32)
    inverse = lax.rsqrt(mean_of(wide * wide) + EPS)
    h_low[...] = (wide * inverse * gains[0:1]).astype(BF16)


def normed(tokens, gains):
    return pl.pallas_call(
        normed_kernel,
        name="normed",
        in_specs=[VMEM, VMEM],
        out_specs=VMEM,
        out_shape=shape(tokens.shape, BF16),
        cost_estimate=pl.CostEstimate(flops=10**10, bytes_accessed=0, transcendentals=0),
        compiler_params=pltpu.CompilerParams(vmem_limit_bytes=8 * 2**20),
    )(tokens, gains)


def head_kernel(*refs):
    (
        (lengths, cosine, sine, h_low, wq, wo, tokens, gains, kw, vw, q, k, v, o),
        (q_out, k_out, v_out, a_out, x_out, t_out, h_all, th_all, kv, hs, gq, gkv, go),
        (mini, h_zero, pq, pkv, po, weights, ta_low, part, h_one, th_one),
        sums_f32,
        sum_refs,
        gather_refs,
        spread_sems,
        share_sems,
        own_sems,
        zero_sems,
        one_sems,
    ) = taken(refs, 14, 13, 10, 4, 20, 12, 2, 2, 1, 10, 10)
    d, t = places()
    core = lax.rem(t, 2)
    width = h_zero.shape[1]
    gain = gains[1:2]
    cos, sin = cosine[...], sine[...]
    enter(HOPS)
    lots = taken(sum_refs, 5, 5, 5, 5)
    primals = [TensorSum(r, part, *lots[r]) for r in range(2)]
    moves = [TensorSum(r, part, *lots[2 + r]) for r in range(2)]
    lots = taken(gather_refs, 2, 2, 2, 2, 2, 2)
    rows = TensorGather(h_low, rows_of(h_zero, 16), *lots[0])
    slices = TensorGather(mini, lambda block: hs.at[:, block], *lots[1])
    rows_h = [TensorGather(h_one.at[r], half_slot(h_all, r), *lots[2 + r]) for r in range(2)]
    rows_th = [TensorGather(th_one.at[r], half_slot(th_all, r), *lots[4 + r]) for r in range(2)]
    spread = DataSpread(h_low, mini, *spread_sems)
    share = CoreShare((kw, vw), lambda j, c: kv.at[:, strip(j, c)], *share_sems)
    own = [
        pltpu.make_async_copy(src, kv.at[:, strip(j, core)], own_sems[0].at[j])
        for j, src in enumerate((kw, vw))
    ]
    zeros = Probes(LargeGather, 0, (q, k, v, o), (pq, pkv, po), zero_sems)
    ones = Probes(LargeGather, 1, (q, k, v, o), (gq, gkv, go), one_sems)

    spread.start()
    rows.start()
    zeros.start()
    share.start()
    for copy in own:
        copy.start()
    q_sum, tq_sum, kv_sum, tkv_sum = sums_f32
    for one in sums_f32:
        one[...] = jnp.zeros_like(one)
    rows.relay()
    spread.finish()
    slices.start()
    for job in zeros.jobs[:3]:
        job.relay()
    rows.finish()
    zeros.jobs[3].relay()
    slices.relay()
    share.finish()
    for copy in own:
        copy.wait()

    @tiles(width, 2 * TILE)
    def _(at):
        h = h_zero[:, at]
        q_sum[...] += contract(h, wq[0, at], 1, 0)
        kv_sum[...] += contract(h, kv[0, :, at], 1, 1)

    attend_primal(lengths[d], cos, sin, q_sum, kv_sum, q_out, k_out, v_out, a_out, weights)

    @tiles(width, TILE)
    def _(at):
        store_by_owner(part, at, contract(a_out[...], wo[0, :, at], 1, 0))

    for one in primals:
        one.start()
    for job in zeros.jobs[:2]:
        job.pass_on()
    for one in primals:
        one.send()
    for job in zeros.jobs[2:]:
        job.pass_on()
    for job in ones.jobs:
        job.start_ring()
    for one in primals:
        one.middle()
    for r in range(2):
        stream = (tokens[r].astype(F32) + primals[r].total()).astype(BF16)
        x_out[r] = stream
        wide = stream.astype(F32)
        inverse = lax.rsqrt(mean_of(wide * wide) + EPS)
        h_one[r] = (wide * inverse * gain).astype(BF16)
        rows_h[r].start()
    for job in ones.jobs:
        job.start_pair()
    for one in primals:
        one.finish()
    zeros.finish()

    @tiles(width, 2 * TILE)
    def _(at):
        h = h_zero[:, at]
        tq_sum[...] += contract(h, pq[at], 1, 0)
        tkv_sum[...] += contract(h, pkv[:, at], 1, 1)

    for one in rows_h:
        one.relay()
    attend_tangent(cos, sin, tq_sum, tkv_sum, q_out, k_out[...], v_out[...], weights, ta_low)

    @tiles(width, TILE)
    def _(at):
        term = contract(ta_low[...], wo[0, :, at], 1, 0) + contract(a_out[...], po[:, at], 1, 0)
        store_by_owner(part, at, term)

    for one in moves:
        one.start()
    for one in moves:
        one.send()
    for job in ones.jobs:
        job.relay_ring()
    for one in moves:
        one.middle()
    for r in range(2):
        tangent = moves[r].total()
        t_out[r] = tangent
        wide = x_out[r].astype(F32)
        inverse = lax.rsqrt(mean_of(wide * wide) + EPS)
        shift = mean_of(wide * tangent)
        th_one[r] = (
            gain * (tangent * inverse - wide * inverse * inverse * inverse * shift)
        ).astype(BF16)
        rows_th[r].start()
    for job in ones.jobs:
        job.relay_pair()
    for one in rows_th:
        one.relay()
    ones.pass_on()
    slices.collect()
    for one in rows_h + rows_th:
        one.collect()
    for one in moves:
        one.finish()
    slices.close()
    for one in rows_h + rows_th:
        one.close()
    ones.finish()


def head(lengths, tables, h_low, wq, wo, tokens, gains, kw, vw, probes):
    half, width = tokens.shape[1:]
    columns = wq.shape[2]
    wide = pltpu.VMEM((LEN, columns), F32)
    return comm_call(
        head_kernel,
        "head",
        1,
        [SMEM] + [VMEM] * 7 + [HBM] * 6,
        [VMEM] * 9 + [ANY] * 4,
        [
            shape((LEN, columns), BF16),
            shape((LEN, HD), BF16),
            shape((LEN, HD), BF16),
            shape((LEN, columns), BF16),
            shape((2, half, width), BF16),
            shape((2, half, width), F32),
            shape((16, 2, half, width), BF16),
            shape((16, 2, half, width), BF16),
            shape((2, 4 * kw.shape[1], width), BF16),
            shape((8, 16, 2 * half, width // 8), BF16),
        ]
        + Probes.shapes(probes),
        [pltpu.VMEM((8, 2 * half, width // 8), BF16), pltpu.VMEM((LEN, width), BF16)]
        + [pltpu.VMEM(one.shape, BF16) for one in Probes.shapes(probes)]
        + [pltpu.VMEM((columns // HD, LEN, LEN), F32), pltpu.VMEM((LEN, columns), BF16)]
        + [pltpu.VMEM((8, 2, 2, half, width), BF16)]
        + [pltpu.VMEM((2, half, width), BF16)] * 2
        + [wide] * 4
        + TensorSum.scratch(width) * 4
        + TensorGather.scratch * 6
        + DataSpread.scratch
        + CoreShare.scratch
        + [DMA((2,))]
        + Probes.scratch(LargeGather) * 2,
        (lengths,) + tables + (h_low, wq, wo, tokens, gains, kw, vw) + probes,
        limit=19,
    )


def turn_kernel(*refs):
    (
        (lengths, cosine, sine, wq, kv, pq, pkv, wo, po, h_one, th_one, t_one, a_zero),
        (q_out, k_out, v_out, c_out, cb_all, ga_zero, ga_one, hs_one),
        (a_one, ta_low, part, c_low),
        sums_f32,
        sum_refs,
        gather_refs,
        sems,
    ) = taken(refs, 13, 8, 4, 4, 10, 4, 6)
    d, t = places()
    width = h_one.shape[1]
    enter(HOPS)
    lots = taken(sum_refs, 5, 5)
    sums = [TensorSum(r, part, *lots[r]) for r in range(2)]
    lots = taken(gather_refs, 2, 2)
    rows = [TensorGather(c_low.at[r], half_slot(cb_all, r), *lots[r]) for r in range(2)]
    jobs = [
        DataGather(a_zero, slot_of(ga_zero), *sems[0:2]),
        DataGather(a_one, slot_of(ga_one), *sems[2:4]),
    ]
    swap = DataExchange(h_one, hs_one, *sems[4:6])
    jobs[0].start()
    swap.start()
    swap.start_pairs()
    q_sum, tq_sum, kv_sum, tkv_sum = sums_f32
    for one in sums_f32:
        one[...] = jnp.zeros_like(one)

    @tiles(width, 2 * TILE)
    def _(at):
        h, th = h_one[:, at], th_one[:, at]
        w, k = wq[1, at], kv[1, :, at]
        q_sum[...] += contract(h, w, 1, 0)
        kv_sum[...] += contract(h, k, 1, 1)
        tq_sum[...] += contract(h, pq[at], 1, 0) + contract(th, w, 1, 0)
        tkv_sum[...] += contract(h, pkv[:, at], 1, 1) + contract(th, k, 1, 1)

    attend(lengths[d], cosine[...], sine[...], sums_f32, q_out, k_out, v_out, a_one, ta_low)
    jobs[1].start()
    jobs[0].relay()

    @tiles(width, TILE)
    def _(at):
        moved = contract(ta_low[...], wo[1, :, at], 1, 0) + contract(a_one[...], po[:, at], 1, 0)
        store_by_owner(part, at, moved)

    for one in sums:
        one.start()
    for one in sums:
        one.send()
    for one in sums:
        one.middle()
    half = t_one.shape[1]
    for r in range(2):
        position = (2 * t + r) * half + lax.broadcasted_iota(jnp.int32, t_one.shape[1:], 0)
        mask = jnp.where(position < lengths[d], 1.0, 0.0)
        cotangent = mask * (t_one[r] + sums[r].total())
        c_out[r] = cotangent
        c_low[r] = cotangent.astype(BF16)
        rows[r].start()
    swap.collect()
    rows[0].relay()
    rows[1].relay()
    jobs[1].relay()
    for job in jobs:
        job.pass_on()
    for one in rows:
        one.collect()
    for one in sums:
        one.finish()
    swap.finish()
    for one in rows:
        one.close()
    for job in jobs:
        job.finish()


def turn(lengths, tables, wq, kv, pq, pkv, wo, po, h_one, th_one, t_one, a_zero):
    half, width = t_one.shape[1:]
    length, columns = a_zero.shape
    return comm_call(
        turn_kernel,
        "turn",
        3,
        [SMEM] + [VMEM] * 12,
        [VMEM] * 5 + [ANY] * 3,
        [
            shape((length, columns), BF16),
            shape((length, HD), BF16),
            shape((length, HD), BF16),
            shape((2, half, width), F32),
            shape((16, 2, half, width), BF16),
            shape((8,) + a_zero.shape, BF16),
            shape((8,) + a_zero.shape, BF16),
            shape((8, length, width // 8), BF16),
        ],
        [
            pltpu.VMEM((length, columns), BF16),
            pltpu.VMEM((length, columns), BF16),
            pltpu.VMEM((8, 2, 2, half, width), BF16),
            pltpu.VMEM((2, half, width), BF16),
            pltpu.VMEM((length, columns), F32),
            pltpu.VMEM((length, columns), F32),
            pltpu.VMEM((length, 2 * HD), F32),
            pltpu.VMEM((length, 2 * HD), F32),
        ]
        + TensorSum.scratch(width) * 2
        + TensorGather.scratch * 2
        + DataGather.scratch * 2
        + DataExchange.scratch,
        (lengths,) + tables + (wq, kv, pq, pkv, wo, po, h_one, th_one, t_one, a_zero),
    )


class Cotangents:
    def __init__(self, gq, gkv, gathered, came, merged, sems):
        self.gkv, self.came, self.merged = gkv, came, merged
        width = gq.shape[1]
        self.jobs = [
            DataGather(gq, lambda block: gathered.at[block, :, 0:width], *sems[0:2]),
            DataGather(
                merged,
                lambda block: gathered.at[block, :, width : width + merged.shape[1]],
                *sems[2:4],
            ),
        ]
        self.sends, self.recvs = sems[4:6]

    @staticmethod
    def scratch(gkv):
        return (
            [pltpu.VMEM(gkv.shape[1:], BF16)] * 2
            + DataGather.scratch * 2
            + [DMA((1,)), DMA((1,))]
        )

    def swap(self):
        d, t = places()
        return remote(
            self.gkv.at[1 - lax.rem(t, 2)],
            self.came,
            self.sends,
            self.recvs,
            0,
            (d, other_core(t)),
        )

    def start(self):
        self.swap().start()
        self.jobs[0].start()

    def merge(self):
        d, t = places()
        self.swap().wait()
        mine = self.gkv[lax.rem(t, 2)].astype(F32) + self.came[...].astype(F32)
        self.merged[...] = mine.astype(BF16)
        self.jobs[1].start()

    def relay(self):
        for job in self.jobs:
            job.relay()

    def pass_on(self):
        for job in self.jobs:
            job.pass_on()

    def finish(self):
        for job in self.jobs:
            job.finish()


def lower_kernel(*refs):
    (
        (lengths, cosine, sine, q, k, v, cb_one, wo, wq, kv, c_two, x_one, gains),
        (cb_all, gg, cbs, mini),
        (ga_sum, gq, gkv, gkv_low, part, c_low),
        sum_refs,
        gather_refs,
        (came, merged),
        sems,
        swap_sems,
        spread_sems,
    ) = taken(refs, 13, 4, 6, 10, 4, 2, 6, 2, 2)
    d, t = places()
    width = cb_one.shape[1]
    enter(HOPS)
    lots = taken(sum_refs, 5, 5)
    sums = [TensorSum(r, part, *lots[r]) for r in range(2)]
    lots = taken(gather_refs, 2, 2)
    rows = [TensorGather(c_low.at[r], half_slot(cb_all, r), *lots[r]) for r in range(2)]
    jobs = Cotangents(gq, gkv, gg, came, merged, sems)
    swap = DataExchange(cb_one, cbs, *swap_sems)
    swap.start()
    swap.start_pairs()
    ga_sum[...] = jnp.zeros_like(ga_sum)

    @tiles(width, 2 * TILE)
    def _(at):
        ga_sum[...] += contract(cb_one[:, at], wo[1, :, at], 1, 1)

    attend_back(
        lengths[d], cosine[...], sine[...], q, k[...], v[...], ga_sum, gq, gkv, gkv_low
    )
    jobs.start()

    @tiles(width, TILE)
    def _(at):
        term = contract(gq[...], wq[1, at], 1, 1) + contract(gkv_low[...], kv[1, :, at], 1, 0)
        store_by_owner(part, at, term)

    for one in sums:
        one.start()
    jobs.merge()
    for one in sums:
        one.send()
    for one in sums:
        one.middle()
    for r in range(2):
        scaled = sums[r].total() * gains[1:2]
        wide = x_one[r].astype(F32)
        inverse = lax.rsqrt(mean_of(wide * wide) + EPS)
        shift = mean_of(wide * scaled)
        cotangent = c_two[r] + inverse * (scaled - wide * inverse * inverse * shift)
        c_low[r] = cotangent.astype(BF16)
        rows[r].start()
    spread = DataSpread(c_low, mini, *spread_sems)
    spread.start()
    swap.collect()
    for one in rows:
        one.relay()
    jobs.relay()
    jobs.pass_on()
    for one in rows:
        one.collect()
    for one in sums:
        one.finish()
    swap.finish()
    spread.finish()
    for one in rows:
        one.close()
    jobs.finish()


def lower(lengths, tables, q, k, v, cb_one, wo, wq, kv, c_two, x_one, gains):
    half, width = c_two.shape[1:]
    length, columns = q.shape
    gkv = shape((2, length, HD), BF16)
    return comm_call(
        lower_kernel,
        "lower",
        4,
        [SMEM] + [VMEM] * 12,
        [VMEM] + [ANY] * 3,
        [
            shape((16, 2, half, width), BF16),
            shape((8, length, columns + HD), BF16),
            shape((8, length, width // 8), BF16),
            shape((8, 2, half, width // 8), BF16),
        ],
        [
            pltpu.VMEM((length, columns), F32),
            pltpu.VMEM((length, columns), BF16),
            pltpu.VMEM(gkv.shape, BF16),
            pltpu.VMEM((length, 2 * HD), BF16),
            pltpu.VMEM((8, 2, 2, half, width), BF16),
            pltpu.VMEM((2, half, width), BF16),
        ]
        + TensorSum.scratch(width) * 2
        + TensorGather.scratch * 2
        + Cotangents.scratch(gkv)
        + DataExchange.scratch
        + DataSpread.scratch,
        (lengths,) + tables + (q, k, v, cb_one, wo, wq, kv, c_two, x_one, gains),
    )


def inner(hs, gathered, g_sum):
    g_sum[...] = jnp.zeros_like(g_sum)

    @pl.loop(0, 4)
    def _(i):
        g = gathered[pl.ds(2 * i, 2)].reshape(-1, gathered.shape[2])
        h = hs[pl.ds(2 * i, 2)].reshape(-1, hs.shape[2])
        g_sum[...] += contract(g, h, 0, 0)


def outer(ga, cs, o_sum):
    o_sum[...] = jnp.zeros(o_sum.shape, F32)

    @pl.loop(0, 4)
    def _(i):
        a = ga[pl.ds(2 * i, 2)].reshape(-1, ga.shape[-1])
        c = cs[pl.ds(2 * i, 2)].reshape(-1, cs.shape[-1])
        o_sum[...] += contract(a, c, 0, 0)


def last_kernel(*refs):
    (
        (lengths, cosine, sine, q, k, v, cb, wo, mini, ga_zero, hs, gg_one, ga, cs),
        (gg, cs_zero, q_out, g_sum, o_sum),
        (ga_sum, gq, gkv),
        (came, merged),
        sems,
        slice_sems,
    ) = taken(refs, 14, 5, 3, 2, 6, 2)
    d, t = places()
    width, columns = cb.shape[1], gq.shape[1]
    enter(NEAR)
    slices = TensorGather(mini, lambda block: cs_zero.at[:, block], *slice_sems)
    jobs = Cotangents(gq, gkv, gg, came, merged, sems)
    slices.start()
    ga_sum[...] = jnp.zeros_like(ga_sum)

    @tiles(width, 2 * TILE)
    def _(at):
        ga_sum[...] += contract(cb[:, at], wo[0, :, at], 1, 1)

    attend_back(lengths[d], cosine[...], sine[...], q, k[...], v[...], ga_sum, gq, gkv, None)
    jobs.start()
    slices.relay()
    jobs.merge()
    inner(hs, gg_one, g_sum)
    q_out[...] = g_sum[0:columns].T
    jobs.relay()
    outer(ga, cs, o_sum.at[1])
    jobs.pass_on()
    slices.finish()
    outer(ga_zero, cs_zero, o_sum.at[0])
    jobs.finish()


def last(lengths, tables, q, k, v, cb, wo, mini, *sides):
    length, columns = q.shape
    share = mini.shape[3]
    gkv = shape((2, length, HD), BF16)
    return comm_call(
        last_kernel,
        "last",
        5,
        [SMEM] + [VMEM] * 13,
        [ANY] + [VMEM] * 4,
        [
            shape((8, length, columns + HD), BF16),
            shape((8, 16) + mini.shape[1:], BF16),
            shape((share, columns), F32),
            shape((columns + HD, share), F32),
            shape((2, columns, share), F32),
        ],
        [
            pltpu.VMEM((length, columns), F32),
            pltpu.VMEM((length, columns), BF16),
            pltpu.VMEM(gkv.shape, BF16),
        ]
        + Cotangents.scratch(gkv)
        + TensorGather.scratch,
        (lengths,) + tables + (q, k, v, cb, wo, mini) + sides,
    )


def products_kernel(hs, gg, q_one, g_one, o_both, q_out, k_out, v_out, o_out, g_sum):
    columns, half = q_out.shape[2], k_out.shape[1]
    o_out[...] = o_both[...]
    inner(hs, gg, g_sum)
    q_out[0] = g_sum[0:columns].T
    q_out[1] = q_one[...]
    for layer, one in ((0, g_sum), (1, g_one)):
        k_out[layer] = one[columns : columns + half]
        v_out[layer] = one[columns + half :]


def products(*operands):
    share, columns = operands[2].shape
    half = (operands[1].shape[2] - columns) // 2
    return pl.pallas_call(
        products_kernel,
        name="products",
        in_specs=[VMEM] * 5,
        out_specs=[VMEM] * 4,
        out_shape=[
            shape((2, share, columns), F32),
            shape((2, half, share), F32),
            shape((2, half, share), F32),
            shape((2, columns, share), F32),
        ],
        scratch_shapes=[pltpu.VMEM(operands[3].shape, F32)],
        compiler_params=pltpu.CompilerParams(vmem_limit_bytes=12 * 2**20),
    )(*operands)


def rope_tables():
    angles = np.arange(LEN)[:, None] * THETA ** (-2.0 * np.arange(HD // 2) / HD)[None, :]
    cosine, sine = np.cos(angles), np.sin(angles)
    return (
        jnp.asarray(np.concatenate([cosine, cosine], axis=1), F32),
        jnp.asarray(np.concatenate([-sine, sine], axis=1), F32),
    )


def body(
    tokens,
    lengths,
    gains,
    query_weight,
    key_weight,
    value_weight,
    out_weight,
    query_probe,
    key_probe,
    value_probe,
    out_probe,
):
    rows, width = tokens.shape
    tables = rope_tables()

    def turned_over(array):
        return jnp.swapaxes(array, 1, 2)

    def all_rows(blocks):
        return blocks.reshape(-1, blocks.shape[-1])

    def by_batch(blocks):
        return blocks.reshape(blocks.shape[0], -1, blocks.shape[-1])

    probes = (query_probe, turned_over(key_probe), turned_over(value_probe), out_probe)
    q0, k0, v0, a_zero, x_one, t_one, h_one, th_one, kv, hs_zero, pq, pkv, po = head(
        lengths,
        tables,
        normed(tokens, gains),
        query_weight,
        out_weight,
        tokens.reshape(2, rows // 2, width),
        gains,
        turned_over(key_weight),
        turned_over(value_weight),
        probes,
    )
    q1, k1, v1, c_two, cb_one, ga_zero, ga_one, hs_one = turn(
        lengths,
        tables,
        query_weight,
        kv,
        pq,
        pkv,
        out_weight,
        po,
        all_rows(h_one),
        all_rows(th_one),
        t_one,
        a_zero,
    )
    cb_zero, gg_one, cs_one, mini = lower(
        lengths,
        tables,
        q1,
        k1,
        v1,
        all_rows(cb_one),
        out_weight,
        query_weight,
        kv,
        c_two,
        x_one,
        gains,
    )
    gg_zero, unused, q_one, g_one, o_both = last(
        lengths,
        tables,
        q0,
        k0,
        v0,
        all_rows(cb_zero),
        out_weight,
        mini,
        ga_zero,
        hs_one,
        gg_one,
        ga_one,
        cs_one,
    )
    q, k, v, o = products(by_batch(hs_zero), gg_zero, q_one, g_one, o_both)
    return (q, turned_over(k), turned_over(v), o)


def solution(mesh):
    placed = (
        P(("dp", "tensor"), None),
        P(),
        P(),
        P(None, None, "tensor"),
        P(None, None, "tensor"),
        P(None, None, "tensor"),
        P(None, "tensor", None),
        P(None, "dp", "tensor"),
        P(None, "dp", "tensor"),
        P(None, "dp", "tensor"),
        P(None, "tensor", "dp"),
    )
    return jax.shard_map(
        body,
        mesh=mesh,
        in_specs=placed,
        out_specs=(
            P(None, "dp", "tensor"),
            P(None, "dp", "tensor"),
            P(None, "dp", "tensor"),
            P(None, "tensor", "dp"),
        ),
        check_vma=False,
    )
```
